32 devices in a mesh: ep: 4 (over z), dp: 8 (over y, x, core).
Axes of the slice: x: 2, y: 2, z: 4, core: 2. Of those that a mesh axis runs over, the one named last changes fastest.
Arguments:
- act_in: bfloat16 [65536, 640], P(('ep', 'dp'))
- grad_out: bfloat16 [65536, 640], P(('ep', 'dp'))
- slot_ids: int32 [2, 65536, 1], P(None, ('ep', 'dp'))
- gate_vals: float32 [2, 65536, 1], P(None, ('ep', 'dp'))
- w_dense: bfloat16 [2, 640, 640], replicated
- w_gate: bfloat16 [2, 16, 640, 1024], P(None, 'ep')
- w_up: bfloat16 [2, 16, 640, 1024], P(None, 'ep')
- w_down: bfloat16 [2, 16, 1024, 640], P(None, 'ep')
- ws_gate: bfloat16 [2, 640, 1024], replicated
- ws_up: bfloat16 [2, 640, 1024], replicated
- ws_down: bfloat16 [2, 1024, 640], replicated
Outputs:
- output 1: bfloat16 [65536, 640], P(('ep', 'dp'))
- output 2: bfloat16 [2, 640, 640], replicated
- output 3: bfloat16 [2, 16, 640, 1024], P(None, 'ep')
- output 4: bfloat16 [2, 16, 640, 1024], P(None, 'ep')
- output 5: bfloat16 [2, 16, 1024, 640], P(None, 'ep')
- output 6: bfloat16 [2, 640, 1024], replicated
- output 7: bfloat16 [2, 640, 1024], replicated
- output 8: bfloat16 [2, 1024, 640], replicated
All inputs are finite; a program needn't handle non-finite values.
Results may differ from the reference program's by a relative error of at most 0.02.
Values are sent between devices in bfloat16 or wider.
A program may use at most 1 GiB of HBM per device.

```python
import functools
import jax
import jax.numpy as jnp
from jax import lax

D = 640
FF = 1024
FS = 1024
EXPERTS = 16
TOP = 1
TOKENS = 2048
EP = 4
DP = 8
LAYERS = 2

NUM_DEV = EP * DP
CAP = 2 * TOKENS * TOP // EXPERTS
ROWS = NUM_DEV * TOKENS


def draw_slots(key):
    key_tok, key_exp = jax.random.split(key)
    mean_load = TOKENS * TOP // EXPERTS
    order = jax.random.permutation(key_tok, TOKENS)
    position = jnp.arange(TOP, dtype=jnp.int32)[None, :] * TOKENS + order[:, None]
    group = position // (4 * mean_load)
    rest = position % (4 * mean_load)
    first = 2 * mean_load
    second = first + mean_load // 2
    third = second + mean_load // 2
    within = (rest >= first).astype(jnp.int32) + (rest >= second).astype(jnp.int32) + (rest >= third).astype(jnp.int32)
    start = jnp.where(rest >= third, third, jnp.where(rest >= second, second, jnp.where(rest >= first, first, 0)))
    expert_perm = jax.random.permutation(key_exp, EXPERTS)
    expert = expert_perm[group * 4 + within]
    return (expert * CAP + rest - start).astype(jnp.int32)


def setup_inputs(seed: int = 0) -> dict:
    keys = jax.random.split(jax.random.key(seed), 12)
    slot_keys = jax.random.split(keys[0], LAYERS * NUM_DEV)
    slot_ids = jax.vmap(draw_slots)(slot_keys).reshape(LAYERS, ROWS, TOP)
    gate_vals = jax.random.uniform(keys[1], (LAYERS, ROWS, TOP), jnp.float32, 0.5, 1.5) / TOP
    act_in = jax.random.normal(keys[2], (ROWS, D), jnp.float32).astype(jnp.bfloat16)
    grad_out = jax.random.normal(keys[3], (ROWS, D), jnp.float32).astype(jnp.bfloat16)
    w_dense = (jax.random.normal(keys[4], (LAYERS, D, D), jnp.float32) * D ** -0.5).astype(jnp.bfloat16)
    w_gate = (jax.random.normal(keys[5], (LAYERS, EXPERTS, D, FF), jnp.float32) * D ** -0.5).astype(jnp.bfloat16)
    w_up = (jax.random.normal(keys[6], (LAYERS, EXPERTS, D, FF), jnp.float32) * D ** -0.5).astype(jnp.bfloat16)
    w_down = (jax.random.normal(keys[7], (LAYERS, EXPERTS, FF, D), jnp.float32) * FF ** -0.5).astype(jnp.bfloat16)
    ws_gate = (jax.random.normal(keys[8], (LAYERS, D, FS), jnp.float32) * D ** -0.5).astype(jnp.bfloat16)
    ws_up = (jax.random.normal(keys[9], (LAYERS, D, FS), jnp.float32) * D ** -0.5).astype(jnp.bfloat16)
    ws_down = (jax.random.normal(keys[10], (LAYERS, FS, D), jnp.float32) * FS ** -0.5).astype(jnp.bfloat16)
    return {"act_in": act_in, "grad_out": grad_out, "slot_ids": slot_ids, "gate_vals": gate_vals, "w_dense": w_dense, "w_gate": w_gate, "w_up": w_up, "w_down": w_down, "ws_gate": ws_gate, "ws_up": ws_up, "ws_down": ws_down}


def expert_block(args, w_gate32, w_up32, w_down32):
    mixed_loc, slot_loc, gate_loc = args
    slot_flat = slot_loc.reshape(TOKENS * TOP)
    copies = jnp.broadcast_to(mixed_loc[:, None, :], (TOKENS, TOP, D)).reshape(TOKENS * TOP, D)
    dispatched = jnp.zeros((EXPERTS * CAP, D), mixed_loc.dtype).at[slot_flat].set(copies)
    dispatched = dispatched.reshape(EXPERTS, CAP, D).astype(jnp.float32)
    a_one = jnp.einsum("ecd,edf->ecf", dispatched, w_gate32)
    a_three = jnp.einsum("ecd,edf->ecf", dispatched, w_up32)
    hidden = (jax.nn.silu(a_one) * a_three).astype(jnp.bfloat16)
    exp_out = jnp.einsum("ecf,efd->ecd", hidden.astype(jnp.float32), w_down32).astype(jnp.bfloat16)
    picked = exp_out.reshape(EXPERTS * CAP, D)[slot_flat].reshape(TOKENS, TOP, D)
    return jnp.sum(gate_loc[:, :, None] * picked.astype(jnp.float32), axis=1)


def moe_layer(act, layer_in):
    w_dense, w_gate, w_up, w_down, ws_gate, ws_up, ws_down, slot_ids, gate_vals = layer_in
    dense_pre = jnp.dot(act, w_dense, preferred_element_type=jnp.float32)
    mixed = (act.astype(jnp.float32) + dense_pre).astype(jnp.bfloat16)
    s_one = jnp.dot(mixed, ws_gate, preferred_element_type=jnp.float32)
    s_three = jnp.dot(mixed, ws_up, preferred_element_type=jnp.float32)
    shared_hidden = (jax.nn.silu(s_one) * s_three).astype(jnp.bfloat16)
    shared_out = jnp.dot(shared_hidden, ws_down, preferred_element_type=jnp.float32)
    block = jax.checkpoint(functools.partial(expert_block, w_gate32=w_gate.astype(jnp.float32), w_up32=w_up.astype(jnp.float32), w_down32=w_down.astype(jnp.float32)))
    routed = lax.map(block, (mixed.reshape(NUM_DEV, TOKENS, D), slot_ids.reshape(NUM_DEV, TOKENS, TOP), gate_vals.reshape(NUM_DEV, TOKENS, TOP)))
    routed = routed.reshape(ROWS, D)
    new_act = (mixed.astype(jnp.float32) + routed + shared_out).astype(jnp.bfloat16)
    return new_act, None


def reference(act_in, grad_out, slot_ids, gate_vals, w_dense, w_gate, w_up, w_down, ws_gate, ws_up, ws_down):
    def forward(act, dense_all, gate_all, up_all, down_all, sgate_all, sup_all, sdown_all):
        final, _ = lax.scan(moe_layer, act, (dense_all, gate_all, up_all, down_all, sgate_all, sup_all, sdown_all, slot_ids, gate_vals))
        return final
    _, pullback = jax.vjp(forward, act_in, w_dense, w_gate, w_up, w_down, ws_gate, ws_up, ws_down)
    grads = pullback(grad_out)
    return (grads[0], grads[1], grads[2], grads[3], grads[4], grads[5], grads[6], grads[7])
```

```python
import jax
import jax.numpy as jnp
from jax import lax
from jax.sharding import PartitionSpec as P

ALL_AXES = ("ep", "dp")


def silu_grad(pre_act):
    sigma = jax.nn.sigmoid(pre_act)
    return sigma * (1.0 + pre_act * (1.0 - sigma))


def contract_rows(left, right):
    return lax.dot_general(left, right, (((0,), (0,)), ((), ())), preferred_element_type=jnp.float32)


def contract_cols(left, right):
    return lax.dot_general(left, right, (((1,), (1,)), ((), ())), preferred_element_type=jnp.float32)


def dot32(left, right):
    return jnp.dot(left, right, preferred_element_type=jnp.float32)


class Place:
    def __init__(self, mesh):
        self.ep, self.dp = mesh.shape["ep"], mesh.shape["dp"]
        self.half_ep = self.ep // 2
        self.group = self.half_ep * self.dp
        self.z = lax.axis_index("ep")
        self.j = lax.axis_index("dp")
        self.core = self.j % 2
        self.chip = self.j // 2
        self.half = self.z // self.half_ep
        self.groups = [[g * self.group + m for m in range(self.group)] for g in range(2)]
        every = range(self.ep * self.dp)
        self.swap_z = [(d, (d + self.group) % (2 * self.group)) for d in every]
        self.swap_core = [(d, d ^ 1) for d in every]

    def exchange(self, rows):
        blocks = rows.reshape(self.group, rows.shape[0] // self.group, rows.shape[1])
        return lax.all_to_all(blocks, ALL_AXES, 0, 0, axis_index_groups=self.groups).reshape(rows.shape)

    def to_partner(self, value):
        return lax.ppermute(value, ALL_AXES, self.swap_z)

    def to_sibling(self, value):
        return lax.ppermute(value, ALL_AXES, self.swap_core)

    def my_half(self, value, core):
        size = value.shape[0] // 2
        return lax.dynamic_slice_in_dim(value, core * size, size, axis=0)


def foreign_weight(place, own):
    got = place.to_partner(place.my_half(own, place.core))
    other = place.to_sibling(got)
    low = jnp.where(place.core == 0, got, other)
    high = jnp.where(place.core == 0, other, got)
    return jnp.concatenate([low, high], axis=0)


def take_rows(source, index):
    return jnp.take(source, index, axis=0, mode="clip")


def with_zero_row(rows):
    return jnp.pad(rows, ((0, 8), (0, 0)))


def ffn_front(rows, w_one, w_three):
    a_one = dot32(rows, w_one)
    a_three = dot32(rows, w_three)
    hidden = (jax.nn.silu(a_one) * a_three).astype(jnp.bfloat16)
    return a_one, a_three, hidden


def ffn_back(grad_out, front, w_two):
    a_one, a_three, _ = front
    grad_hidden = contract_cols(grad_out, w_two)
    grad_one = (grad_hidden * a_three * silu_grad(a_one)).astype(jnp.bfloat16)
    grad_three = (grad_hidden * jax.nn.silu(a_one)).astype(jnp.bfloat16)
    return grad_one, grad_three


def ffn_weight_grads(rows, grad_out, hidden, grad_one, grad_three):
    return (contract_rows(rows, grad_one).astype(jnp.bfloat16), contract_rows(rows, grad_three).astype(jnp.bfloat16), contract_rows(hidden, grad_out).astype(jnp.bfloat16))


def ffn_rows_grad(grad_one, grad_three, w_one, w_three):
    return contract_cols(grad_one, w_one) + contract_cols(grad_three, w_three)


def reduce_expert(place, own, foreign):
    theirs = [place.to_sibling(place.my_half(part, 1 - place.core)) for part in (own, foreign)]
    mine = [place.my_half(part, place.core).astype(jnp.float32) + got.astype(jnp.float32) for part, got in zip((own, foreign), theirs)]
    home = place.to_partner(mine[1].astype(jnp.bfloat16))
    total = (mine[0] + home.astype(jnp.float32)).astype(jnp.bfloat16)
    return lax.all_gather(total, "dp", axis=0, tiled=True).reshape((place.dp // 2,) + own.shape)


def solution(mesh):
    tok_spec = P(ALL_AXES, None)
    route_spec = P(None, ALL_AXES, None)
    exp_spec = P(None, "ep", None, None)
    repl_spec = P(None, None, None)

    def body(act_in, grad_out, slot_ids, gate_vals, w_dense, w_gate, w_up, w_down, ws_gate, ws_up, ws_down):
        place = Place(mesh)
        layers = w_dense.shape[0]
        tokens = act_in.shape[0]
        slots = 2 * tokens
        half_slots = slots // 2

        own_w = [[lax.dynamic_index_in_dim(w[layer], place.chip, 0, keepdims=False) for w in (w_gate, w_up, w_down)] for layer in range(layers)]
        foreign_w = [[foreign_weight(place, w) for w in own_w[layer]] for layer in range(layers)]

        token_ids = jnp.arange(tokens, dtype=jnp.int32)
        slot_idx = slot_ids.reshape(layers, tokens)
        turned = (slot_idx + place.half * half_slots) % slots
        flat = (turned + jnp.arange(layers, dtype=jnp.int32)[:, None] * slots).reshape(-1)
        owner = jnp.full((layers * slots,), tokens, jnp.int32).at[flat].set(jnp.tile(token_ids, layers), unique_indices=True).reshape(layers, 2, half_slots)

        def dispatch(layer, rows):
            ext = with_zero_row(rows)
            return [place.exchange(take_rows(ext, owner[layer, part])) for part in range(2)]

        def collect(layer, parts):
            back = jnp.concatenate([place.exchange(part) for part in parts], axis=0)
            return take_rows(back, turned[layer]).astype(jnp.float32)

        saved = []
        act = act_in
        for layer in range(layers):
            mixed = (act.astype(jnp.float32) + dot32(act, w_dense[layer])).astype(jnp.bfloat16)
            recv = dispatch(layer, mixed)
            weights = (own_w[layer], foreign_w[layer])
            fronts = [ffn_front(rows, w[0], w[1]) for rows, w in zip(recv, weights)]
            shared = ffn_front(mixed, ws_gate[layer], ws_up[layer])
            saved.append((act, mixed, recv, weights, fronts, shared))
            if layer + 1 < layers:
                outs = [dot32(front[2], w[2]).astype(jnp.bfloat16) for front, w in zip(fronts, weights)]
                routed = gate_vals[layer] * collect(layer, outs)
                act = (mixed.astype(jnp.float32) + routed + dot32(shared[2], ws_down[layer])).astype(jnp.bfloat16)

        grad_y = grad_out
        dense_sums = [None] * layers
        expert_sums = [None] * layers
        for layer in reversed(range(layers)):
            act, mixed, recv, weights, fronts, shared = saved[layer]
            grad_y32 = grad_y.astype(jnp.float32)
            grad_recv = dispatch(layer, (gate_vals[layer] * grad_y32).astype(jnp.bfloat16))
            backs = [ffn_back(g, front, w[2]) for g, front, w in zip(grad_recv, fronts, weights)]
            grad_rows = [ffn_rows_grad(b[0], b[1], w[0], w[1]).astype(jnp.bfloat16) for b, w in zip(backs, weights)]
            grad_routed = collect(layer, grad_rows)
            parts = [ffn_weight_grads(rows, g, front[2], b[0], b[1]) for rows, g, front, b in zip(recv, grad_recv, fronts, backs)]
            expert_sums[layer] = [reduce_expert(place, own, foreign) for own, foreign in zip(*parts)]
            s_back = ffn_back(grad_y, shared, ws_down[layer])
            s_grads = ffn_weight_grads(mixed, grad_y, shared[2], s_back[0], s_back[1])
            grad_mixed = (grad_y32 + grad_routed + ffn_rows_grad(s_back[0], s_back[1], ws_gate[layer], ws_up[layer])).astype(jnp.bfloat16)
            g_dense = contract_rows(act, grad_mixed).astype(jnp.bfloat16)
            grad_y = (grad_mixed.astype(jnp.float32) + contract_cols(grad_mixed, w_dense[layer])).astype(jnp.bfloat16)
            dense_sums[layer] = [lax.psum(part, ALL_AXES) for part in (g_dense,) + s_grads]
        dense_out = [jnp.stack([dense_sums[layer][which] for layer in range(layers)]) for which in range(4)]
        expert_out = [jnp.stack([expert_sums[layer][which] for layer in range(layers)]) for which in range(3)]
        return (grad_y, dense_out[0], expert_out[0], expert_out[1], expert_out[2], dense_out[1], dense_out[2], dense_out[3])

    return jax.shard_map(body, mesh=mesh, in_specs=(tok_spec, tok_spec, route_spec, route_spec, repl_spec, exp_spec, exp_spec, exp_spec, repl_spec, repl_spec, repl_spec), out_specs=(tok_spec, repl_spec, exp_spec, exp_spec, exp_spec, repl_spec, repl_spec, repl_spec), check_vma=False)
```

```python
import functools

import jax
import jax.numpy as jnp
from jax import lax
from jax.experimental import pallas as pl
from jax.experimental.pallas import tpu as pltpu
from jax.sharding import PartitionSpec as P


ALL_AXES = ("ep", "dp")
MESH = pl.DeviceIdType.MESH
STEPS = 2


def contract_rows(left, right):
    return lax.dot_general(left, right, (((0,), (0,)), ((), ())), preferred_element_type=jnp.float32)


def contract_cols(left, right):
    return lax.dot_general(left, right, (((1,), (1,)), ((), ())), preferred_element_type=jnp.float32)


def dot32(left, right):
    return jnp.dot(left, right, preferred_element_type=jnp.float32)


class Geometry:
    def __init__(self, ep, dp):
        self.ep, self.dp = ep, dp
        self.chips = (ep // 2) * (dp // 2)
        z, j = lax.axis_index("ep"), lax.axis_index("dp")
        self.core = j % 2
        self.local = j // 2
        self.base = (z // (ep // 2)) * (ep // 2)
        self.chip = (z % (ep // 2)) * (dp // 2) + j // 2
        self.me = 2 * self.chip + self.core
        self.sibling = (z, (j // 2) * 2 + 1 - self.core)
        self.partner = ((z + ep // 2) % ep, j)

    def member(self, index):
        return (self.base + index // self.dp, index % self.dp)

    def out_chip(self, step):
        return (self.chip + step) % self.chips

    def in_chip(self, step):
        return (self.chip - step + self.chips) % self.chips

    def entry_barrier(self):
        barrier = pltpu.get_barrier_semaphore()

        @pl.loop(1, self.chips)
        def _(step):
            for core in range(2):
                pl.semaphore_signal(barrier, inc=1, device_id=self.member(2 * self.out_chip(step) + core), device_id_type=MESH)

        for device in (self.sibling, self.partner):
            pl.semaphore_signal(barrier, inc=1, device_id=device, device_id_type=MESH)
        pl.semaphore_wait(barrier, 2 * self.chips)


class Outbound:
    def __init__(self, geo, send, recv, send_sem, recv_sem):
        self.geo, self.send, self.recv, self.send_sem, self.recv_sem = geo, send, recv, send_sem, recv_sem

    def copy(self, step, core):
        geo = self.geo
        index = 2 * geo.out_chip(step) + core
        return pltpu.make_async_remote_copy(src_ref=self.send.at[index], dst_ref=self.recv.at[step, geo.core], send_sem=self.send_sem.at[step, core], recv_sem=self.recv_sem.at[step, geo.core], device_id=geo.member(index), device_id_type=MESH)

    def own(self):
        geo = self.geo
        return pltpu.make_async_copy(self.send.at[geo.me], self.recv.at[0, geo.core], self.recv_sem.at[0, geo.core])

    def start(self):
        self.own().start()
        self.copy(0, 1 - self.geo.core).start()

        @pl.loop(1, self.geo.chips)
        def _(step):
            for core in range(2):
                self.copy(step, core).start()

    def wait_recv(self, step):
        for core in range(2):
            pltpu.make_async_copy(self.send.at[0], self.recv.at[step, core], self.recv_sem.at[step, core]).wait()

    def wait_sends(self):
        self.copy(0, 1 - self.geo.core).wait_send()

        @pl.loop(1, self.geo.chips)
        def _(step):
            for core in range(2):
                self.copy(step, core).wait_send()


class Return:
    def __init__(self, geo, rows, back, send_sem, recv_sem):
        self.geo, self.rows, self.back, self.send_sem, self.recv_sem = geo, rows, back, send_sem, recv_sem

    def copy(self, step, core):
        geo = self.geo
        return pltpu.make_async_remote_copy(src_ref=self.rows.at[step, core], dst_ref=self.back.at[geo.me], send_sem=self.send_sem.at[step, core], recv_sem=self.recv_sem.at[geo.me], device_id=geo.member(2 * geo.in_chip(step) + core), device_id_type=MESH)

    def start(self, step):
        geo = self.geo

        @pl.when(step == 0)
        def _():
            pltpu.make_async_copy(self.rows.at[0, geo.core], self.back.at[geo.me], self.recv_sem.at[geo.me]).start()
            self.copy(0, 1 - geo.core).start()

        @pl.when(step > 0)
        def _():
            for core in range(2):
                self.copy(step, core).start()

    def wait_all(self):
        geo = self.geo
        self.copy(0, 1 - geo.core).wait_send()

        @pl.loop(1, geo.chips)
        def _(step):
            for core in range(2):
                self.copy(step, core).wait_send()

        @pl.loop(0, 2 * geo.chips)
        def _(index):
            pltpu.make_async_copy(self.rows.at[0, 0], self.back.at[index], self.recv_sem.at[index]).wait()


def half_rows(rows, core):
    return pl.ds(pl.multiple_of(core * (rows // 2), 8), rows // 2)


class WeightSwap:
    def __init__(self, geo, layer, own, foreign, sems):
        self.geo, self.layer, self.own, self.foreign, self.sems = geo, layer, own, foreign, sems

    def over(self, which):
        geo = self.geo
        rows = half_rows(self.foreign[which].shape[0], geo.core)
        return pltpu.make_async_remote_copy(src_ref=self.own[which].at[self.layer, geo.local, rows], dst_ref=self.foreign[which].at[rows], send_sem=self.sems.at[0, which], recv_sem=self.sems.at[1, which], device_id=geo.partner, device_id_type=MESH)

    def across(self, which):
        geo = self.geo
        rows = self.foreign[which].at[half_rows(self.foreign[which].shape[0], geo.core)]
        return pltpu.make_async_remote_copy(src_ref=rows, dst_ref=rows, send_sem=self.sems.at[2, which], recv_sem=self.sems.at[3, which], device_id=geo.sibling, device_id_type=MESH)

    def start(self):
        for which in range(3):
            self.over(which).start()

    def pass_on(self):
        for which in range(3):
            self.over(which).wait()
            self.across(which).start()

    def finish(self):
        for which in range(3):
            self.across(which).wait()


def silu(value):
    return value * jax.nn.sigmoid(value)


def forward_kernel(ep, dp, send, mixed, *refs):
    refs = list(refs)

    def take(count):
        got = refs[:count]
        del refs[:count]
        return got

    experts, ws, got = take(3), take(3), take(3)
    recv_out, back, shared = take(3)
    keep_out, next_out = take(3), take(3)
    recv, outs = take(2)
    shared_w, own_w, foreign_w = take(3), take(3), take(3)
    go_sem, get_sem, ret_sem, res_sem, swap_sem, pass_sem, load_sem, save_sem = refs
    geo = Geometry(ep, dp)
    geo.entry_barrier()
    outbound = [Outbound(geo, send.at[part], recv.at[part], go_sem.at[part], get_sem.at[part]) for part in range(2)]
    returns = [Return(geo, outs.at[part], back.at[part], ret_sem.at[part], res_sem.at[part]) for part in range(2)]
    swap = WeightSwap(geo, 1, experts, next_out, swap_sem)
    outbound[0].start()
    loads = []
    passes = []
    for which in range(3):
        mine = half_rows(foreign_w[which].shape[0], geo.core)
        loads.append(pltpu.make_async_copy(ws[which].at[0], shared_w[which], load_sem.at[0, which]))
        loads.append(pltpu.make_async_copy(experts[which].at[0, geo.local], own_w[which], load_sem.at[1, which]))
        loads.append(pltpu.make_async_copy(got[which], foreign_w[which].at[mine], load_sem.at[2, which]))
        passes.append(pltpu.make_async_remote_copy(src_ref=got[which], dst_ref=foreign_w[which].at[mine], send_sem=pass_sem.at[0, which], recv_sem=pass_sem.at[1, which], device_id=geo.sibling, device_id_type=MESH))
    for copy in loads + passes:
        copy.start()
    outbound[1].start()
    swap.start()

    tile = 2 * STEPS * recv.shape[3]

    def ffn(rows, w_one, w_three, w_two):
        a_one = dot32(rows, w_one[...])
        a_three = dot32(rows, w_three[...])
        hidden = (silu(a_one) * a_three).astype(jnp.bfloat16)
        return dot32(hidden, w_two[...])

    for copy in loads + passes:
        copy.wait()

    @pl.loop(0, mixed.shape[0] // tile)
    def _(t):
        at = pl.ds(pl.multiple_of(t * tile, tile), tile)
        shared[at, :] = ffn(mixed[at, :], *shared_w)

    keeps = [pltpu.make_async_copy(src, dst, load_sem.at[0, which]) for which, (src, dst) in enumerate(zip(foreign_w, keep_out))]
    for keep in keeps:
        keep.start()
    width = mixed.shape[1]
    for part, weights in enumerate((own_w, foreign_w)):

        @pl.loop(0, geo.chips // STEPS)
        def _(t):
            steps = pl.ds(t * STEPS, STEPS)
            for step in range(STEPS):
                outbound[part].wait_recv(t * STEPS + step)
            pltpu.make_async_copy(recv.at[part, steps], recv_out.at[part, steps], save_sem.at[part, t]).start()
            rows = recv[part, steps].reshape(tile, width)
            outs[part, steps] = ffn(rows, *weights).astype(jnp.bfloat16).reshape(STEPS, 2, tile // (2 * STEPS), width)

            @pl.when(t > 0)
            def _():
                for step in range(STEPS):
                    returns[part].start((t - 1) * STEPS + step)

        for step in range(STEPS):
            returns[part].start(geo.chips - STEPS + step)
    swap.pass_on()
    for part in range(2):
        outbound[part].wait_sends()
        returns[part].wait_all()

        @pl.loop(0, geo.chips // STEPS)
        def _(t):
            steps = pl.ds(t * STEPS, STEPS)
            pltpu.make_async_copy(recv.at[part, steps], recv_out.at[part, steps], save_sem.at[part, t]).wait()

    for keep in keeps:
        keep.wait()
    swap.finish()


def forward_exchange(mesh, send, mixed, experts, shared, got):
    ep, dp = mesh.shape["ep"], mesh.shape["dp"]
    members, block, width = send.shape[1:]
    tokens = mixed.shape[0]
    bf16, f32 = jnp.bfloat16, jnp.float32
    shapes = [w.shape[2:] for w in experts]
    hidden = shapes[0][1]
    chips = members // 2
    anywhere = pl.BlockSpec(memory_space=pl.ANY)
    inside = pl.BlockSpec(memory_space=pltpu.VMEM)
    flops = 2 * 3 * width * hidden * (2 * members * block + tokens)
    expert = [jax.ShapeDtypeStruct(s, bf16) for s in shapes]
    dma = pltpu.SemaphoreType.DMA
    return pl.pallas_call(
        functools.partial(forward_kernel, ep, dp),
        name="forward_exchange",
        out_shape=[jax.ShapeDtypeStruct((2, chips, 2, block, width), bf16), jax.ShapeDtypeStruct((2, members, block, width), bf16), jax.ShapeDtypeStruct((tokens, width), f32)] + expert + expert,
        in_specs=[anywhere, inside] + [anywhere] * 9,
        out_specs=[anywhere, anywhere, inside] + [anywhere] * 6,
        scratch_shapes=[pltpu.VMEM((2, chips, 2, block, width), bf16) for _ in range(2)]
        + [pltpu.VMEM(s, bf16) for _ in range(3) for s in shapes]
        + [dma((2, chips, 2)), dma((2, chips, 2)), dma((2, chips, 2)), dma((2, members)), dma((4, 3)), dma((2, 3)), dma((3, 3)), dma((2, chips // STEPS))],
        compiler_params=pltpu.CompilerParams(collective_id=0, has_side_effects=True, vmem_limit_bytes=60 * 2**20),
        cost_estimate=pl.CostEstimate(flops=flops, bytes_accessed=40 * 2**20, transcendentals=0),
    )(send, mixed, *experts, *shared, *got)


class PairSum:
    def __init__(self, geo, stages, theirs, sems, expert):
        self.geo, self.stages, self.theirs, self.sems, self.expert = geo, stages, theirs, sems, expert

    def mine(self, which):
        return self.stages[which].at[self.expert, half_rows(self.stages[which].shape[1], self.geo.core)]

    def copy(self, which):
        geo = self.geo
        return pltpu.make_async_remote_copy(src_ref=self.stages[which].at[self.expert, half_rows(self.stages[which].shape[1], 1 - geo.core)], dst_ref=self.theirs[which].at[self.expert], send_sem=self.sems.at[0, self.expert, which], recv_sem=self.sems.at[1, self.expert, which], device_id=geo.sibling, device_id_type=MESH)

    def start(self):
        for which in range(3):
            self.copy(which).start()

    def finish(self):
        for which in range(3):
            self.copy(which).wait()
            mine = self.mine(which)
            mine[...] = (mine[...].astype(jnp.float32) + self.theirs[which][self.expert].astype(jnp.float32)).astype(jnp.bfloat16)


def backward_kernel(ep, dp, layer, *refs):
    refs = list(refs)

    def take(count):
        got = refs[:count]
        del refs[:count]
        return got

    held, send, mixed, grad_y = take(4)
    own_w, foreign_w, shared_w = take(3), take(3), take(3)
    back, shared_dx, recv = take(3)
    shared_out, own_out = take(3), take(3)
    x_buf, g_buf, dx_rows, dx_buf = take(4)
    weights, acc, stages, theirs, partner_in = take(3), take(3), take(3), take(3), take(3)
    go_sem, get_sem, ret_sem, res_sem, partner_sem, load_sem, x_sem, g_sem, dx_sem, pair_sem = refs

    geo = Geometry(ep, dp)
    geo.entry_barrier()
    tile = 2 * send.shape[2]
    width = mixed.shape[1]
    per_set = mixed.shape[0] // tile
    total = 3 * per_set
    outbound = [Outbound(geo, send.at[part], recv.at[part], go_sem.at[part], get_sem.at[part]) for part in range(2)]
    returns = [Return(geo, dx_rows.at[part], back.at[part], ret_sem.at[part], res_sem.at[part]) for part in range(2)]
    pairs = [PairSum(geo, stages, theirs, pair_sem, expert) for expert in range(2)]
    outbound[1].start()
    loads = []
    for which in range(3):
        loads.append(pltpu.make_async_copy(shared_w[which].at[layer], weights[which].at[2], load_sem.at[2, which]))
        loads.append(pltpu.make_async_copy(own_w[which].at[layer, geo.local], weights[which].at[0], load_sem.at[0, which]))
        loads.append(pltpu.make_async_copy(foreign_w[which], weights[which].at[1], load_sem.at[1, which]))
    for load in loads:
        load.start()
    outbound[0].start()
    moved, moved_sem, kept, kept_sem = (x_buf, x_sem, g_buf, g_sem) if layer else (g_buf, g_sem, x_buf, x_sem)

    def held_block(part, step, core):
        if layer:
            return held.at[2 * geo.in_chip(step) + core, part]
        return held.at[part, step, core]

    def fetch(i, slot):
        @pl.when(i < per_set)
        def _():
            at = pl.ds(pl.multiple_of(i * tile, tile), tile)
            pltpu.make_async_copy(mixed.at[at], x_buf.at[slot], x_sem.at[slot]).start()
            pltpu.make_async_copy(grad_y.at[at], g_buf.at[slot], g_sem.at[slot]).start()

        for part in range(2):
            begin = (2 - part) * per_set

            @pl.when((i >= begin) & (i < begin + per_set))
            def _(part=part, begin=begin):
                step = i - begin
                outbound[part].wait_recv(step)
                for core in range(2):
                    at = pl.ds(core * (tile // 2), tile // 2)
                    pltpu.make_async_copy(recv.at[part, step, core], moved.at[slot, at], moved_sem.at[slot]).start()
                    pltpu.make_async_copy(held_block(part, step, core), kept.at[slot, at], kept_sem.at[slot]).start()

    def store_shared(i):
        return pltpu.make_async_copy(dx_buf.at[i % 2], shared_dx.at[pl.ds(pl.multiple_of(i * tile, tile), tile)], dx_sem.at[i % 2])

    def partner_copies():
        return [pltpu.make_async_remote_copy(src_ref=pairs[1].mine(which), dst_ref=partner_in[which], send_sem=partner_sem.at[0, which], recv_sem=partner_sem.at[1, which], device_id=geo.partner, device_id_type=MESH) for which in range(3)]

    fetch(0, 0)
    for load in loads:
        load.wait()

    @pl.loop(0, total)
    def _(i):
        slot = i % 2
        which_set = 2 - i // per_set
        fetch(i + 1, (i + 1) % 2)
        pltpu.make_async_copy(mixed.at[pl.ds(0, tile)], x_buf.at[slot], x_sem.at[slot]).wait()
        pltpu.make_async_copy(mixed.at[pl.ds(0, tile)], g_buf.at[slot], g_sem.at[slot]).wait()

        @pl.when(i % per_set == 0)
        def _():
            for a in acc:
                a[...] = jnp.zeros(a.shape, jnp.float32)

        x = x_buf[slot]
        g = g_buf[slot]
        w_one, w_three, w_two = [w.at[which_set] for w in weights]
        a_one = dot32(x, w_one[...])
        a_three = dot32(x, w_three[...])
        grad_hidden = contract_cols(g, w_two[...])
        sigma = jax.nn.sigmoid(a_one)
        gated = a_one * sigma
        hidden = (gated * a_three).astype(jnp.bfloat16)
        grad_one = (grad_hidden * a_three * (sigma * (1.0 + a_one * (1.0 - sigma)))).astype(jnp.bfloat16)
        grad_three = (grad_hidden * gated).astype(jnp.bfloat16)
        acc[0][...] += contract_rows(x, grad_one)
        acc[1][...] += contract_rows(x, grad_three)
        acc[2][...] += contract_rows(hidden, g)
        dx = contract_cols(grad_one, w_one[...]) + contract_cols(grad_three, w_three[...])

        @pl.when(i < per_set)
        def _():
            pl.when(i >= 2)(lambda: store_shared(i - 2).wait())
            dx_buf[slot] = dx
            store_shared(i).start()

        @pl.when(i == per_set - 1)
        def _():
            for a, out in zip(acc, shared_out):
                out[...] = a[...].astype(jnp.bfloat16)

        for part in range(2):
            begin = (2 - part) * per_set

            @pl.when((i >= begin) & (i < begin + per_set))
            def _(part=part, begin=begin):
                dx_rows[part, i - begin] = dx.astype(jnp.bfloat16).reshape(2, tile // 2, width)

            @pl.when((i > begin) & (i <= begin + per_set))
            def _(part=part, begin=begin):
                returns[part].start(i - 1 - begin)

            @pl.when(i == begin + per_set - 1)
            def _(part=part):
                for a, stage in zip(acc, stages):
                    stage[part] = a[...].astype(jnp.bfloat16)

        pl.when(i == 2 * per_set)(pairs[1].start)
        pl.when(i == 2 * per_set + 1)(pairs[1].finish)

        @pl.when(i == 2 * per_set + 2)
        def _():
            for copy in partner_copies():
                copy.start()

    returns[0].start(per_set - 1)
    pairs[0].start()
    pairs[0].finish()
    for which, copy in enumerate(partner_copies()):
        copy.wait()
        own_out[which][...] = (pairs[0].mine(which)[...].astype(jnp.float32) + partner_in[which][...].astype(jnp.float32)).astype(jnp.bfloat16)
    store_shared(per_set - 2).wait()
    store_shared(per_set - 1).wait()
    for part in range(2):
        outbound[part].wait_sends()
        returns[part].wait_all()


def backward_exchange(mesh, layer, held, send, mixed, grad_y, own, foreign, shared):
    ep, dp = mesh.shape["ep"], mesh.shape["dp"]
    members, block, width = send.shape[1:]
    chips = members // 2
    tokens = mixed.shape[0]
    tile = 2 * block
    bf16, f32 = jnp.bfloat16, jnp.float32
    anywhere = pl.BlockSpec(memory_space=pl.ANY)
    inside = pl.BlockSpec(memory_space=pltpu.VMEM)
    shapes = [w.shape for w in foreign]
    halves = [(s[0] // 2, s[1]) for s in shapes]
    like = jax.ShapeDtypeStruct
    by_step = like((2, chips, 2, block, width), bf16)
    outs = [like((2, members, block, width), bf16), like((tokens, width), f32), by_step] + [like(s, bf16) for s in shapes + halves]
    vmem = pltpu.VMEM
    scratch = [vmem((2, tile, width), bf16), vmem((2, tile, width), bf16), vmem(by_step.shape, bf16), vmem((2, tile, width), f32)]
    scratch += [vmem((3,) + s, bf16) for s in shapes] + [vmem(s, f32) for s in shapes] + [vmem((2,) + s, bf16) for s in shapes]
    scratch += [vmem((2,) + s, bf16) for s in halves] + [vmem(s, bf16) for s in halves]
    dma = pltpu.SemaphoreType.DMA
    scratch += [dma((2, chips, 2)), dma((2, chips, 2)), dma((2, chips, 2)), dma((2, members)), dma((2, 3)), dma((3, 3)), dma((2,)), dma((2,)), dma((2,)), dma((2, 2, 3))]
    operands = [held, send, mixed, grad_y, *own, *foreign, *shared]
    flops = 2 * 8 * width * shapes[0][1] * (2 * members * block + tokens)
    return pl.pallas_call(
        functools.partial(backward_kernel, ep, dp, layer),
        name="backward_second" if layer else "backward_first",
        out_shape=outs,
        in_specs=[anywhere] * len(operands),
        out_specs=[anywhere] * 3 + [inside] * 6,
        scratch_shapes=scratch,
        compiler_params=pltpu.CompilerParams(collective_id=1 + layer, has_side_effects=True, vmem_limit_bytes=63 * 2**20),
        cost_estimate=pl.CostEstimate(flops=flops, bytes_accessed=60 * 2**20, transcendentals=0),
    )(*operands)


def final_kernel(ep, dp, *refs):
    refs = list(refs)

    def take(count):
        got = refs[:count]
        del refs[:count]
        return got

    halves, parts = take(3), take(4)
    full, sums = take(3), take(4)
    first, mine, wide, piece, other, last = [take(4) for _ in range(6)]
    load_sem, pair_sem, wide_send, wide_recv, partner_sem, spread_send, spread_recv, cross_sem, gather_send, gather_recv, local_sem, fold_sem = refs
    geo = Geometry(ep, dp)
    geo.entry_barrier()
    plane = dp // 2
    z, core = lax.axis_index("ep"), geo.core
    four, three = range(4), range(3)
    f32, bf16 = jnp.float32, jnp.bfloat16

    to_sibling = [pltpu.make_async_remote_copy(src_ref=parts[n].at[1 - core], dst_ref=first[n], send_sem=pair_sem.at[0, n], recv_sem=pair_sem.at[1, n], device_id=geo.sibling, device_id_type=MESH) for n in four]
    keep = [pltpu.make_async_copy(parts[n].at[core], mine[n], load_sem.at[n]) for n in four]
    for copy in to_sibling + keep:
        copy.start()

    def gather(n, step):
        to = (geo.local + step) % plane
        return pltpu.make_async_remote_copy(src_ref=halves[n], dst_ref=full[n].at[geo.local, core], send_sem=gather_send.at[n, step], recv_sem=gather_recv.at[n, step], device_id=(z, 2 * to + core), device_id_type=MESH)

    def gathered(n, step):
        return full[n].at[(geo.local - step + plane) % plane, core]

    def fold(n, step):
        return pltpu.make_async_remote_copy(src_ref=gathered(n, step), dst_ref=gathered(n, step), send_sem=fold_sem.at[0, n, step], recv_sem=fold_sem.at[1, n, step], device_id=geo.sibling, device_id_type=MESH)

    def fold_own(n):
        return pltpu.make_async_remote_copy(src_ref=halves[n], dst_ref=full[n].at[geo.local, core], send_sem=fold_sem.at[0, n, 0], recv_sem=fold_sem.at[1, n, 0], device_id=geo.sibling, device_id_type=MESH)

    local = [pltpu.make_async_copy(halves[n], full[n].at[geo.local, core], local_sem.at[n]) for n in three]

    for n in four:
        to_sibling[n].wait()
        keep[n].wait()
        mine[n][...] = (mine[n][...].astype(f32) + first[n][...].astype(f32)).astype(bf16)

    def widen(n, step):
        to = geo.out_chip(step)
        return pltpu.make_async_remote_copy(src_ref=mine[n].at[to], dst_ref=wide[n].at[step], send_sem=wide_send.at[n, step], recv_sem=wide_recv.at[n, step], device_id=geo.member(2 * to + core), device_id_type=MESH)

    for n in four:
        for step in range(1, geo.chips):
            widen(n, step).start()
    for n in three:
        local[n].start()
        fold_own(n).start()
        for step in range(1, plane):
            gather(n, step).start()
    for n in four:
        total = mine[n][geo.chip].astype(f32)
        for step in range(1, geo.chips):
            widen(n, step).wait()
            total += wide[n][step].astype(f32)
        piece[n][...] = total.astype(bf16)

    def swap(n):
        return pltpu.make_async_remote_copy(src_ref=piece[n], dst_ref=other[n], send_sem=partner_sem.at[0, n], recv_sem=partner_sem.at[1, n], device_id=geo.partner, device_id_type=MESH)

    for n in four:
        swap(n).start()
    for n in four:
        swap(n).wait()
        last[n][...] = (piece[n][...].astype(f32) + other[n][...].astype(f32)).astype(bf16)

    def spread(n, step):
        return pltpu.make_async_remote_copy(src_ref=last[n], dst_ref=sums[n].at[core, geo.chip], send_sem=spread_send.at[n, step], recv_sem=spread_recv.at[n, step], device_id=geo.member(2 * geo.out_chip(step) + core), device_id_type=MESH)

    own = [pltpu.make_async_copy(last[n], sums[n].at[core, geo.chip], load_sem.at[n]) for n in four]
    for n in four:
        own[n].start()
        for step in range(1, geo.chips):
            spread(n, step).start()
    for n in three:
        local[n].wait()
        fold_own(n).wait()
        for step in range(1, plane):
            gather(n, step).wait()
            fold(n, step).start()

    def cross(n):
        return pltpu.make_async_remote_copy(src_ref=sums[n].at[core], dst_ref=sums[n].at[core], send_sem=cross_sem.at[0, n], recv_sem=cross_sem.at[1, n], device_id=geo.sibling, device_id_type=MESH)

    for n in four:
        own[n].wait()
        for step in range(1, geo.chips):
            spread(n, step).wait()
        cross(n).start()
    for n in four:
        cross(n).wait()
    for n in three:
        for step in range(1, plane):
            fold(n, step).wait()


def final_exchange(mesh, halves, parts):
    ep, dp = mesh.shape["ep"], mesh.shape["dp"]
    chips, plane = ep * dp // 4, dp // 2
    bf16 = jnp.bfloat16
    anywhere = pl.BlockSpec(memory_space=pl.ANY)
    like = jax.ShapeDtypeStruct
    cut = [part.reshape(2, chips, part.shape[0] // (2 * chips), part.shape[1]) for part in parts]
    piece = [c.shape[2:] for c in cut]
    vmem, dma = pltpu.VMEM, pltpu.SemaphoreType.DMA
    scratch = [vmem((chips,) + s, bf16) for _ in range(3) for s in piece] + [vmem(s, bf16) for _ in range(3) for s in piece]
    scratch += [dma((4,)), dma((2, 4)), dma((4, chips)), dma((4, chips)), dma((2, 4)), dma((4, chips)), dma((4, chips)), dma((2, 4)), dma((3, plane)), dma((3, plane)), dma((3,)), dma((2, 3, plane))]
    outs = pl.pallas_call(
        functools.partial(final_kernel, ep, dp),
        name="final_exchange",
        out_shape=[like((plane, 2) + h.shape, bf16) for h in halves] + [like(c.shape, bf16) for c in cut],
        in_specs=[anywhere] * 7,
        out_specs=[anywhere] * 7,
        scratch_shapes=scratch,
        compiler_params=pltpu.CompilerParams(collective_id=3, has_side_effects=True, vmem_limit_bytes=40 * 2**20),
        cost_estimate=pl.CostEstimate(flops=10**10, bytes_accessed=30 * 2**20, transcendentals=0),
    )(*halves, *cut)
    full = [out.reshape(plane, 2 * out.shape[2], out.shape[3]) for out in outs[:3]]
    return full, [out.reshape(part.shape) for out, part in zip(outs[3:], parts)]


def take_rows(source, index):
    return jnp.take(source, index, axis=0, mode="clip")


def solution(mesh):
    tok_spec = P(ALL_AXES, None)
    route_spec = P(None, ALL_AXES, None)
    exp_spec = P(None, "ep", None, None)
    repl_spec = P(None, None, None)
    ep, dp = mesh.shape["ep"], mesh.shape["dp"]
    members = ep * dp // 2
    to_partner = [(d, (d + members) % (2 * members)) for d in range(2 * members)]
    groups = [[side * members + m for m in range(members)] for side in range(2)]

    def body(act_in, grad_out, slot_ids, gate_vals, w_dense, w_gate, w_up, w_down, ws_gate, ws_up, ws_down):
        tokens, width = act_in.shape
        slots = 2 * tokens
        block = tokens // members
        experts = (w_gate, w_up, w_down)
        shared = (ws_gate, ws_up, ws_down)
        core, local = lax.axis_index("dp") % 2, lax.axis_index("dp") // 2

        got = []
        for w in experts:
            rows, columns = w.shape[2] // 2, w.shape[3]
            mine = lax.dynamic_slice(w, (0, local, core * rows, 0), (1, 1, rows, columns)).reshape(rows, columns)
            got.append(lax.ppermute(mine, ALL_AXES, to_partner))

        side = lax.axis_index("ep") // (ep // 2)
        turned = (slot_ids.reshape(2, tokens) + side * tokens) % slots
        flat = (turned + jnp.arange(2, dtype=jnp.int32)[:, None] * slots).reshape(-1)
        token_ids = jnp.tile(jnp.arange(tokens, dtype=jnp.int32), 2)
        owner = jnp.full((2 * slots,), tokens, jnp.int32).at[flat].set(token_ids, unique_indices=True).reshape(2, 2, members, block)

        def extended(rows):
            return jnp.pad(rows, ((0, 8), (0, 0)))

        def to_slots(layer, rows):
            return take_rows(extended(rows), owner[layer].reshape(-1)).reshape(2, members, block, width)

        def from_slots(layer, back):
            return take_rows(back.reshape(slots, width), turned[layer]).astype(jnp.float32)

        def mix(act, layer):
            return (act.astype(jnp.float32) + dot32(act, w_dense[layer])).astype(jnp.bfloat16)

        def gated(grad, layer):
            return (gate_vals[layer] * grad.astype(jnp.float32)).astype(jnp.bfloat16)

        by_member = owner[1].transpose(1, 0, 2).reshape(-1)
        grads_two = take_rows(extended(gated(grad_out, 1)), by_member).reshape(members, 2, block, width)
        mixed_one = mix(act_in, 0)
        sent_one = to_slots(0, mixed_one)
        sent_one, grads_two = lax.optimization_barrier((sent_one, grads_two))
        recv, back, shared_y, *foreign = forward_exchange(mesh, sent_one, mixed_one, experts, shared, got)
        back, grads_two = lax.optimization_barrier((back, grads_two))
        grads_two = lax.all_to_all(grads_two, ALL_AXES, 0, 0, axis_index_groups=groups)
        routed = from_slots(0, back)
        act_two = (mixed_one.astype(jnp.float32) + gate_vals[0] * routed + shared_y).astype(jnp.bfloat16)
        mixed_two = mix(act_two, 1)

        def finish(layer, act, grad_y, back, shared_dx):
            routed = from_slots(layer, back)
            grad_mixed = (grad_y.astype(jnp.float32) + routed + shared_dx).astype(jnp.bfloat16)
            g_dense = contract_rows(act, grad_mixed).astype(jnp.bfloat16)
            return (grad_mixed.astype(jnp.float32) + contract_cols(grad_mixed, w_dense[layer])).astype(jnp.bfloat16), g_dense

        def gather(half):
            return lax.all_gather(half, "dp", axis=0, tiled=True).reshape((dp // 2, 2 * half.shape[0], half.shape[1]))

        out = backward_exchange(mesh, 1, grads_two, to_slots(1, mixed_two), mixed_two, grad_out, experts, foreign[3:], shared)
        shared_two, own_two = out[3:6], out[6:9]
        experts_two = [gather(half) for half in own_two]
        grad_one, dense_two = finish(1, act_two, grad_out, out[0], out[1])
        sums_two = [lax.psum(part, ALL_AXES) for part in (dense_two, *shared_two)]

        out = backward_exchange(mesh, 0, recv, to_slots(0, gated(grad_one, 0)), mixed_one, grad_one, experts, foreign[:3], shared)
        shared_one, own_one = out[3:6], out[6:9]
        grad_act, dense_one = finish(0, act_in, grad_one, out[0], out[1])
        experts_one, sums_one = final_exchange(mesh, own_one, [dense_one, *shared_one])

        expert_out = [jnp.stack(pair) for pair in zip(experts_one, experts_two)]
        sums_out = [jnp.stack(pair) for pair in zip(sums_one, sums_two)]
        return (grad_act, sums_out[0], *expert_out, *sums_out[1:])

    return jax.shard_map(body, mesh=mesh, in_specs=(tok_spec, tok_spec, route_spec, route_spec, repl_spec, exp_spec, exp_spec, exp_spec, repl_spec, repl_spec, repl_spec), out_specs=(tok_spec, repl_spec, exp_spec, exp_spec, exp_spec, repl_spec, repl_spec, repl_spec), check_vma=False)
```

```python
import functools

import jax
import jax.numpy as jnp
from jax import lax
from jax.experimental import pallas as pl
from jax.experimental.pallas import tpu as pltpu
from jax.sharding import PartitionSpec as P


ALL_AXES = ("ep", "dp")
MESH = pl.DeviceIdType.MESH
STEPS = 2
ORDER = (0, 7, 3, 4, 5, 2, 1, 6)
ORDER_CODE = sum(mask * 8**step for step, mask in enumerate(ORDER))
AT_ONCE = (1, 2, 4, 6)
RELEASED = ((1, 3), (2, 5), (4, 7))
EARLY = (1, 2, 4)


def contract_rows(left, right):
    return lax.dot_general(left, right, (((0,), (0,)), ((), ())), preferred_element_type=jnp.float32)


def contract_cols(left, right):
    return lax.dot_general(left, right, (((1,), (1,)), ((), ())), preferred_element_type=jnp.float32)


def dot32(left, right):
    return jnp.dot(left, right, preferred_element_type=jnp.float32)


class Geometry:
    def __init__(self, ep, dp):
        self.ep, self.dp = ep, dp
        self.chips = (ep // 2) * (dp // 2)
        z, j = lax.axis_index("ep"), lax.axis_index("dp")
        self.core = j % 2
        self.local = j // 2
        self.base = (z // (ep // 2)) * (ep // 2)
        self.chip = (z % (ep // 2)) * (dp // 2) + j // 2
        self.me = 2 * self.chip + self.core
        self.sibling = (z, (j // 2) * 2 + 1 - self.core)
        self.partner = ((z + ep // 2) % ep, j)

    def member(self, index):
        return (self.base + index // self.dp, index % self.dp)

    def across(self, mask):
        total = 0
        for bit in (1, 2, 4):
            total += (self.chip // bit + mask // bit) % 2 * bit
        return total

    def at_step(self, step):
        power = (1 + 7 * (step % 2)) * (1 + 63 * (step // 2 % 2)) * (1 + 4095 * (step // 4))
        return self.across(ORDER_CODE // power % 8)

    def entry_barrier(self):
        barrier = pltpu.get_barrier_semaphore()

        @pl.loop(1, self.chips)
        def _(mask):
            for core in range(2):
                pl.semaphore_signal(barrier, inc=1, device_id=self.member(2 * self.across(mask) + core), device_id_type=MESH)

        for device in (self.sibling, self.partner):
            pl.semaphore_signal(barrier, inc=1, device_id=device, device_id_type=MESH)
        pl.semaphore_wait(barrier, 2 * self.chips)


class Outbound:
    def __init__(self, geo, send, recv, send_sem, recv_sem):
        self.geo, self.send, self.recv, self.send_sem, self.recv_sem = geo, send, recv, send_sem, recv_sem

    def copy(self, step, core):
        geo = self.geo
        index = 2 * geo.at_step(step) + core
        return pltpu.make_async_remote_copy(src_ref=self.send.at[index], dst_ref=self.recv.at[step, geo.core], send_sem=self.send_sem.at[step, core], recv_sem=self.recv_sem.at[step, geo.core], device_id=geo.member(index), device_id_type=MESH)

    def start(self):
        geo = self.geo
        pltpu.make_async_copy(self.send.at[geo.me], self.recv.at[0, geo.core], self.recv_sem.at[0, geo.core]).start()
        self.copy(0, 1 - geo.core).start()
        for step in AT_ONCE:
            self.issue(step)

    def issue(self, step):
        for core in range(2):
            self.copy(step, core).start()

    def arrive(self, step):
        for core in range(2):
            pltpu.make_async_copy(self.send.at[0], self.recv.at[step, core], self.recv_sem.at[step, core]).wait()
        for trigger, later in RELEASED:
            if isinstance(step, int):
                if step == trigger:
                    self.issue(later)
            else:
                pl.when(step == trigger)(functools.partial(self.issue, later))

    def wait_sends(self):
        self.copy(0, 1 - self.geo.core).wait_send()

        @pl.loop(1, self.geo.chips)
        def _(step):
            for core in range(2):
                self.copy(step, core).wait_send()


class Return:
    def __init__(self, geo, rows, back, send_sem, recv_sem):
        self.geo, self.rows, self.back, self.send_sem, self.recv_sem = geo, rows, back, send_sem, recv_sem

    def copy(self, step, core):
        geo = self.geo
        return pltpu.make_async_remote_copy(src_ref=self.rows.at[step, core], dst_ref=self.back.at[geo.me], send_sem=self.send_sem.at[step, core], recv_sem=self.recv_sem.at[geo.me], device_id=geo.member(2 * geo.at_step(step) + core), device_id_type=MESH)

    def start(self, step):
        geo = self.geo

        @pl.when(step == 0)
        def _():
            pltpu.make_async_copy(self.rows.at[0, geo.core], self.back.at[geo.me], self.recv_sem.at[geo.me]).start()
            self.copy(0, 1 - geo.core).start()

        @pl.when(step > 0)
        def _():
            for core in range(2):
                self.copy(step, core).start()

    def wait_all(self):
        geo = self.geo
        self.copy(0, 1 - geo.core).wait_send()

        @pl.loop(1, geo.chips)
        def _(step):
            for core in range(2):
                self.copy(step, core).wait_send()

        @pl.loop(0, 2 * geo.chips)
        def _(index):
            pltpu.make_async_copy(self.rows.at[0, 0], self.back.at[index], self.recv_sem.at[index]).wait()


def half_rows(rows, core):
    return pl.ds(pl.multiple_of(core * (rows // 2), 8), rows // 2)


class WeightSwap:
    def __init__(self, geo, layer, own, foreign, sems):
        self.geo, self.layer, self.own, self.foreign, self.sems = geo, layer, own, foreign, sems

    def over(self, which):
        geo = self.geo
        rows = half_rows(self.foreign[which].shape[0], geo.core)
        return pltpu.make_async_remote_copy(src_ref=self.own[which].at[self.layer, geo.local, rows], dst_ref=self.foreign[which].at[rows], send_sem=self.sems.at[0, which], recv_sem=self.sems.at[1, which], device_id=geo.partner, device_id_type=MESH)

    def across(self, which):
        geo = self.geo
        rows = self.foreign[which].at[half_rows(self.foreign[which].shape[0], geo.core)]
        return pltpu.make_async_remote_copy(src_ref=rows, dst_ref=rows, send_sem=self.sems.at[2, which], recv_sem=self.sems.at[3, which], device_id=geo.sibling, device_id_type=MESH)

    def start(self):
        for which in range(3):
            self.over(which).start()

    def pass_on(self):
        for which in range(3):
            self.over(which).wait()
            self.across(which).start()

    def finish(self):
        for which in range(3):
            self.across(which).wait()


def silu(value):
    return value * jax.nn.sigmoid(value)


def forward_kernel(ep, dp, send, mixed, *refs):
    refs = list(refs)

    def take(count):
        got = refs[:count]
        del refs[:count]
        return got

    experts, ws, got = take(3), take(3), take(3)
    recv_out, back, shared = take(3)
    keep_out, next_out = take(3), take(3)
    recv, outs = take(2)
    shared_w, own_w, foreign_w = take(3), take(3), take(3)
    go_sem, get_sem, ret_sem, res_sem, swap_sem, pass_sem, load_sem, save_sem = refs
    geo = Geometry(ep, dp)
    geo.entry_barrier()
    outbound = [Outbound(geo, send.at[part], recv.at[part], go_sem.at[part], get_sem.at[part]) for part in range(2)]
    returns = [Return(geo, outs.at[part], back.at[part], ret_sem.at[part], res_sem.at[part]) for part in range(2)]
    swap = WeightSwap(geo, 1, experts, next_out, swap_sem)
    outbound[0].start()
    loads = []
    passes = []
    for which in range(3):
        mine = half_rows(foreign_w[which].shape[0], geo.core)
        loads.append(pltpu.make_async_copy(ws[which].at[0], shared_w[which], load_sem.at[0, which]))
        loads.append(pltpu.make_async_copy(experts[which].at[0, geo.local], own_w[which], load_sem.at[1, which]))
        loads.append(pltpu.make_async_copy(got[which], foreign_w[which].at[mine], load_sem.at[2, which]))
        passes.append(pltpu.make_async_remote_copy(src_ref=got[which], dst_ref=foreign_w[which].at[mine], send_sem=pass_sem.at[0, which], recv_sem=pass_sem.at[1, which], device_id=geo.sibling, device_id_type=MESH))
    for copy in loads + passes:
        copy.start()
    outbound[1].start()
    swap.start()

    tile = 2 * STEPS * recv.shape[3]

    def ffn(rows, w_one, w_three, w_two):
        a_one = dot32(rows, w_one[...])
        a_three = dot32(rows, w_three[...])
        hidden = (silu(a_one) * a_three).astype(jnp.bfloat16)
        return dot32(hidden, w_two[...])

    for copy in loads + passes:
        copy.wait()

    @pl.loop(0, mixed.shape[0] // tile)
    def _(t):
        at = pl.ds(pl.multiple_of(t * tile, tile), tile)
        shared[at, :] = ffn(mixed[at, :], *shared_w)

    keeps = [pltpu.make_async_copy(src, dst, load_sem.at[0, which]) for which, (src, dst) in enumerate(zip(foreign_w, keep_out))]
    for keep in keeps:
        keep.start()
    width = mixed.shape[1]
    for part, weights in enumerate((own_w, foreign_w)):

        @pl.loop(0, geo.chips // STEPS)
        def _(t):
            steps = pl.ds(t * STEPS, STEPS)
            for step in range(STEPS):
                outbound[part].arrive(t * STEPS + step)
            pltpu.make_async_copy(recv.at[part, steps], recv_out.at[part, steps], save_sem.at[part, t]).start()
            rows = recv[part, steps].reshape(tile, width)
            outs[part, steps] = ffn(rows, *weights).astype(jnp.bfloat16).reshape(STEPS, 2, tile // (2 * STEPS), width)

            @pl.when(t > 0)
            def _():
                for step in range(STEPS):
                    returns[part].start((t - 1) * STEPS + step)

        for step in range(STEPS):
            returns[part].start(geo.chips - STEPS + step)
    swap.pass_on()
    for part in range(2):
        outbound[part].wait_sends()
        returns[part].wait_all()

        @pl.loop(0, geo.chips // STEPS)
        def _(t):
            steps = pl.ds(t * STEPS, STEPS)
            pltpu.make_async_copy(recv.at[part, steps], recv_out.at[part, steps], save_sem.at[part, t]).wait()

    for keep in keeps:
        keep.wait()
    swap.finish()


def forward_exchange(mesh, send, mixed, experts, shared, got):
    ep, dp = mesh.shape["ep"], mesh.shape["dp"]
    members, block, width = send.shape[1:]
    tokens = mixed.shape[0]
    bf16, f32 = jnp.bfloat16, jnp.float32
    shapes = [w.shape[2:] for w in experts]
    hidden = shapes[0][1]
    chips = members // 2
    anywhere = pl.BlockSpec(memory_space=pl.ANY)
    inside = pl.BlockSpec(memory_space=pltpu.VMEM)
    flops = 2 * 3 * width * hidden * (2 * members * block + tokens)
    expert = [jax.ShapeDtypeStruct(s, bf16) for s in shapes]
    dma = pltpu.SemaphoreType.DMA
    return pl.pallas_call(
        functools.partial(forward_kernel, ep, dp),
        name="forward_exchange",
        out_shape=[jax.ShapeDtypeStruct((2, chips, 2, block, width), bf16), jax.ShapeDtypeStruct((2, members, block, width), bf16), jax.ShapeDtypeStruct((tokens, width), f32)] + expert + expert,
        in_specs=[anywhere, inside] + [anywhere] * 9,
        out_specs=[anywhere, anywhere, inside] + [anywhere] * 6,
        scratch_shapes=[pltpu.VMEM((2, chips, 2, block, width), bf16) for _ in range(2)]
        + [pltpu.VMEM(s, bf16) for _ in range(3) for s in shapes]
        + [dma((2, chips, 2)), dma((2, chips, 2)), dma((2, chips, 2)), dma((2, members)), dma((4, 3)), dma((2, 3)), dma((3, 3)), dma((2, chips // STEPS))],
        compiler_params=pltpu.CompilerParams(collective_id=0, has_side_effects=True, vmem_limit_bytes=60 * 2**20),
        cost_estimate=pl.CostEstimate(flops=flops, bytes_accessed=40 * 2**20, transcendentals=0),
    )(send, mixed, *experts, *shared, *got)


class PairSum:
    def __init__(self, geo, stages, theirs, sems, expert):
        self.geo, self.stages, self.theirs, self.sems, self.expert = geo, stages, theirs, sems, expert

    def mine(self, which):
        return self.stages[which].at[self.expert, half_rows(self.stages[which].shape[1], self.geo.core)]

    def copy(self, which):
        geo = self.geo
        return pltpu.make_async_remote_copy(src_ref=self.stages[which].at[self.expert, half_rows(self.stages[which].shape[1], 1 - geo.core)], dst_ref=self.theirs[which].at[self.expert], send_sem=self.sems.at[0, self.expert, which], recv_sem=self.sems.at[1, self.expert, which], device_id=geo.sibling, device_id_type=MESH)

    def start(self):
        for which in range(3):
            self.copy(which).start()

    def finish(self):
        for which in range(3):
            self.copy(which).wait()
            mine = self.mine(which)
            mine[...] = (mine[...].astype(jnp.float32) + self.theirs[which][self.expert].astype(jnp.float32)).astype(jnp.bfloat16)


def backward_kernel(ep, dp, layer, *refs):
    refs = list(refs)

    def take(count):
        got = refs[:count]
        del refs[:count]
        return got

    held, send, mixed, grad_y = take(4)
    own_w, foreign_w, shared_w = take(3), take(3), take(3)
    back, shared_dx, recv = take(3)
    shared_out, own_out = take(3), take(3)
    x_buf, g_buf, dx_rows, dx_buf = take(4)
    weights, acc, stages, theirs, partner_in = take(3), take(3), take(3), take(3), take(3)
    go_sem, get_sem, ret_sem, res_sem, partner_sem, load_sem, x_sem, g_sem, dx_sem, pair_sem = refs

    geo = Geometry(ep, dp)
    geo.entry_barrier()
    tile = 2 * send.shape[2]
    width = mixed.shape[1]
    per_set = mixed.shape[0] // tile
    total = 3 * per_set
    outbound = [Outbound(geo, send.at[part], recv.at[part], go_sem.at[part], get_sem.at[part]) for part in range(2)]
    returns = [Return(geo, dx_rows.at[part], back.at[part], ret_sem.at[part], res_sem.at[part]) for part in range(2)]
    pairs = [PairSum(geo, stages, theirs, pair_sem, expert) for expert in range(2)]
    outbound[1].start()
    loads = []
    for which in range(3):
        loads.append(pltpu.make_async_copy(shared_w[which].at[layer], weights[which].at[2], load_sem.at[2, which]))
        loads.append(pltpu.make_async_copy(own_w[which].at[layer, geo.local], weights[which].at[0], load_sem.at[0, which]))
        loads.append(pltpu.make_async_copy(foreign_w[which], weights[which].at[1], load_sem.at[1, which]))
    for load in loads:
        load.start()
    outbound[0].start()
    moved, moved_sem, kept, kept_sem = (x_buf, x_sem, g_buf, g_sem) if layer else (g_buf, g_sem, x_buf, x_sem)

    def held_block(part, step, core):
        if layer:
            return held.at[2 * geo.at_step(step) + core, part]
        return held.at[part, step, core]

    def fetch(i, slot):
        @pl.when(i < per_set)
        def _():
            at = pl.ds(pl.multiple_of(i * tile, tile), tile)
            pltpu.make_async_copy(mixed.at[at], x_buf.at[slot], x_sem.at[slot]).start()
            pltpu.make_async_copy(grad_y.at[at], g_buf.at[slot], g_sem.at[slot]).start()

        for part in range(2):
            begin = (2 - part) * per_set

            @pl.when((i >= begin) & (i < begin + per_set))
            def _(part=part, begin=begin):
                step = i - begin
                early = (step == EARLY[0]) | (step == EARLY[1]) | (step == EARLY[2])
                pl.when(jnp.logical_not(early))(lambda: outbound[part].arrive(step))
                for core in range(2):
                    at = pl.ds(core * (tile // 2), tile // 2)
                    pltpu.make_async_copy(recv.at[part, step, core], moved.at[slot, at], moved_sem.at[slot]).start()
                    pltpu.make_async_copy(held_block(part, step, core), kept.at[slot, at], kept_sem.at[slot]).start()

    def store_shared(i):
        return pltpu.make_async_copy(dx_buf.at[i % 2], shared_dx.at[pl.ds(pl.multiple_of(i * tile, tile), tile)], dx_sem.at[i % 2])

    def partner_copies():
        return [pltpu.make_async_remote_copy(src_ref=pairs[1].mine(which), dst_ref=partner_in[which], send_sem=partner_sem.at[0, which], recv_sem=partner_sem.at[1, which], device_id=geo.partner, device_id_type=MESH) for which in range(3)]

    fetch(0, 0)
    for load in loads:
        load.wait()

    @pl.loop(0, total)
    def _(i):
        slot = i % 2
        which_set = 2 - i // per_set
        for part, ahead in ((1, 3), (0, per_set + 4)):
            for n, step in enumerate(EARLY):
                pl.when(i == ahead + 2 * n)(functools.partial(outbound[part].arrive, step))
        fetch(i + 1, (i + 1) % 2)
        pltpu.make_async_copy(mixed.at[pl.ds(0, tile)], x_buf.at[slot], x_sem.at[slot]).wait()
        pltpu.make_async_copy(mixed.at[pl.ds(0, tile)], g_buf.at[slot], g_sem.at[slot]).wait()

        @pl.when(i % per_set == 0)
        def _():
            for a in acc:
                a[...] = jnp.zeros(a.shape, jnp.float32)

        x = x_buf[slot]
        g = g_buf[slot]
        w_one, w_three, w_two = [w.at[which_set] for w in weights]
        a_one = dot32(x, w_one[...])
        a_three = dot32(x, w_three[...])
        grad_hidden = contract_cols(g, w_two[...])
        sigma = jax.nn.sigmoid(a_one)
        gated = a_one * sigma
        hidden = (gated * a_three).astype(jnp.bfloat16)
        grad_one = (grad_hidden * a_three * (sigma * (1.0 + a_one * (1.0 - sigma)))).astype(jnp.bfloat16)
        grad_three = (grad_hidden * gated).astype(jnp.bfloat16)
        acc[0][...] += contract_rows(x, grad_one)
        acc[1][...] += contract_rows(x, grad_three)
        acc[2][...] += contract_rows(hidden, g)
        dx = contract_cols(grad_one, w_one[...]) + contract_cols(grad_three, w_three[...])

        @pl.when(i < per_set)
        def _():
            pl.when(i >= 2)(lambda: store_shared(i - 2).wait())
            dx_buf[slot] = dx
            store_shared(i).start()

        @pl.when(i == per_set - 1)
        def _():
            for a, out in zip(acc, shared_out):
                out[...] = a[...].astype(jnp.bfloat16)

        for part in range(2):
            begin = (2 - part) * per_set

            @pl.when((i >= begin) & (i < begin + per_set))
            def _(part=part, begin=begin):
                dx_rows[part, i - begin] = dx.astype(jnp.bfloat16).reshape(2, tile // 2, width)

            @pl.when((i > begin) & (i <= begin + per_set))
            def _(part=part, begin=begin):
                returns[part].start(i - 1 - begin)

            @pl.when(i == begin + per_set - 1)
            def _(part=part):
                for a, stage in zip(acc, stages):
                    stage[part] = a[...].astype(jnp.bfloat16)

        pl.when(i == 2 * per_set)(pairs[1].start)
        pl.when(i == 2 * per_set + 1)(pairs[1].finish)

        @pl.when(i == 2 * per_set + 2)
        def _():
            for copy in partner_copies():
                copy.start()

    returns[0].start(per_set - 1)
    pairs[0].start()
    pairs[0].finish()
    for which, copy in enumerate(partner_copies()):
        copy.wait()
        own_out[which][...] = (pairs[0].mine(which)[...].astype(jnp.float32) + partner_in[which][...].astype(jnp.float32)).astype(jnp.bfloat16)
    store_shared(per_set - 2).wait()
    store_shared(per_set - 1).wait()
    for part in range(2):
        outbound[part].wait_sends()
        returns[part].wait_all()


def backward_exchange(mesh, layer, held, send, mixed, grad_y, own, foreign, shared):
    ep, dp = mesh.shape["ep"], mesh.shape["dp"]
    members, block, width = send.shape[1:]
    chips = members // 2
    tokens = mixed.shape[0]
    tile = 2 * block
    bf16, f32 = jnp.bfloat16, jnp.float32
    anywhere = pl.BlockSpec(memory_space=pl.ANY)
    inside = pl.BlockSpec(memory_space=pltpu.VMEM)
    shapes = [w.shape for w in foreign]
    halves = [(s[0] // 2, s[1]) for s in shapes]
    like = jax.ShapeDtypeStruct
    by_step = like((2, chips, 2, block, width), bf16)
    outs = [like((2, members, block, width), bf16), like((tokens, width), f32), by_step] + [like(s, bf16) for s in shapes + halves]
    vmem = pltpu.VMEM
    scratch = [vmem((2, tile, width), bf16), vmem((2, tile, width), bf16), vmem(by_step.shape, bf16), vmem((2, tile, width), f32)]
    scratch += [vmem((3,) + s, bf16) for s in shapes] + [vmem(s, f32) for s in shapes] + [vmem((2,) + s, bf16) for s in shapes]
    scratch += [vmem((2,) + s, bf16) for s in halves] + [vmem(s, bf16) for s in halves]
    dma = pltpu.SemaphoreType.DMA
    scratch += [dma((2, chips, 2)), dma((2, chips, 2)), dma((2, chips, 2)), dma((2, members)), dma((2, 3)), dma((3, 3)), dma((2,)), dma((2,)), dma((2,)), dma((2, 2, 3))]
    operands = [held, send, mixed, grad_y, *own, *foreign, *shared]
    flops = 2 * 8 * width * shapes[0][1] * (2 * members * block + tokens)
    return pl.pallas_call(
        functools.partial(backward_kernel, ep, dp, layer),
        name="backward_second" if layer else "backward_first",
        out_shape=outs,
        in_specs=[anywhere] * len(operands),
        out_specs=[anywhere] * 3 + [inside] * 6,
        scratch_shapes=scratch,
        compiler_params=pltpu.CompilerParams(collective_id=1 + layer, has_side_effects=True, vmem_limit_bytes=63 * 2**20),
        cost_estimate=pl.CostEstimate(flops=flops, bytes_accessed=60 * 2**20, transcendentals=0),
    )(*operands)


def final_kernel(ep, dp, *refs):
    refs = list(refs)

    def take(count):
        got = refs[:count]
        del refs[:count]
        return got

    halves, parts = take(3), take(4)
    full, sums = take(3), take(4)
    first, mine, wide, piece, other, last = [take(4) for _ in range(6)]
    load_sem, pair_sem, wide_send, wide_recv, partner_sem, spread_send, spread_recv, cross_sem, gather_sem, local_sem, fold_sem = refs
    geo = Geometry(ep, dp)
    geo.entry_barrier()
    z, core = lax.axis_index("ep"), geo.core
    four, three = range(4), range(3)
    f32, bf16 = jnp.float32, jnp.bfloat16

    to_sibling = [pltpu.make_async_remote_copy(src_ref=parts[n].at[1 - core], dst_ref=first[n], send_sem=pair_sem.at[0, n], recv_sem=pair_sem.at[1, n], device_id=geo.sibling, device_id_type=MESH) for n in four]
    keep = [pltpu.make_async_copy(parts[n].at[core], mine[n], load_sem.at[n]) for n in four]
    for copy in to_sibling + keep:
        copy.start()

    def place(mask):
        return geo.across(mask) % (dp // 2)

    def hop(n, index, src, dst, mask):
        return pltpu.make_async_remote_copy(src_ref=src, dst_ref=dst, send_sem=gather_sem.at[0, n, index], recv_sem=gather_sem.at[1, n, index], device_id=(z, 2 * place(mask) + core), device_id_type=MESH)

    def direct(n, mask):
        return hop(n, mask - 1, halves[n], full[n].at[geo.local, core], mask)

    def relay(n, mask):
        rows = halves[n].shape[0] // 2
        block = full[n].at[place(3 - mask), core, pl.ds((mask - 1) * rows, rows)]
        return hop(n, mask + 1, block, block, mask)

    def fold(n, mask):
        block = full[n].at[place(mask), core]
        return pltpu.make_async_remote_copy(src_ref=halves[n] if mask == 0 else block, dst_ref=block, send_sem=fold_sem.at[0, n, mask], recv_sem=fold_sem.at[1, n, mask], device_id=geo.sibling, device_id_type=MESH)

    local = [pltpu.make_async_copy(halves[n], full[n].at[geo.local, core], local_sem.at[n]) for n in three]

    def gather(n):
        for mask in (1, 2):
            direct(n, mask).start()
        fold(n, 0).start()
        local[n].start()

    def forward(n):
        for mask in (1, 2):
            direct(n, mask).wait()
        for mask in (1, 2):
            relay(n, mask).start()
            fold(n, mask).start()

    gather(2)
    for n in four:
        to_sibling[n].wait()
        keep[n].wait()
        mine[n][...] = (mine[n][...].astype(f32) + first[n][...].astype(f32)).astype(bf16)

    def widen(n, mask):
        to = geo.across(mask)
        return pltpu.make_async_remote_copy(src_ref=mine[n].at[to], dst_ref=wide[n].at[mask], send_sem=wide_send.at[n, mask], recv_sem=wide_recv.at[n, mask], device_id=geo.member(2 * to + core), device_id_type=MESH)

    for n in four:
        for mask in ORDER[1:]:
            widen(n, mask).start()
    gather(0)
    for n in four:
        for mask in ORDER[1:]:
            widen(n, mask).wait()
        total = mine[n][geo.chip].astype(f32)
        for mask in ORDER[1:]:
            total += wide[n][mask].astype(f32)
        piece[n][...] = total.astype(bf16)

    def swap(n):
        return pltpu.make_async_remote_copy(src_ref=piece[n], dst_ref=other[n], send_sem=partner_sem.at[0, n], recv_sem=partner_sem.at[1, n], device_id=geo.partner, device_id_type=MESH)

    for n in four:
        swap(n).start()
    forward(2)
    for n in four:
        swap(n).wait()
        last[n][...] = (piece[n][...].astype(f32) + other[n][...].astype(f32)).astype(bf16)

    def spread(n, mask):
        return pltpu.make_async_remote_copy(src_ref=last[n], dst_ref=sums[n].at[core, geo.chip], send_sem=spread_send.at[n, mask], recv_sem=spread_recv.at[n, mask], device_id=geo.member(2 * geo.across(mask) + core), device_id_type=MESH)

    own = [pltpu.make_async_copy(last[n], sums[n].at[core, geo.chip], load_sem.at[n]) for n in four]
    for n in four:
        own[n].start()
        for mask in ORDER[1:]:
            spread(n, mask).start()
    gather(1)
    forward(0)

    def cross(n):
        return pltpu.make_async_remote_copy(src_ref=sums[n].at[core], dst_ref=sums[n].at[core], send_sem=cross_sem.at[0, n], recv_sem=cross_sem.at[1, n], device_id=geo.sibling, device_id_type=MESH)

    for n in four:
        own[n].wait()
        for mask in ORDER[1:]:
            spread(n, mask).wait()
        cross(n).start()
    forward(1)
    for n in (2, 0, 1):
        for mask in (1, 2):
            relay(n, mask).wait()
        fold(n, 3).start()
    for n in three:
        local[n].wait()
        for mask in range(4):
            fold(n, mask).wait()
    for n in four:
        cross(n).wait()


def final_exchange(mesh, halves, parts):
    ep, dp = mesh.shape["ep"], mesh.shape["dp"]
    chips, plane = ep * dp // 4, dp // 2
    bf16 = jnp.bfloat16
    anywhere = pl.BlockSpec(memory_space=pl.ANY)
    like = jax.ShapeDtypeStruct
    cut = [part.reshape(2, chips, part.shape[0] // (2 * chips), part.shape[1]) for part in parts]
    piece = [c.shape[2:] for c in cut]
    vmem, dma = pltpu.VMEM, pltpu.SemaphoreType.DMA
    scratch = [vmem((chips,) + s, bf16) for _ in range(3) for s in piece] + [vmem(s, bf16) for _ in range(3) for s in piece]
    scratch += [dma((4,)), dma((2, 4)), dma((4, chips)), dma((4, chips)), dma((2, 4)), dma((4, chips)), dma((4, chips)), dma((2, 4)), dma((2, 3, 4)), dma((3,)), dma((2, 3, plane))]
    outs = pl.pallas_call(
        functools.partial(final_kernel, ep, dp),
        name="final_exchange",
        out_shape=[like((plane, 2) + h.shape, bf16) for h in halves] + [like(c.shape, bf16) for c in cut],
        in_specs=[anywhere] * 7,
        out_specs=[anywhere] * 7,
        scratch_shapes=scratch,
        compiler_params=pltpu.CompilerParams(collective_id=3, has_side_effects=True, vmem_limit_bytes=40 * 2**20),
        cost_estimate=pl.CostEstimate(flops=10**10, bytes_accessed=30 * 2**20, transcendentals=0),
    )(*halves, *cut)
    full = [out.reshape(plane, 2 * out.shape[2], out.shape[3]) for out in outs[:3]]
    return full, [out.reshape(part.shape) for out, part in zip(outs[3:], parts)]


def take_rows(source, index):
    return jnp.take(source, index, axis=0, mode="clip")


def slot_owners(slot_of_token, slots):
    tokens = slot_of_token.shape[1]
    fine = 64
    token = jnp.arange(tokens, dtype=jnp.int32)
    coarse = (slot_of_token[:, :, None] // fine == jnp.arange(slots // fine, dtype=jnp.int32)).astype(jnp.bfloat16)
    value = jnp.stack([token // 256, token % 256, jnp.ones_like(token)], axis=1).astype(jnp.bfloat16)
    within = (slot_of_token[:, :, None] % fine == jnp.arange(fine, dtype=jnp.int32)).astype(jnp.bfloat16)
    spread = (value[None, :, :, None] * within[:, :, None, :]).reshape(slot_of_token.shape[0], tokens, 3 * fine)
    found = jnp.einsum("lta,ltb->lab", coarse, spread, preferred_element_type=jnp.float32).astype(jnp.int32)
    high, low, used = found[:, :, :fine], found[:, :, fine:2 * fine], found[:, :, 2 * fine:]
    return (high * 256 + low + (1 - used) * tokens).reshape(slot_of_token.shape[0], slots)


def solution(mesh):
    tok_spec = P(ALL_AXES, None)
    route_spec = P(None, ALL_AXES, None)
    exp_spec = P(None, "ep", None, None)
    repl_spec = P(None, None, None)
    ep, dp = mesh.shape["ep"], mesh.shape["dp"]
    members = ep * dp // 2
    to_partner = [(d, (d + members) % (2 * members)) for d in range(2 * members)]
    groups = [[side * members + m for m in range(members)] for side in range(2)]

    def body(act_in, grad_out, slot_ids, gate_vals, w_dense, w_gate, w_up, w_down, ws_gate, ws_up, ws_down):
        tokens, width = act_in.shape
        slots = 2 * tokens
        block = tokens // members
        experts = (w_gate, w_up, w_down)
        shared = (ws_gate, ws_up, ws_down)
        core, local = lax.axis_index("dp") % 2, lax.axis_index("dp") // 2

        got = []
        for w in experts:
            rows, columns = w.shape[2] // 2, w.shape[3]
            mine = lax.dynamic_slice(w, (0, local, core * rows, 0), (1, 1, rows, columns)).reshape(rows, columns)
            got.append(lax.ppermute(mine, ALL_AXES, to_partner))

        side = lax.axis_index("ep") // (ep // 2)
        turned = (slot_ids.reshape(2, tokens) + side * tokens) % slots
        owner = slot_owners(turned, slots).reshape(2, 2, members, block)

        def extended(rows):
            return jnp.pad(rows, ((0, 8), (0, 0)))

        def to_slots(layer, rows):
            return take_rows(extended(rows), owner[layer].reshape(-1)).reshape(2, members, block, width)

        def from_slots(layer, back):
            return take_rows(back.reshape(slots, width), turned[layer]).astype(jnp.float32)

        def mix(act, layer):
            return (act.astype(jnp.float32) + dot32(act, w_dense[layer])).astype(jnp.bfloat16)

        def gated(grad, layer):
            return (gate_vals[layer] * grad.astype(jnp.float32)).astype(jnp.bfloat16)

        by_member = owner[1].transpose(1, 0, 2).reshape(-1)
        grads_two = take_rows(extended(gated(grad_out, 1)), by_member).reshape(members, 2, block, width)
        mixed_one = mix(act_in, 0)
        sent_one = to_slots(0, mixed_one)
        sent_one, grads_two = lax.optimization_barrier((sent_one, grads_two))
        recv, back, shared_y, *foreign = forward_exchange(mesh, sent_one, mixed_one, experts, shared, got)
        back, grads_two = lax.optimization_barrier((back, grads_two))
        grads_two = lax.all_to_all(grads_two, ALL_AXES, 0, 0, axis_index_groups=groups)
        routed = from_slots(0, back)
        act_two = (mixed_one.astype(jnp.float32) + gate_vals[0] * routed + shared_y).astype(jnp.bfloat16)
        mixed_two = mix(act_two, 1)

        def finish(layer, act, grad_y, back, shared_dx):
            routed = from_slots(layer, back)
            grad_mixed = (grad_y.astype(jnp.float32) + routed + shared_dx).astype(jnp.bfloat16)
            g_dense = contract_rows(act, grad_mixed).astype(jnp.bfloat16)
            return (grad_mixed.astype(jnp.float32) + contract_cols(grad_mixed, w_dense[layer])).astype(jnp.bfloat16), g_dense

        def gather(half):
            return lax.all_gather(half, "dp", axis=0, tiled=True).reshape((dp // 2, 2 * half.shape[0], half.shape[1]))

        out = backward_exchange(mesh, 1, grads_two, to_slots(1, mixed_two), mixed_two, grad_out, experts, foreign[3:], shared)
        shared_two, own_two = out[3:6], out[6:9]
        experts_two = [gather(half) for half in own_two]
        grad_one, dense_two = finish(1, act_two, grad_out, out[0], out[1])
        sums_two = [lax.psum(part, ALL_AXES) for part in (dense_two, *shared_two)]

        out = backward_exchange(mesh, 0, recv, to_slots(0, gated(grad_one, 0)), mixed_one, grad_one, experts, foreign[:3], shared)
        shared_one, own_one = out[3:6], out[6:9]
        grad_act, dense_one = finish(0, act_in, grad_one, out[0], out[1])
        experts_one, sums_one = final_exchange(mesh, own_one, [dense_one, *shared_one])

        expert_out = [jnp.stack(pair) for pair in zip(experts_one, experts_two)]
        sums_out = [jnp.stack(pair) for pair in zip(sums_one, sums_two)]
        return (grad_act, sums_out[0], *expert_out, *sums_out[1:])

    return jax.shard_map(body, mesh=mesh, in_specs=(tok_spec, tok_spec, route_spec, route_spec, repl_spec, exp_spec, exp_spec, exp_spec, repl_spec, repl_spec, repl_spec), out_specs=(tok_spec, repl_spec, exp_spec, exp_spec, exp_spec, repl_spec, repl_spec, repl_spec), check_vma=False)
```

```python
import functools

import jax
import jax.numpy as jnp
from jax import lax
from jax.experimental import pallas as pl
from jax.experimental.pallas import tpu as pltpu
from jax.sharding import PartitionSpec as P


ALL_AXES = ("ep", "dp")
MESH = pl.DeviceIdType.MESH
STEPS = 2
ORDER = (0, 7, 3, 4, 5, 2, 1, 6)
ORDER_CODE = sum(mask * 8**step for step, mask in enumerate(ORDER))
AT_ONCE = (1, 2, 4, 6)
RELEASED = ((1, 3), (2, 5), (4, 7))
EARLY = (1, 2, 4)
PACK_CODE = sum(step * 8**n for n, step in enumerate((1, 2, 4, 6, 0, 3, 5, 7)))


def contract_rows(left, right):
    return lax.dot_general(left, right, (((0,), (0,)), ((), ())), preferred_element_type=jnp.float32)


def contract_cols(left, right):
    return lax.dot_general(left, right, (((1,), (1,)), ((), ())), preferred_element_type=jnp.float32)


def dot32(left, right):
    return jnp.dot(left, right, preferred_element_type=jnp.float32)


class Geometry:
    def __init__(self, ep, dp):
        self.ep, self.dp = ep, dp
        self.chips = (ep // 2) * (dp // 2)
        z, j = lax.axis_index("ep"), lax.axis_index("dp")
        self.core = j % 2
        self.local = j // 2
        self.base = (z // (ep // 2)) * (ep // 2)
        self.chip = (z % (ep // 2)) * (dp // 2) + j // 2
        self.me = 2 * self.chip + self.core
        self.sibling = (z, (j // 2) * 2 + 1 - self.core)
        self.partner = ((z + ep // 2) % ep, j)

    def member(self, index):
        return (self.base + index // self.dp, index % self.dp)

    def across(self, mask):
        total = 0
        for bit in (1, 2, 4):
            total += (self.chip // bit + mask // bit) % 2 * bit
        return total

    def at_step(self, step):
        power = (1 + 7 * (step % 2)) * (1 + 63 * (step // 2 % 2)) * (1 + 4095 * (step // 4))
        return self.across(ORDER_CODE // power % 8)

    def entry_barrier(self):
        barrier = pltpu.get_barrier_semaphore()

        @pl.loop(1, self.chips)
        def _(mask):
            for core in range(2):
                pl.semaphore_signal(barrier, inc=1, device_id=self.member(2 * self.across(mask) + core), device_id_type=MESH)

        for device in (self.sibling, self.partner):
            pl.semaphore_signal(barrier, inc=1, device_id=device, device_id_type=MESH)
        pl.semaphore_wait(barrier, 2 * self.chips)


class Outbound:
    def __init__(self, geo, part, send, recv, send_sem, recv_sem):
        self.geo, self.part = geo, part
        self.send, self.recv, self.send_sem, self.recv_sem = [ref.at[part] for ref in (send, recv, send_sem, recv_sem)]

    def copy(self, step, core):
        geo = self.geo
        index = 2 * geo.at_step(step) + core
        return pltpu.make_async_remote_copy(src_ref=self.send.at[index], dst_ref=self.recv.at[step, geo.core], send_sem=self.send_sem.at[step, core], recv_sem=self.recv_sem.at[step, geo.core], device_id=geo.member(index), device_id_type=MESH)

    def own(self):
        geo = self.geo
        return pltpu.make_async_copy(self.send.at[geo.me], self.recv.at[0, geo.core], self.recv_sem.at[0, geo.core])

    def pack(self, slots, rows):
        geo = self.geo
        tokens = rows.shape[0]
        block = self.send.shape[1]

        @pl.loop(0, geo.chips)
        def _(n):
            power = (1 + 7 * (n % 2)) * (1 + 63 * (n // 2 % 2)) * (1 + 4095 * (n // 4))
            chip = geo.at_step(PACK_CODE // power % 8)
            base = self.part * tokens + chip * 2 * block
            wanted = base + lax.broadcasted_iota(jnp.int32, (2 * block, tokens), 0)
            pick = (wanted == slots[...]).astype(jnp.float32).astype(jnp.bfloat16)
            self.send[pl.ds(2 * chip, 2)] = dot32(pick, rows[...]).astype(jnp.bfloat16).reshape(2, block, rows.shape[1])
            for when, step in enumerate(AT_ONCE):
                pl.when(n == when + 1)(functools.partial(self.issue, step))

        self.own().start()
        self.copy(0, 1 - geo.core).start()

    def issue(self, step):
        for core in range(2):
            self.copy(step, core).start()

    def arrive(self, step):
        for core in range(2):
            pltpu.make_async_copy(self.send.at[0], self.recv.at[step, core], self.recv_sem.at[step, core]).wait()
        for trigger, later in RELEASED:
            if isinstance(step, int):
                if step == trigger:
                    self.issue(later)
            else:
                pl.when(step == trigger)(functools.partial(self.issue, later))

    def wait_sends(self):
        self.copy(0, 1 - self.geo.core).wait_send()

        @pl.loop(1, self.geo.chips)
        def _(step):
            for core in range(2):
                self.copy(step, core).wait_send()


class Return:
    def __init__(self, geo, rows, back, send_sem, recv_sem):
        self.geo, self.rows, self.back, self.send_sem, self.recv_sem = geo, rows, back, send_sem, recv_sem

    def copy(self, step, core):
        geo = self.geo
        return pltpu.make_async_remote_copy(src_ref=self.rows.at[step, core], dst_ref=self.back.at[geo.me], send_sem=self.send_sem.at[step, core], recv_sem=self.recv_sem.at[geo.me], device_id=geo.member(2 * geo.at_step(step) + core), device_id_type=MESH)

    def start(self, step):
        geo = self.geo

        @pl.when(step == 0)
        def _():
            pltpu.make_async_copy(self.rows.at[0, geo.core], self.back.at[geo.me], self.recv_sem.at[geo.me]).start()
            self.copy(0, 1 - geo.core).start()

        @pl.when(step > 0)
        def _():
            for core in range(2):
                self.copy(step, core).start()

    def wait_all(self):
        geo = self.geo
        self.copy(0, 1 - geo.core).wait_send()

        @pl.loop(1, geo.chips)
        def _(step):
            for core in range(2):
                self.copy(step, core).wait_send()

        @pl.loop(0, 2 * geo.chips)
        def _(index):
            pltpu.make_async_copy(self.rows.at[0, 0], self.back.at[index], self.recv_sem.at[index]).wait()


def half_rows(rows, core):
    return pl.ds(pl.multiple_of(core * (rows // 2), 8), rows // 2)


class WeightSwap:
    def __init__(self, geo, layer, own, foreign, sems, which):
        self.geo, self.layer, self.own, self.foreign, self.sems, self.every = geo, layer, own, foreign, sems, which

    def over(self, which):
        geo = self.geo
        rows = half_rows(self.foreign[which].shape[0], geo.core)
        return pltpu.make_async_remote_copy(src_ref=self.own[which].at[self.layer, geo.local, rows], dst_ref=self.foreign[which].at[rows], send_sem=self.sems.at[0, which], recv_sem=self.sems.at[1, which], device_id=geo.partner, device_id_type=MESH)

    def across(self, which):
        geo = self.geo
        rows = self.foreign[which].at[half_rows(self.foreign[which].shape[0], geo.core)]
        return pltpu.make_async_remote_copy(src_ref=rows, dst_ref=rows, send_sem=self.sems.at[2, which], recv_sem=self.sems.at[3, which], device_id=geo.sibling, device_id_type=MESH)

    def start(self):
        for which in self.every:
            self.over(which).start()

    def pass_on(self):
        for which in self.every:
            self.over(which).wait()
            self.across(which).start()

    def finish(self):
        for which in self.every:
            self.across(which).wait()


def silu(value):
    return value * jax.nn.sigmoid(value)


def forward_kernel(ep, dp, slots, mixed, *refs):
    refs = list(refs)

    def take(count):
        got = refs[:count]
        del refs[:count]
        return got

    experts, ws, got = take(3), take(3), take(2)
    recv_out, back, shared = take(3)
    keep_out, next_out = take(3), take(3)
    send, recv, outs = take(3)
    shared_w, own_w, foreign_w = take(3), take(3), take(3)
    go_sem, get_sem, ret_sem, res_sem, swap_sem, down_sem, pass_sem, load_sem, save_sem = refs
    geo = Geometry(ep, dp)
    geo.entry_barrier()
    outbound = [Outbound(geo, part, send, recv, go_sem, get_sem) for part in range(2)]
    returns = [Return(geo, outs.at[part], back.at[part], ret_sem.at[part], res_sem.at[part]) for part in range(2)]
    swap = WeightSwap(geo, 1, experts, next_out, swap_sem, range(3))
    down = WeightSwap(geo, 0, experts, foreign_w, down_sem, (2,))
    loads = []
    passes = []
    for which in range(3):
        loads.append(pltpu.make_async_copy(ws[which].at[0], shared_w[which], load_sem.at[0, which]))
        loads.append(pltpu.make_async_copy(experts[which].at[0, geo.local], own_w[which], load_sem.at[1, which]))
    for which in range(2):
        mine = half_rows(foreign_w[which].shape[0], geo.core)
        loads.append(pltpu.make_async_copy(got[which], foreign_w[which].at[mine], load_sem.at[2, which]))
        passes.append(pltpu.make_async_remote_copy(src_ref=got[which], dst_ref=foreign_w[which].at[mine], send_sem=pass_sem.at[0, which], recv_sem=pass_sem.at[1, which], device_id=geo.sibling, device_id_type=MESH))
    down.start()
    for copy in loads + passes:
        copy.start()
    outbound[0].pack(slots, mixed)
    outbound[1].pack(slots, mixed)
    swap.start()

    tile = 2 * STEPS * recv.shape[3]

    def ffn(rows, w_one, w_three, w_two):
        a_one = dot32(rows, w_one[...])
        a_three = dot32(rows, w_three[...])
        hidden = (silu(a_one) * a_three).astype(jnp.bfloat16)
        return dot32(hidden, w_two[...])

    for copy in loads + passes:
        copy.wait()

    @pl.loop(0, mixed.shape[0] // tile)
    def _(t):
        at = pl.ds(pl.multiple_of(t * tile, tile), tile)
        shared[at, :] = ffn(mixed[at, :], *shared_w)

    width = mixed.shape[1]
    for part, weights in enumerate((own_w, foreign_w)):
        if part == 1:
            down.finish()
            keeps = [pltpu.make_async_copy(src, dst, load_sem.at[0, which]) for which, (src, dst) in enumerate(zip(foreign_w, keep_out))]
            for keep in keeps:
                keep.start()

        @pl.loop(0, geo.chips // STEPS)
        def _(t):
            steps = pl.ds(t * STEPS, STEPS)
            for step in range(STEPS):
                outbound[part].arrive(t * STEPS + step)
            pltpu.make_async_copy(recv.at[part, steps], recv_out.at[part, steps], save_sem.at[part, t]).start()
            rows = recv[part, steps].reshape(tile, width)
            outs[part, steps] = ffn(rows, *weights).astype(jnp.bfloat16).reshape(STEPS, 2, tile // (2 * STEPS), width)

            @pl.when(t > 0)
            def _():
                for step in range(STEPS):
                    returns[part].start((t - 1) * STEPS + step)

        for step in range(STEPS):
            returns[part].start(geo.chips - STEPS + step)
        if part == 0:
            down.pass_on()
    swap.pass_on()
    for part in range(2):
        outbound[part].wait_sends()
        returns[part].wait_all()

        @pl.loop(0, geo.chips // STEPS)
        def _(t):
            steps = pl.ds(t * STEPS, STEPS)
            pltpu.make_async_copy(recv.at[part, steps], recv_out.at[part, steps], save_sem.at[part, t]).wait()

    for keep in keeps:
        keep.wait()
    swap.finish()


def forward_exchange(mesh, slots, mixed, experts, shared, got):
    ep, dp = mesh.shape["ep"], mesh.shape["dp"]
    tokens, width = mixed.shape
    members = ep * dp // 2
    block = tokens // members
    bf16, f32 = jnp.bfloat16, jnp.float32
    shapes = [w.shape[2:] for w in experts]
    hidden = shapes[0][1]
    chips = members // 2
    anywhere = pl.BlockSpec(memory_space=pl.ANY)
    inside = pl.BlockSpec(memory_space=pltpu.VMEM)
    flops = 2 * 3 * width * hidden * (2 * members * block + tokens)
    expert = [jax.ShapeDtypeStruct(s, bf16) for s in shapes]
    dma = pltpu.SemaphoreType.DMA
    return pl.pallas_call(
        functools.partial(forward_kernel, ep, dp),
        name="forward_exchange",
        out_shape=[jax.ShapeDtypeStruct((2, chips, 2, block, width), bf16), jax.ShapeDtypeStruct((2, members, block, width), bf16), jax.ShapeDtypeStruct((tokens, width), f32)] + expert + expert,
        in_specs=[inside, inside] + [anywhere] * 8,
        out_specs=[anywhere, anywhere, inside] + [anywhere] * 6,
        scratch_shapes=[pltpu.VMEM((2, members, block, width), bf16)]
        + [pltpu.VMEM((2, chips, 2, block, width), bf16) for _ in range(2)]
        + [pltpu.VMEM(s, bf16) for _ in range(3) for s in shapes]
        + [dma((2, chips, 2)), dma((2, chips, 2)), dma((2, chips, 2)), dma((2, members)), dma((4, 3)), dma((4, 3)), dma((2, 3)), dma((3, 3)), dma((2, chips // STEPS))],
        compiler_params=pltpu.CompilerParams(collective_id=0, has_side_effects=True, vmem_limit_bytes=60 * 2**20),
        cost_estimate=pl.CostEstimate(flops=flops, bytes_accessed=40 * 2**20, transcendentals=0),
    )(slots, mixed, *experts, *shared, *got)


class PairSum:
    def __init__(self, geo, stages, theirs, sems, expert):
        self.geo, self.stages, self.theirs, self.sems, self.expert = geo, stages, theirs, sems, expert

    def mine(self, which):
        return self.stages[which].at[self.expert, half_rows(self.stages[which].shape[1], self.geo.core)]

    def copy(self, which):
        geo = self.geo
        return pltpu.make_async_remote_copy(src_ref=self.stages[which].at[self.expert, half_rows(self.stages[which].shape[1], 1 - geo.core)], dst_ref=self.theirs[which].at[self.expert], send_sem=self.sems.at[0, self.expert, which], recv_sem=self.sems.at[1, self.expert, which], device_id=geo.sibling, device_id_type=MESH)

    def start(self):
        for which in range(3):
            self.copy(which).start()

    def finish(self):
        for which in range(3):
            self.copy(which).wait()
            mine = self.mine(which)
            mine[...] = (mine[...].astype(jnp.float32) + self.theirs[which][self.expert].astype(jnp.float32)).astype(jnp.bfloat16)


def backward_kernel(ep, dp, layer, *refs):
    refs = list(refs)

    def take(count):
        got = refs[:count]
        del refs[:count]
        return got

    slots = take(1)[0]
    held = take(2 if layer else 1)
    rows_in, mixed, grad_y = take(3)
    own_w, foreign_w, shared_w = take(3), take(3), take(3)
    back, shared_dx, recv = take(3)
    shared_out, own_out = take(3), take(3)
    source, send, x_buf, g_buf, dx_rows, dx_buf = take(6)
    weights, acc, stages, theirs, partner_in = take(3), take(3), take(3), take(3), take(3)
    go_sem, get_sem, ret_sem, res_sem, partner_sem, load_sem, x_sem, g_sem, dx_sem, pair_sem = refs

    geo = Geometry(ep, dp)
    geo.entry_barrier()
    tile = 2 * send.shape[2]
    fill = pltpu.make_async_copy(rows_in, source, dx_sem.at[0])
    fill.start()
    width = mixed.shape[1]
    per_set = mixed.shape[0] // tile
    total = 3 * per_set
    outbound = [Outbound(geo, part, send, recv, go_sem, get_sem) for part in range(2)]
    returns = [Return(geo, dx_rows.at[part], back.at[part], ret_sem.at[part], res_sem.at[part]) for part in range(2)]
    pairs = [PairSum(geo, stages, theirs, pair_sem, expert) for expert in range(2)]
    loads = []
    for which in range(3):
        loads.append(pltpu.make_async_copy(shared_w[which].at[layer], weights[which].at[2], load_sem.at[2, which]))
        loads.append(pltpu.make_async_copy(own_w[which].at[layer, geo.local], weights[which].at[0], load_sem.at[0, which]))
        loads.append(pltpu.make_async_copy(foreign_w[which], weights[which].at[1], load_sem.at[1, which]))
    for load in loads:
        load.start()
    fill.wait()
    outbound[1].pack(slots, source)
    outbound[0].pack(slots, source)
    moved, moved_sem, kept, kept_sem = (x_buf, x_sem, g_buf, g_sem) if layer else (g_buf, g_sem, x_buf, x_sem)

    def held_block(part, step, core):
        if layer:
            return held[part].at[2 * geo.at_step(step) + core]
        return held[0].at[part, step, core]

    def fetch(i, slot):
        @pl.when(i < per_set)
        def _():
            at = pl.ds(pl.multiple_of(i * tile, tile), tile)
            pltpu.make_async_copy(mixed.at[at], x_buf.at[slot], x_sem.at[slot]).start()
            pltpu.make_async_copy(grad_y.at[at], g_buf.at[slot], g_sem.at[slot]).start()

        for part in range(2):
            begin = (2 - part) * per_set

            @pl.when((i >= begin) & (i < begin + per_set))
            def _(part=part, begin=begin):
                step = i - begin
                early = (step == EARLY[0]) | (step == EARLY[1]) | (step == EARLY[2])
                pl.when(jnp.logical_not(early))(lambda: outbound[part].arrive(step))
                for core in range(2):
                    at = pl.ds(core * (tile // 2), tile // 2)
                    pltpu.make_async_copy(recv.at[part, step, core], moved.at[slot, at], moved_sem.at[slot]).start()
                    pltpu.make_async_copy(held_block(part, step, core), kept.at[slot, at], kept_sem.at[slot]).start()

    def store_shared(i):
        return pltpu.make_async_copy(dx_buf.at[i % 2], shared_dx.at[pl.ds(pl.multiple_of(i * tile, tile), tile)], dx_sem.at[i % 2])

    def partner_copies():
        return [pltpu.make_async_remote_copy(src_ref=pairs[1].mine(which), dst_ref=partner_in[which], send_sem=partner_sem.at[0, which], recv_sem=partner_sem.at[1, which], device_id=geo.partner, device_id_type=MESH) for which in range(3)]

    fetch(0, 0)
    for load in loads:
        load.wait()

    @pl.loop(0, total)
    def _(i):
        slot = i % 2
        which_set = 2 - i // per_set
        for part, ahead in ((1, 3), (0, per_set + 4)):
            for n, step in enumerate(EARLY):
                pl.when(i == ahead + 2 * n)(functools.partial(outbound[part].arrive, step))
        fetch(i + 1, (i + 1) % 2)
        pltpu.make_async_copy(mixed.at[pl.ds(0, tile)], x_buf.at[slot], x_sem.at[slot]).wait()
        pltpu.make_async_copy(mixed.at[pl.ds(0, tile)], g_buf.at[slot], g_sem.at[slot]).wait()

        @pl.when(i % per_set == 0)
        def _():
            for a in acc:
                a[...] = jnp.zeros(a.shape, jnp.float32)

        x = x_buf[slot]
        g = g_buf[slot]
        w_one, w_three, w_two = [w.at[which_set] for w in weights]
        a_one = dot32(x, w_one[...])
        a_three = dot32(x, w_three[...])
        grad_hidden = contract_cols(g, w_two[...])
        sigma = jax.nn.sigmoid(a_one)
        gated = a_one * sigma
        hidden = (gated * a_three).astype(jnp.bfloat16)
        grad_one = (grad_hidden * a_three * (sigma * (1.0 + a_one * (1.0 - sigma)))).astype(jnp.bfloat16)
        grad_three = (grad_hidden * gated).astype(jnp.bfloat16)
        acc[0][...] += contract_rows(x, grad_one)
        acc[1][...] += contract_rows(x, grad_three)
        acc[2][...] += contract_rows(hidden, g)
        dx = contract_cols(grad_one, w_one[...]) + contract_cols(grad_three, w_three[...])

        @pl.when(i < per_set)
        def _():
            pl.when(i >= 2)(lambda: store_shared(i - 2).wait())
            dx_buf[slot] = dx
            store_shared(i).start()

        @pl.when(i == per_set - 1)
        def _():
            for a, out in zip(acc, shared_out):
                out[...] = a[...].astype(jnp.bfloat16)

        for part in range(2):
            begin = (2 - part) * per_set

            @pl.when((i >= begin) & (i < begin + per_set))
            def _(part=part, begin=begin):
                dx_rows[part, i - begin] = dx.astype(jnp.bfloat16).reshape(2, tile // 2, width)

            @pl.when((i > begin) & (i <= begin + per_set))
            def _(part=part, begin=begin):
                returns[part].start(i - 1 - begin)

            @pl.when(i == begin + per_set - 1)
            def _(part=part):
                for a, stage in zip(acc, stages):
                    stage[part] = a[...].astype(jnp.bfloat16)

        pl.when(i == 2 * per_set)(pairs[1].start)
        pl.when(i == 2 * per_set + 1)(pairs[1].finish)

        @pl.when(i == 2 * per_set + 2)
        def _():
            for copy in partner_copies():
                copy.start()

    returns[0].start(per_set - 1)
    pairs[0].start()
    pairs[0].finish()
    for which, copy in enumerate(partner_copies()):
        copy.wait()
        own_out[which][...] = (pairs[0].mine(which)[...].astype(jnp.float32) + partner_in[which][...].astype(jnp.float32)).astype(jnp.bfloat16)
    store_shared(per_set - 2).wait()
    store_shared(per_set - 1).wait()
    for part in range(2):
        outbound[part].wait_sends()
        returns[part].wait_all()


def backward_exchange(mesh, layer, slots, held, rows, mixed, grad_y, own, foreign, shared):
    ep, dp = mesh.shape["ep"], mesh.shape["dp"]
    tokens, width = mixed.shape
    members = ep * dp // 2
    block = tokens // members
    chips = members // 2
    tile = 2 * block
    bf16, f32 = jnp.bfloat16, jnp.float32
    anywhere = pl.BlockSpec(memory_space=pl.ANY)
    inside = pl.BlockSpec(memory_space=pltpu.VMEM)
    shapes = [w.shape for w in foreign]
    halves = [(s[0] // 2, s[1]) for s in shapes]
    like = jax.ShapeDtypeStruct
    by_step = like((2, chips, 2, block, width), bf16)
    outs = [like((2, members, block, width), bf16), like((tokens, width), f32), by_step] + [like(s, bf16) for s in shapes + halves]
    vmem = pltpu.VMEM
    scratch = [vmem((tokens, width), bf16), vmem((2, members, block, width), bf16), vmem((2, tile, width), bf16), vmem((2, tile, width), bf16), vmem(by_step.shape, bf16), vmem((2, tile, width), f32)]
    scratch += [vmem((3,) + s, bf16) for s in shapes] + [vmem(s, f32) for s in shapes] + [vmem((2,) + s, bf16) for s in shapes]
    scratch += [vmem((2,) + s, bf16) for s in halves] + [vmem(s, bf16) for s in halves]
    dma = pltpu.SemaphoreType.DMA
    scratch += [dma((2, chips, 2)), dma((2, chips, 2)), dma((2, chips, 2)), dma((2, members)), dma((2, 3)), dma((3, 3)), dma((2,)), dma((2,)), dma((2,)), dma((2, 2, 3))]
    operands = [slots, *held, rows, mixed, grad_y, *own, *foreign, *shared]
    flops = 2 * 8 * width * shapes[0][1] * (2 * members * block + tokens)
    return pl.pallas_call(
        functools.partial(backward_kernel, ep, dp, layer),
        name="backward_second" if layer else "backward_first",
        out_shape=outs,
        in_specs=[inside] + [anywhere] * (len(operands) - 1),
        out_specs=[anywhere] * 3 + [inside] * 6,
        scratch_shapes=scratch,
        compiler_params=pltpu.CompilerParams(collective_id=1 + layer, has_side_effects=True, vmem_limit_bytes=63 * 2**20),
        cost_estimate=pl.CostEstimate(flops=flops, bytes_accessed=60 * 2**20, transcendentals=0),
    )(*operands)


def final_kernel(ep, dp, *refs):
    refs = list(refs)

    def take(count):
        got = refs[:count]
        del refs[:count]
        return got

    halves, parts = take(3), take(4)
    full, sums = take(3), take(4)
    first, mine, wide, piece, other, last = [take(4) for _ in range(6)]
    load_sem, pair_sem, wide_send, wide_recv, partner_sem, spread_send, spread_recv, cross_sem, gather_sem, local_sem, fold_sem = refs
    geo = Geometry(ep, dp)
    geo.entry_barrier()
    z, core = lax.axis_index("ep"), geo.core
    four, three = range(4), range(3)
    f32, bf16 = jnp.float32, jnp.bfloat16

    to_sibling = [pltpu.make_async_remote_copy(src_ref=parts[n].at[1 - core], dst_ref=first[n], send_sem=pair_sem.at[0, n], recv_sem=pair_sem.at[1, n], device_id=geo.sibling, device_id_type=MESH) for n in four]
    keep = [pltpu.make_async_copy(parts[n].at[core], mine[n], load_sem.at[n]) for n in four]
    for copy in to_sibling + keep:
        copy.start()

    def place(mask):
        return geo.across(mask) % (dp // 2)

    def hop(n, index, src, dst, mask):
        return pltpu.make_async_remote_copy(src_ref=src, dst_ref=dst, send_sem=gather_sem.at[0, n, index], recv_sem=gather_sem.at[1, n, index], device_id=(z, 2 * place(mask) + core), device_id_type=MESH)

    def direct(n, mask):
        return hop(n, mask - 1, halves[n], full[n].at[geo.local, core], mask)

    def relay(n, mask):
        rows = halves[n].shape[0] // 2
        block = full[n].at[place(3 - mask), core, pl.ds((mask - 1) * rows, rows)]
        return hop(n, mask + 1, block, block, mask)

    def fold(n, mask):
        block = full[n].at[place(mask), core]
        return pltpu.make_async_remote_copy(src_ref=halves[n] if mask == 0 else block, dst_ref=block, send_sem=fold_sem.at[0, n, mask], recv_sem=fold_sem.at[1, n, mask], device_id=geo.sibling, device_id_type=MESH)

    local = [pltpu.make_async_copy(halves[n], full[n].at[geo.local, core], local_sem.at[n]) for n in three]

    def gather(n):
        for mask in (1, 2):
            direct(n, mask).start()
        fold(n, 0).start()
        local[n].start()

    def forward(n):
        for mask in (1, 2):
            direct(n, mask).wait()
        for mask in (1, 2):
            relay(n, mask).start()
            fold(n, mask).start()

    gather(2)
    for n in four:
        to_sibling[n].wait()
        keep[n].wait()
        mine[n][...] = (mine[n][...].astype(f32) + first[n][...].astype(f32)).astype(bf16)

    def widen(n, mask):
        to = geo.across(mask)
        return pltpu.make_async_remote_copy(src_ref=mine[n].at[to], dst_ref=wide[n].at[mask], send_sem=wide_send.at[n, mask], recv_sem=wide_recv.at[n, mask], device_id=geo.member(2 * to + core), device_id_type=MESH)

    for n in four:
        for mask in ORDER[1:]:
            widen(n, mask).start()
    gather(0)
    for n in four:
        for mask in ORDER[1:]:
            widen(n, mask).wait()
        total = mine[n][geo.chip].astype(f32)
        for mask in ORDER[1:]:
            total += wide[n][mask].astype(f32)
        piece[n][...] = total.astype(bf16)

    def swap(n):
        return pltpu.make_async_remote_copy(src_ref=piece[n], dst_ref=other[n], send_sem=partner_sem.at[0, n], recv_sem=partner_sem.at[1, n], device_id=geo.partner, device_id_type=MESH)

    for n in four:
        swap(n).start()
    forward(2)
    for n in four:
        swap(n).wait()
        last[n][...] = (piece[n][...].astype(f32) + other[n][...].astype(f32)).astype(bf16)

    def spread(n, mask):
        return pltpu.make_async_remote_copy(src_ref=last[n], dst_ref=sums[n].at[core, geo.chip], send_sem=spread_send.at[n, mask], recv_sem=spread_recv.at[n, mask], device_id=geo.member(2 * geo.across(mask) + core), device_id_type=MESH)

    own = [pltpu.make_async_copy(last[n], sums[n].at[core, geo.chip], load_sem.at[n]) for n in four]
    for n in four:
        own[n].start()
        for mask in ORDER[1:]:
            spread(n, mask).start()
    gather(1)
    forward(0)

    def cross(n):
        return pltpu.make_async_remote_copy(src_ref=sums[n].at[core], dst_ref=sums[n].at[core], send_sem=cross_sem.at[0, n], recv_sem=cross_sem.at[1, n], device_id=geo.sibling, device_id_type=MESH)

    for n in four:
        own[n].wait()
        for mask in ORDER[1:]:
            spread(n, mask).wait()
        cross(n).start()
    forward(1)
    for n in (2, 0, 1):
        for mask in (1, 2):
            relay(n, mask).wait()
        fold(n, 3).start()
    for n in three:
        local[n].wait()
        for mask in range(4):
            fold(n, mask).wait()
    for n in four:
        cross(n).wait()


def final_exchange(mesh, halves, parts):
    ep, dp = mesh.shape["ep"], mesh.shape["dp"]
    chips, plane = ep * dp // 4, dp // 2
    bf16 = jnp.bfloat16
    anywhere = pl.BlockSpec(memory_space=pl.ANY)
    like = jax.ShapeDtypeStruct
    cut = [part.reshape(2, chips, part.shape[0] // (2 * chips), part.shape[1]) for part in parts]
    piece = [c.shape[2:] for c in cut]
    vmem, dma = pltpu.VMEM, pltpu.SemaphoreType.DMA
    scratch = [vmem((chips,) + s, bf16) for _ in range(3) for s in piece] + [vmem(s, bf16) for _ in range(3) for s in piece]
    scratch += [dma((4,)), dma((2, 4)), dma((4, chips)), dma((4, chips)), dma((2, 4)), dma((4, chips)), dma((4, chips)), dma((2, 4)), dma((2, 3, 4)), dma((3,)), dma((2, 3, plane))]
    outs = pl.pallas_call(
        functools.partial(final_kernel, ep, dp),
        name="final_exchange",
        out_shape=[like((plane, 2) + h.shape, bf16) for h in halves] + [like(c.shape, bf16) for c in cut],
        in_specs=[anywhere] * 7,
        out_specs=[anywhere] * 7,
        scratch_shapes=scratch,
        compiler_params=pltpu.CompilerParams(collective_id=3, has_side_effects=True, vmem_limit_bytes=40 * 2**20),
        cost_estimate=pl.CostEstimate(flops=10**10, bytes_accessed=30 * 2**20, transcendentals=0),
    )(*halves, *cut)
    full = [out.reshape(plane, 2 * out.shape[2], out.shape[3]) for out in outs[:3]]
    return full, [out.reshape(part.shape) for out, part in zip(outs[3:], parts)]


def take_rows(source, index):
    return jnp.take(source, index, axis=0, mode="clip")


def slot_owners(slot_of_token, slots):
    tokens = slot_of_token.shape[1]
    fine = 64
    token = jnp.arange(tokens, dtype=jnp.int32)
    coarse = (slot_of_token[:, :, None] // fine == jnp.arange(slots // fine, dtype=jnp.int32)).astype(jnp.bfloat16)
    value = jnp.stack([token // 256, token % 256, jnp.ones_like(token)], axis=1).astype(jnp.bfloat16)
    within = (slot_of_token[:, :, None] % fine == jnp.arange(fine, dtype=jnp.int32)).astype(jnp.bfloat16)
    spread = (value[None, :, :, None] * within[:, :, None, :]).reshape(slot_of_token.shape[0], tokens, 3 * fine)
    found = jnp.einsum("lta,ltb->lab", coarse, spread, preferred_element_type=jnp.float32).astype(jnp.int32)
    high, low, used = found[:, :, :fine], found[:, :, fine:2 * fine], found[:, :, 2 * fine:]
    return (high * 256 + low + (1 - used) * tokens).reshape(slot_of_token.shape[0], slots)


def solution(mesh):
    tok_spec = P(ALL_AXES, None)
    route_spec = P(None, ALL_AXES, None)
    exp_spec = P(None, "ep", None, None)
    repl_spec = P(None, None, None)
    ep, dp = mesh.shape["ep"], mesh.shape["dp"]
    members = ep * dp // 2
    to_partner = [(d, (d + members) % (2 * members)) for d in range(2 * members)]
    groups = [[side * members + m for m in range(members)] for side in range(2)]

    def body(act_in, grad_out, slot_ids, gate_vals, w_dense, w_gate, w_up, w_down, ws_gate, ws_up, ws_down):
        tokens, width = act_in.shape
        slots = 2 * tokens
        block = tokens // members
        experts = (w_gate, w_up, w_down)
        shared = (ws_gate, ws_up, ws_down)
        core, local = lax.axis_index("dp") % 2, lax.axis_index("dp") // 2

        got = []
        for w in experts[:2]:
            rows, columns = w.shape[2] // 2, w.shape[3]
            mine = lax.dynamic_slice(w, (0, local, core * rows, 0), (1, 1, rows, columns)).reshape(rows, columns)
            got.append(lax.ppermute(mine, ALL_AXES, to_partner))

        side = lax.axis_index("ep") // (ep // 2)
        turned = (slot_ids.reshape(2, tokens) + side * tokens) % slots
        owner = slot_owners(turned[1:], slots).reshape(2, members, block)

        def extended(rows):
            return jnp.pad(rows, ((0, 8), (0, 0)))

        def from_slots(layer, back):
            return take_rows(back.reshape(slots, width), turned[layer]).astype(jnp.float32)

        def mix(act, layer):
            return (act.astype(jnp.float32) + dot32(act, w_dense[layer])).astype(jnp.bfloat16)

        def gated(grad, layer):
            return (gate_vals[layer] * grad.astype(jnp.float32)).astype(jnp.bfloat16)

        def go_out(part, rows):
            blocks = take_rows(rows, owner[part].reshape(-1)).reshape(members, block, width)
            return lax.all_to_all(blocks, ALL_AXES, 0, 0, axis_index_groups=groups)

        grads_two = extended(gated(grad_out, 1))
        grads_first = go_out(1, grads_two)
        mixed_one = mix(act_in, 0)
        recv, back, shared_y, *foreign = forward_exchange(mesh, turned[0:1], mixed_one, experts, shared, got)
        back, grads_two = lax.optimization_barrier((back, grads_two))
        grads_second = go_out(0, grads_two)
        routed = from_slots(0, back)
        act_two = (mixed_one.astype(jnp.float32) + gate_vals[0] * routed + shared_y).astype(jnp.bfloat16)
        mixed_two = mix(act_two, 1)

        def finish(layer, act, grad_y, back, shared_dx):
            routed = from_slots(layer, back)
            grad_mixed = (grad_y.astype(jnp.float32) + routed + shared_dx).astype(jnp.bfloat16)
            g_dense = contract_rows(act, grad_mixed).astype(jnp.bfloat16)
            return (grad_mixed.astype(jnp.float32) + contract_cols(grad_mixed, w_dense[layer])).astype(jnp.bfloat16), g_dense

        def gather(half):
            return lax.all_gather(half, "dp", axis=0, tiled=True).reshape((dp // 2, 2 * half.shape[0], half.shape[1]))

        out = backward_exchange(mesh, 1, turned[1:2], [grads_second, grads_first], mixed_two, mixed_two, grad_out, experts, foreign[3:], shared)
        shared_two, own_two = out[3:6], out[6:9]
        experts_two = [gather(half) for half in own_two]
        grad_one, dense_two = finish(1, act_two, grad_out, out[0], out[1])
        sums_two = [lax.psum(part, ALL_AXES) for part in (dense_two, *shared_two)]

        out = backward_exchange(mesh, 0, turned[0:1], [recv], gated(grad_one, 0), mixed_one, grad_one, experts, foreign[:3], shared)
        shared_one, own_one = out[3:6], out[6:9]
        grad_act, dense_one = finish(0, act_in, grad_one, out[0], out[1])
        experts_one, sums_one = final_exchange(mesh, own_one, [dense_one, *shared_one])

        expert_out = [jnp.stack(pair) for pair in zip(experts_one, experts_two)]
        sums_out = [jnp.stack(pair) for pair in zip(sums_one, sums_two)]
        return (grad_act, sums_out[0], *expert_out, *sums_out[1:])

    return jax.shard_map(body, mesh=mesh, in_specs=(tok_spec, tok_spec, route_spec, route_spec, repl_spec, exp_spec, exp_spec, exp_spec, repl_spec, repl_spec, repl_spec), out_specs=(tok_spec, repl_spec, exp_spec, exp_spec, exp_spec, repl_spec, repl_spec, repl_spec), check_vma=False)
```

```python
import functools

import jax
import jax.numpy as jnp
from jax import lax
from jax.experimental import pallas as pl
from jax.experimental.pallas import tpu as pltpu
from jax.sharding import PartitionSpec as P


ALL_AXES = ("ep", "dp")
MESH = pl.DeviceIdType.MESH
STEPS = 2
ORDER = (0, 7, 3, 4, 5, 2, 1, 6)
ORDER_CODE = sum(mask * 8**step for step, mask in enumerate(ORDER))
AT_ONCE = (1, 2, 4, 6)
RELEASED = ((1, 3), (2, 5), (4, 7))
EARLY = (1, 2, 4)
PACK_CODE = sum(step * 8**n for n, step in enumerate((1, 2, 4, 6, 0, 3, 5, 7)))


def contract_rows(left, right):
    return lax.dot_general(left, right, (((0,), (0,)), ((), ())), preferred_element_type=jnp.float32)


def contract_cols(left, right):
    return lax.dot_general(left, right, (((1,), (1,)), ((), ())), preferred_element_type=jnp.float32)


def dot32(left, right):
    return jnp.dot(left, right, preferred_element_type=jnp.float32)


class Geometry:
    def __init__(self, ep, dp):
        self.ep, self.dp = ep, dp
        self.chips = (ep // 2) * (dp // 2)
        z, j = lax.axis_index("ep"), lax.axis_index("dp")
        self.core = j % 2
        self.local = j // 2
        self.base = (z // (ep // 2)) * (ep // 2)
        self.chip = (z % (ep // 2)) * (dp // 2) + j // 2
        self.me = 2 * self.chip + self.core
        self.sibling = (z, (j // 2) * 2 + 1 - self.core)
        self.partner = ((z + ep // 2) % ep, j)

    def member(self, index):
        return (self.base + index // self.dp, index % self.dp)

    def across(self, mask):
        total = 0
        for bit in (1, 2, 4):
            total += (self.chip // bit + mask // bit) % 2 * bit
        return total

    def at_step(self, step):
        power = (1 + 7 * (step % 2)) * (1 + 63 * (step // 2 % 2)) * (1 + 4095 * (step // 4))
        return self.across(ORDER_CODE // power % 8)

    def entry_barrier(self):
        barrier = pltpu.get_barrier_semaphore()

        @pl.loop(1, self.chips)
        def _(mask):
            for core in range(2):
                pl.semaphore_signal(barrier, inc=1, device_id=self.member(2 * self.across(mask) + core), device_id_type=MESH)

        for device in (self.sibling, self.partner):
            pl.semaphore_signal(barrier, inc=1, device_id=device, device_id_type=MESH)
        pl.semaphore_wait(barrier, 2 * self.chips)


class Outbound:
    def __init__(self, geo, part, send, recv, send_sem, recv_sem):
        self.geo, self.part = geo, part
        self.send, self.recv, self.send_sem, self.recv_sem = [ref.at[part] for ref in (send, recv, send_sem, recv_sem)]

    def copy(self, step, core):
        geo = self.geo
        index = 2 * geo.at_step(step) + core
        return pltpu.make_async_remote_copy(src_ref=self.send.at[index], dst_ref=self.recv.at[step, geo.core], send_sem=self.send_sem.at[step, core], recv_sem=self.recv_sem.at[step, geo.core], device_id=geo.member(index), device_id_type=MESH)

    def own(self):
        geo = self.geo
        return pltpu.make_async_copy(self.send.at[geo.me], self.recv.at[0, geo.core], self.recv_sem.at[0, geo.core])

    def pack(self, slots, rows):
        geo = self.geo
        tokens = rows.shape[0]
        block = self.send.shape[1]

        @pl.loop(0, geo.chips)
        def _(n):
            power = (1 + 7 * (n % 2)) * (1 + 63 * (n // 2 % 2)) * (1 + 4095 * (n // 4))
            chip = geo.at_step(PACK_CODE // power % 8)
            base = self.part * tokens + chip * 2 * block
            wanted = base + lax.broadcasted_iota(jnp.int32, (2 * block, tokens), 0)
            pick = (wanted == slots[...]).astype(jnp.float32).astype(jnp.bfloat16)
            self.send[pl.ds(2 * chip, 2)] = dot32(pick, rows[...]).astype(jnp.bfloat16).reshape(2, block, rows.shape[1])
            for when, step in enumerate(AT_ONCE):
                pl.when(n == when + 1)(functools.partial(self.issue, step))

        self.own().start()
        self.copy(0, 1 - geo.core).start()

    def issue(self, step):
        for core in range(2):
            self.copy(step, core).start()

    def arrive(self, step):
        for core in range(2):
            pltpu.make_async_copy(self.send.at[0], self.recv.at[step, core], self.recv_sem.at[step, core]).wait()
        for trigger, later in RELEASED:
            if isinstance(step, int):
                if step == trigger:
                    self.issue(later)
            else:
                pl.when(step == trigger)(functools.partial(self.issue, later))

    def wait_sends(self):
        self.copy(0, 1 - self.geo.core).wait_send()

        @pl.loop(1, self.geo.chips)
        def _(step):
            for core in range(2):
                self.copy(step, core).wait_send()


class Return:
    def __init__(self, geo, rows, back, send_sem, recv_sem):
        self.geo, self.rows, self.back, self.send_sem, self.recv_sem = geo, rows, back, send_sem, recv_sem

    def copy(self, step, core):
        geo = self.geo
        return pltpu.make_async_remote_copy(src_ref=self.rows.at[step, core], dst_ref=self.back.at[geo.me], send_sem=self.send_sem.at[step, core], recv_sem=self.recv_sem.at[geo.me], device_id=geo.member(2 * geo.at_step(step) + core), device_id_type=MESH)

    def start(self, step):
        geo = self.geo

        @pl.when(step == 0)
        def _():
            pltpu.make_async_copy(self.rows.at[0, geo.core], self.back.at[geo.me], self.recv_sem.at[geo.me]).start()
            self.copy(0, 1 - geo.core).start()

        @pl.when(step > 0)
        def _():
            for core in range(2):
                self.copy(step, core).start()

    def wait_all(self):
        geo = self.geo
        self.copy(0, 1 - geo.core).wait_send()

        @pl.loop(1, geo.chips)
        def _(step):
            for core in range(2):
                self.copy(step, core).wait_send()

        @pl.loop(0, 2 * geo.chips)
        def _(index):
            pltpu.make_async_copy(self.rows.at[0, 0], self.back.at[index], self.recv_sem.at[index]).wait()


def half_rows(rows, core):
    return pl.ds(pl.multiple_of(core * (rows // 2), 8), rows // 2)


class WeightSwap:
    def __init__(self, geo, layer, own, foreign, sems, which):
        self.geo, self.layer, self.own, self.foreign, self.sems, self.every = geo, layer, own, foreign, sems, which

    def over(self, which):
        geo = self.geo
        rows = half_rows(self.foreign[which].shape[0], geo.core)
        return pltpu.make_async_remote_copy(src_ref=self.own[which].at[self.layer, geo.local, rows], dst_ref=self.foreign[which].at[rows], send_sem=self.sems.at[0, which], recv_sem=self.sems.at[1, which], device_id=geo.partner, device_id_type=MESH)

    def across(self, which):
        geo = self.geo
        rows = self.foreign[which].at[half_rows(self.foreign[which].shape[0], geo.core)]
        return pltpu.make_async_remote_copy(src_ref=rows, dst_ref=rows, send_sem=self.sems.at[2, which], recv_sem=self.sems.at[3, which], device_id=geo.sibling, device_id_type=MESH)

    def start(self):
        for which in self.every:
            self.over(which).start()

    def pass_on(self):
        for which in self.every:
            self.over(which).wait()
            self.across(which).start()

    def finish(self):
        for which in self.every:
            self.across(which).wait()


def silu(value):
    return value * jax.nn.sigmoid(value)


def forward_kernel(ep, dp, slots, mixed, *refs):
    refs = list(refs)

    def take(count):
        got = refs[:count]
        del refs[:count]
        return got

    experts, ws, got = take(3), take(3), take(2)
    recv_out, back, shared = take(3)
    keep_out, next_out = take(3), take(1)
    send, recv, outs = take(3)
    shared_w, own_w, foreign_w = take(3), take(3), take(3)
    go_sem, get_sem, ret_sem, res_sem, swap_sem, down_sem, pass_sem, load_sem, save_sem = refs
    geo = Geometry(ep, dp)
    geo.entry_barrier()
    outbound = [Outbound(geo, part, send, recv, go_sem, get_sem) for part in range(2)]
    returns = [Return(geo, outs.at[part], back.at[part], ret_sem.at[part], res_sem.at[part]) for part in range(2)]
    swap = WeightSwap(geo, 1, experts, next_out, swap_sem, (0,))
    down = WeightSwap(geo, 0, experts, foreign_w, down_sem, (2,))
    loads = []
    passes = []
    for which in range(3):
        loads.append(pltpu.make_async_copy(ws[which].at[0], shared_w[which], load_sem.at[0, which]))
        loads.append(pltpu.make_async_copy(experts[which].at[0, geo.local], own_w[which], load_sem.at[1, which]))
    for which in range(2):
        mine = half_rows(foreign_w[which].shape[0], geo.core)
        loads.append(pltpu.make_async_copy(got[which], foreign_w[which].at[mine], load_sem.at[2, which]))
        passes.append(pltpu.make_async_remote_copy(src_ref=got[which], dst_ref=foreign_w[which].at[mine], send_sem=pass_sem.at[0, which], recv_sem=pass_sem.at[1, which], device_id=geo.sibling, device_id_type=MESH))
    down.start()
    for copy in loads + passes:
        copy.start()
    outbound[0].pack(slots, mixed)
    outbound[1].pack(slots, mixed)
    swap.start()

    tile = 2 * STEPS * recv.shape[3]

    def ffn(rows, w_one, w_three, w_two):
        a_one = dot32(rows, w_one[...])
        a_three = dot32(rows, w_three[...])
        hidden = (silu(a_one) * a_three).astype(jnp.bfloat16)
        return dot32(hidden, w_two[...])

    for copy in loads + passes:
        copy.wait()

    @pl.loop(0, mixed.shape[0] // tile)
    def _(t):
        at = pl.ds(pl.multiple_of(t * tile, tile), tile)
        shared[at, :] = ffn(mixed[at, :], *shared_w)

    width = mixed.shape[1]
    for part, weights in enumerate((own_w, foreign_w)):
        if part == 1:
            down.finish()
            keeps = [pltpu.make_async_copy(src, dst, load_sem.at[0, which]) for which, (src, dst) in enumerate(zip(foreign_w, keep_out))]
            for keep in keeps:
                keep.start()

        @pl.loop(0, geo.chips // STEPS)
        def _(t):
            steps = pl.ds(t * STEPS, STEPS)
            for step in range(STEPS):
                outbound[part].arrive(t * STEPS + step)
            pltpu.make_async_copy(recv.at[part, steps], recv_out.at[part, steps], save_sem.at[part, t]).start()
            rows = recv[part, steps].reshape(tile, width)
            outs[part, steps] = ffn(rows, *weights).astype(jnp.bfloat16).reshape(STEPS, 2, tile // (2 * STEPS), width)

            @pl.when(t > 0)
            def _():
                for step in range(STEPS):
                    returns[part].start((t - 1) * STEPS + step)

        for step in range(STEPS):
            returns[part].start(geo.chips - STEPS + step)
        if part == 0:
            down.pass_on()
    swap.pass_on()
    for part in range(2):
        outbound[part].wait_sends()
        returns[part].wait_all()

        @pl.loop(0, geo.chips // STEPS)
        def _(t):
            steps = pl.ds(t * STEPS, STEPS)
            pltpu.make_async_copy(recv.at[part, steps], recv_out.at[part, steps], save_sem.at[part, t]).wait()

    for keep in keeps:
        keep.wait()
    swap.finish()


def forward_exchange(mesh, slots, mixed, experts, shared, got):
    ep, dp = mesh.shape["ep"], mesh.shape["dp"]
    tokens, width = mixed.shape
    members = ep * dp // 2
    block = tokens // members
    bf16, f32 = jnp.bfloat16, jnp.float32
    shapes = [w.shape[2:] for w in experts]
    hidden = shapes[0][1]
    chips = members // 2
    anywhere = pl.BlockSpec(memory_space=pl.ANY)
    inside = pl.BlockSpec(memory_space=pltpu.VMEM)
    flops = 2 * 3 * width * hidden * (2 * members * block + tokens)
    expert = [jax.ShapeDtypeStruct(s, bf16) for s in shapes]
    dma = pltpu.SemaphoreType.DMA
    return pl.pallas_call(
        functools.partial(forward_kernel, ep, dp),
        name="forward_exchange",
        out_shape=[jax.ShapeDtypeStruct((2, chips, 2, block, width), bf16), jax.ShapeDtypeStruct((2, members, block, width), bf16), jax.ShapeDtypeStruct((tokens, width), f32)] + expert + expert[:1],
        in_specs=[inside, inside] + [anywhere] * 8,
        out_specs=[anywhere, anywhere, inside] + [anywhere] * 4,
        scratch_shapes=[pltpu.VMEM((2, members, block, width), bf16)]
        + [pltpu.VMEM((2, chips, 2, block, width), bf16) for _ in range(2)]
        + [pltpu.VMEM(s, bf16) for _ in range(3) for s in shapes]
        + [dma((2, chips, 2)), dma((2, chips, 2)), dma((2, chips, 2)), dma((2, members)), dma((4, 3)), dma((4, 3)), dma((2, 3)), dma((3, 3)), dma((2, chips // STEPS))],
        compiler_params=pltpu.CompilerParams(collective_id=0, has_side_effects=True, vmem_limit_bytes=60 * 2**20),
        cost_estimate=pl.CostEstimate(flops=flops, bytes_accessed=40 * 2**20, transcendentals=0),
    )(slots, mixed, *experts, *shared, *got)


class PairSum:
    def __init__(self, geo, stages, theirs, sems, expert):
        self.geo, self.stages, self.theirs, self.sems, self.expert = geo, stages, theirs, sems, expert

    def mine(self, which):
        return self.stages[which].at[self.expert, half_rows(self.stages[which].shape[1], self.geo.core)]

    def copy(self, which):
        geo = self.geo
        return pltpu.make_async_remote_copy(src_ref=self.stages[which].at[self.expert, half_rows(self.stages[which].shape[1], 1 - geo.core)], dst_ref=self.theirs[which].at[self.expert], send_sem=self.sems.at[0, self.expert, which], recv_sem=self.sems.at[1, self.expert, which], device_id=geo.sibling, device_id_type=MESH)

    def start(self):
        for which in range(3):
            self.copy(which).start()

    def finish(self):
        for which in range(3):
            self.copy(which).wait()
            mine = self.mine(which)
            mine[...] = (mine[...].astype(jnp.float32) + self.theirs[which][self.expert].astype(jnp.float32)).astype(jnp.bfloat16)


def backward_kernel(ep, dp, layer, *refs):
    refs = list(refs)

    def take(count):
        got = refs[:count]
        del refs[:count]
        return got

    slots = take(1)[0]
    held = take(2 if layer else 1)
    rows_in, mixed, grad_y = take(3)
    own_w, foreign_w, shared_w = take(3), take(3), take(3)
    back, shared_dx, recv = take(3)
    shared_out, own_out = take(3), take(3)
    source, send, x_buf, g_buf, dx_rows, dx_buf = take(6)
    weights, acc, stages, theirs, partner_in = take(3), take(3), take(3), take(3), take(3)
    go_sem, get_sem, ret_sem, res_sem, partner_sem, load_sem, x_sem, g_sem, dx_sem, pair_sem, pass_sem = refs

    geo = Geometry(ep, dp)
    geo.entry_barrier()
    tile = 2 * send.shape[2]
    fill = pltpu.make_async_copy(rows_in, source, dx_sem.at[0])
    fill.start()
    width = mixed.shape[1]
    per_set = mixed.shape[0] // tile
    total = 3 * per_set
    outbound = [Outbound(geo, part, send, recv, go_sem, get_sem) for part in range(2)]
    returns = [Return(geo, dx_rows.at[part], back.at[part], ret_sem.at[part], res_sem.at[part]) for part in range(2)]
    pairs = [PairSum(geo, stages, theirs, pair_sem, expert) for expert in range(2)]
    begins = (2 * per_set, 0)
    loads = []
    for which in range(3):
        loads.append(pltpu.make_async_copy(shared_w[which].at[layer], weights[which].at[2], load_sem.at[2, which]))
        loads.append(pltpu.make_async_copy(own_w[which].at[layer, geo.local], weights[which].at[0], load_sem.at[0, which]))
        whole = foreign_w[which].shape == weights[which].shape[1:]
        rows = weights[which].at[1] if whole else weights[which].at[1, half_rows(weights[which].shape[1], geo.core)]
        loads.append(pltpu.make_async_copy(foreign_w[which], rows, load_sem.at[1, which]))
        if not whole:
            loads.append(pltpu.make_async_remote_copy(src_ref=foreign_w[which], dst_ref=rows, send_sem=pass_sem.at[0, which], recv_sem=pass_sem.at[1, which], device_id=geo.sibling, device_id_type=MESH))
    for load in loads:
        load.start()
    fill.wait()
    outbound[1].pack(slots, source)
    outbound[0].pack(slots, source)
    moved, moved_sem, kept, kept_sem = (x_buf, x_sem, g_buf, g_sem) if layer else (g_buf, g_sem, x_buf, x_sem)

    def held_block(part, step, core):
        if layer:
            return held[part].at[2 * geo.at_step(step) + core]
        return held[0].at[part, step, core]

    def fetch(i, slot):
        @pl.when(i // per_set == 1)
        def _():
            at = pl.ds(pl.multiple_of((i - per_set) * tile, tile), tile)
            pltpu.make_async_copy(mixed.at[at], x_buf.at[slot], x_sem.at[slot]).start()
            pltpu.make_async_copy(grad_y.at[at], g_buf.at[slot], g_sem.at[slot]).start()

        for part in range(2):
            begin = begins[part]

            @pl.when((i >= begin) & (i < begin + per_set))
            def _(part=part, begin=begin):
                step = i - begin
                if part == 1:
                    outbound[part].arrive(step)
                else:
                    early = (step == EARLY[0]) | (step == EARLY[1]) | (step == EARLY[2])
                    pl.when(jnp.logical_not(early))(lambda: outbound[part].arrive(step))
                for core in range(2):
                    at = pl.ds(core * (tile // 2), tile // 2)
                    pltpu.make_async_copy(recv.at[part, step, core], moved.at[slot, at], moved_sem.at[slot]).start()
                    pltpu.make_async_copy(held_block(part, step, core), kept.at[slot, at], kept_sem.at[slot]).start()

    def store_shared(i):
        return pltpu.make_async_copy(dx_buf.at[i % 2], shared_dx.at[pl.ds(pl.multiple_of((i - per_set) * tile, tile), tile)], dx_sem.at[i % 2])

    def partner_copies():
        return [pltpu.make_async_remote_copy(src_ref=pairs[1].mine(which), dst_ref=partner_in[which], send_sem=partner_sem.at[0, which], recv_sem=partner_sem.at[1, which], device_id=geo.partner, device_id_type=MESH) for which in range(3)]

    fetch(0, 0)
    for load in loads:
        load.wait()

    @pl.loop(0, total)
    def _(i):
        slot = i % 2
        which_set = (i // per_set + 1) % 3
        for n, step in enumerate(EARLY):
            pl.when(i == per_set + 1 + 2 * n)(functools.partial(outbound[0].arrive, step))
        fetch(i + 1, (i + 1) % 2)
        pltpu.make_async_copy(mixed.at[pl.ds(0, tile)], x_buf.at[slot], x_sem.at[slot]).wait()
        pltpu.make_async_copy(mixed.at[pl.ds(0, tile)], g_buf.at[slot], g_sem.at[slot]).wait()

        @pl.when(i % per_set == 0)
        def _():
            for a in acc:
                a[...] = jnp.zeros(a.shape, jnp.float32)

        x = x_buf[slot]
        g = g_buf[slot]
        w_one, w_three, w_two = [w.at[which_set] for w in weights]
        a_one = dot32(x, w_one[...])
        a_three = dot32(x, w_three[...])
        grad_hidden = contract_cols(g, w_two[...])
        sigma = jax.nn.sigmoid(a_one)
        gated = a_one * sigma
        hidden = (gated * a_three).astype(jnp.bfloat16)
        grad_one = (grad_hidden * a_three * (sigma * (1.0 + a_one * (1.0 - sigma)))).astype(jnp.bfloat16)
        grad_three = (grad_hidden * gated).astype(jnp.bfloat16)
        acc[0][...] += contract_rows(x, grad_one)
        acc[1][...] += contract_rows(x, grad_three)
        acc[2][...] += contract_rows(hidden, g)
        dx = contract_cols(grad_one, w_one[...]) + contract_cols(grad_three, w_three[...])

        @pl.when(i // per_set == 1)
        def _():
            pl.when(i >= per_set + 2)(lambda: store_shared(i - 2).wait())
            dx_buf[slot] = dx
            store_shared(i).start()

        @pl.when(i == 2 * per_set - 1)
        def _():
            for a, out in zip(acc, shared_out):
                out[...] = a[...].astype(jnp.bfloat16)

        for part in range(2):
            begin = begins[part]

            @pl.when((i >= begin) & (i < begin + per_set))
            def _(part=part, begin=begin):
                dx_rows[part, i - begin] = dx.astype(jnp.bfloat16).reshape(2, tile // 2, width)

            @pl.when((i > begin) & (i <= begin + per_set))
            def _(part=part, begin=begin):
                returns[part].start(i - 1 - begin)

            @pl.when(i == begin + per_set - 1)
            def _(part=part):
                for a, stage in zip(acc, stages):
                    stage[part] = a[...].astype(jnp.bfloat16)

        pl.when(i == per_set)(pairs[1].start)
        pl.when(i == per_set + 1)(pairs[1].finish)

        @pl.when(i == per_set + 2)
        def _():
            for copy in partner_copies():
                copy.start()

    returns[0].start(per_set - 1)
    pairs[0].start()
    pairs[0].finish()
    for which, copy in enumerate(partner_copies()):
        copy.wait()
        own_out[which][...] = (pairs[0].mine(which)[...].astype(jnp.float32) + partner_in[which][...].astype(jnp.float32)).astype(jnp.bfloat16)
    store_shared(2 * per_set - 2).wait()
    store_shared(2 * per_set - 1).wait()
    for part in range(2):
        outbound[part].wait_sends()
        returns[part].wait_all()


def backward_exchange(mesh, layer, slots, held, rows, mixed, grad_y, own, foreign, shared):
    ep, dp = mesh.shape["ep"], mesh.shape["dp"]
    tokens, width = mixed.shape
    members = ep * dp // 2
    block = tokens // members
    chips = members // 2
    tile = 2 * block
    bf16, f32 = jnp.bfloat16, jnp.float32
    anywhere = pl.BlockSpec(memory_space=pl.ANY)
    inside = pl.BlockSpec(memory_space=pltpu.VMEM)
    shapes = [w.shape[2:] for w in own]
    halves = [(s[0] // 2, s[1]) for s in shapes]
    like = jax.ShapeDtypeStruct
    by_step = like((2, chips, 2, block, width), bf16)
    outs = [like((2, members, block, width), bf16), like((tokens, width), f32), by_step] + [like(s, bf16) for s in shapes + halves]
    vmem = pltpu.VMEM
    scratch = [vmem((tokens, width), bf16), vmem((2, members, block, width), bf16), vmem((2, tile, width), bf16), vmem((2, tile, width), bf16), vmem(by_step.shape, bf16), vmem((2, tile, width), f32)]
    scratch += [vmem((3,) + s, bf16) for s in shapes] + [vmem(s, f32) for s in shapes] + [vmem((2,) + s, bf16) for s in shapes]
    scratch += [vmem((2,) + s, bf16) for s in halves] + [vmem(s, bf16) for s in halves]
    dma = pltpu.SemaphoreType.DMA
    scratch += [dma((2, chips, 2)), dma((2, chips, 2)), dma((2, chips, 2)), dma((2, members)), dma((2, 3)), dma((3, 3)), dma((2,)), dma((2,)), dma((2,)), dma((2, 2, 3)), dma((2, 3))]
    operands = [slots, *held, rows, mixed, grad_y, *own, *foreign, *shared]
    flops = 2 * 8 * width * shapes[0][1] * (2 * members * block + tokens)
    return pl.pallas_call(
        functools.partial(backward_kernel, ep, dp, layer),
        name="backward_second" if layer else "backward_first",
        out_shape=outs,
        in_specs=[inside] + [anywhere] * (len(operands) - 1),
        out_specs=[anywhere] * 3 + [inside] * 6,
        scratch_shapes=scratch,
        compiler_params=pltpu.CompilerParams(collective_id=1 + layer, has_side_effects=True, vmem_limit_bytes=63 * 2**20),
        cost_estimate=pl.CostEstimate(flops=flops, bytes_accessed=60 * 2**20, transcendentals=0),
    )(*operands)


def final_kernel(ep, dp, *refs):
    refs = list(refs)

    def take(count):
        got = refs[:count]
        del refs[:count]
        return got

    halves, parts = take(3), take(4)
    full, sums = take(3), take(4)
    first, mine, wide, piece, other, last = [take(4) for _ in range(6)]
    load_sem, pair_sem, wide_send, wide_recv, partner_sem, spread_send, spread_recv, cross_sem, gather_sem, local_sem, fold_sem = refs
    geo = Geometry(ep, dp)
    geo.entry_barrier()
    z, core = lax.axis_index("ep"), geo.core
    four, three = range(4), range(3)
    f32, bf16 = jnp.float32, jnp.bfloat16

    to_sibling = [pltpu.make_async_remote_copy(src_ref=parts[n].at[1 - core], dst_ref=first[n], send_sem=pair_sem.at[0, n], recv_sem=pair_sem.at[1, n], device_id=geo.sibling, device_id_type=MESH) for n in four]
    keep = [pltpu.make_async_copy(parts[n].at[core], mine[n], load_sem.at[n]) for n in four]
    for copy in to_sibling + keep:
        copy.start()

    def place(mask):
        return geo.across(mask) % (dp // 2)

    def hop(n, index, src, dst, mask):
        return pltpu.make_async_remote_copy(src_ref=src, dst_ref=dst, send_sem=gather_sem.at[0, n, index], recv_sem=gather_sem.at[1, n, index], device_id=(z, 2 * place(mask) + core), device_id_type=MESH)

    def direct(n, mask):
        return hop(n, mask - 1, halves[n], full[n].at[geo.local, core], mask)

    def relay(n, mask):
        rows = halves[n].shape[0] // 2
        block = full[n].at[place(3 - mask), core, pl.ds((mask - 1) * rows, rows)]
        return hop(n, mask + 1, block, block, mask)

    def fold(n, mask):
        block = full[n].at[place(mask), core]
        return pltpu.make_async_remote_copy(src_ref=halves[n] if mask == 0 else block, dst_ref=block, send_sem=fold_sem.at[0, n, mask], recv_sem=fold_sem.at[1, n, mask], device_id=geo.sibling, device_id_type=MESH)

    local = [pltpu.make_async_copy(halves[n], full[n].at[geo.local, core], local_sem.at[n]) for n in three]

    def gather(n):
        for mask in (1, 2):
            direct(n, mask).start()
        fold(n, 0).start()
        local[n].start()

    def forward(n):
        for mask in (1, 2):
            direct(n, mask).wait()
        for mask in (1, 2):
            relay(n, mask).start()
            fold(n, mask).start()

    gather(2)
    for n in four:
        to_sibling[n].wait()
        keep[n].wait()
        mine[n][...] = (mine[n][...].astype(f32) + first[n][...].astype(f32)).astype(bf16)

    def widen(n, mask):
        to = geo.across(mask)
        return pltpu.make_async_remote_copy(src_ref=mine[n].at[to], dst_ref=wide[n].at[mask], send_sem=wide_send.at[n, mask], recv_sem=wide_recv.at[n, mask], device_id=geo.member(2 * to + core), device_id_type=MESH)

    for n in four:
        for mask in ORDER[1:]:
            widen(n, mask).start()
    gather(0)
    for n in four:
        for mask in ORDER[1:]:
            widen(n, mask).wait()
        total = mine[n][geo.chip].astype(f32)
        for mask in ORDER[1:]:
            total += wide[n][mask].astype(f32)
        piece[n][...] = total.astype(bf16)

    def swap(n):
        return pltpu.make_async_remote_copy(src_ref=piece[n], dst_ref=other[n], send_sem=partner_sem.at[0, n], recv_sem=partner_sem.at[1, n], device_id=geo.partner, device_id_type=MESH)

    for n in four:
        swap(n).start()
    forward(2)
    for n in four:
        swap(n).wait()
        last[n][...] = (piece[n][...].astype(f32) + other[n][...].astype(f32)).astype(bf16)

    def spread(n, mask):
        return pltpu.make_async_remote_copy(src_ref=last[n], dst_ref=sums[n].at[core, geo.chip], send_sem=spread_send.at[n, mask], recv_sem=spread_recv.at[n, mask], device_id=geo.member(2 * geo.across(mask) + core), device_id_type=MESH)

    own = [pltpu.make_async_copy(last[n], sums[n].at[core, geo.chip], load_sem.at[n]) for n in four]
    for n in four:
        own[n].start()
        for mask in ORDER[1:]:
            spread(n, mask).start()
    gather(1)
    forward(0)

    def cross(n):
        return pltpu.make_async_remote_copy(src_ref=sums[n].at[core], dst_ref=sums[n].at[core], send_sem=cross_sem.at[0, n], recv_sem=cross_sem.at[1, n], device_id=geo.sibling, device_id_type=MESH)

    for n in four:
        own[n].wait()
        for mask in ORDER[1:]:
            spread(n, mask).wait()
        cross(n).start()
    forward(1)
    for n in (2, 0, 1):
        for mask in (1, 2):
            relay(n, mask).wait()
        fold(n, 3).start()
    for n in three:
        local[n].wait()
        for mask in range(4):
            fold(n, mask).wait()
    for n in four:
        cross(n).wait()


def final_exchange(mesh, halves, parts):
    ep, dp = mesh.shape["ep"], mesh.shape["dp"]
    chips, plane = ep * dp // 4, dp // 2
    bf16 = jnp.bfloat16
    anywhere = pl.BlockSpec(memory_space=pl.ANY)
    like = jax.ShapeDtypeStruct
    cut = [part.reshape(2, chips, part.shape[0] // (2 * chips), part.shape[1]) for part in parts]
    piece = [c.shape[2:] for c in cut]
    vmem, dma = pltpu.VMEM, pltpu.SemaphoreType.DMA
    scratch = [vmem((chips,) + s, bf16) for _ in range(3) for s in piece] + [vmem(s, bf16) for _ in range(3) for s in piece]
    scratch += [dma((4,)), dma((2, 4)), dma((4, chips)), dma((4, chips)), dma((2, 4)), dma((4, chips)), dma((4, chips)), dma((2, 4)), dma((2, 3, 4)), dma((3,)), dma((2, 3, plane))]
    outs = pl.pallas_call(
        functools.partial(final_kernel, ep, dp),
        name="final_exchange",
        out_shape=[like((plane, 2) + h.shape, bf16) for h in halves] + [like(c.shape, bf16) for c in cut],
        in_specs=[anywhere] * 7,
        out_specs=[anywhere] * 7,
        scratch_shapes=scratch,
        compiler_params=pltpu.CompilerParams(collective_id=3, has_side_effects=True, vmem_limit_bytes=40 * 2**20),
        cost_estimate=pl.CostEstimate(flops=10**10, bytes_accessed=30 * 2**20, transcendentals=0),
    )(*halves, *cut)
    full = [out.reshape(plane, 2 * out.shape[2], out.shape[3]) for out in outs[:3]]
    return full, [out.reshape(part.shape) for out, part in zip(outs[3:], parts)]


def take_rows(source, index):
    return jnp.take(source, index, axis=0, mode="clip")


def slot_owners(slot_of_token, slots):
    tokens = slot_of_token.shape[1]
    fine = 64
    token = jnp.arange(tokens, dtype=jnp.int32)
    coarse = (slot_of_token[:, :, None] // fine == jnp.arange(slots // fine, dtype=jnp.int32)).astype(jnp.bfloat16)
    value = jnp.stack([token // 256, token % 256, jnp.ones_like(token)], axis=1).astype(jnp.bfloat16)
    within = (slot_of_token[:, :, None] % fine == jnp.arange(fine, dtype=jnp.int32)).astype(jnp.bfloat16)
    spread = (value[None, :, :, None] * within[:, :, None, :]).reshape(slot_of_token.shape[0], tokens, 3 * fine)
    found = jnp.einsum("lta,ltb->lab", coarse, spread, preferred_element_type=jnp.float32).astype(jnp.int32)
    high, low, used = found[:, :, :fine], found[:, :, fine:2 * fine], found[:, :, 2 * fine:]
    return (high * 256 + low + (1 - used) * tokens).reshape(slot_of_token.shape[0], slots)


def solution(mesh):
    tok_spec = P(ALL_AXES, None)
    route_spec = P(None, ALL_AXES, None)
    exp_spec = P(None, "ep", None, None)
    repl_spec = P(None, None, None)
    ep, dp = mesh.shape["ep"], mesh.shape["dp"]
    members = ep * dp // 2
    to_partner = [(d, (d + members) % (2 * members)) for d in range(2 * members)]
    groups = [[side * members + m for m in range(members)] for side in range(2)]

    def body(act_in, grad_out, slot_ids, gate_vals, w_dense, w_gate, w_up, w_down, ws_gate, ws_up, ws_down):
        tokens, width = act_in.shape
        slots = 2 * tokens
        block = tokens // members
        experts = (w_gate, w_up, w_down)
        shared = (ws_gate, ws_up, ws_down)
        core, local = lax.axis_index("dp") % 2, lax.axis_index("dp") // 2

        def my_half(layer, w):
            rows, columns = w.shape[2] // 2, w.shape[3]
            return lax.dynamic_slice(w, (layer, local, core * rows, 0), (1, 1, rows, columns)).reshape(rows, columns)

        got = [lax.ppermute(my_half(0, w), ALL_AXES, to_partner) for w in experts[:2]]
        halves_two = [my_half(1, w) for w in experts[1:]]

        side = lax.axis_index("ep") // (ep // 2)
        turned = (slot_ids.reshape(2, tokens) + side * tokens) % slots
        owner = slot_owners(turned[1:], slots).reshape(2, members, block)

        def extended(rows):
            return jnp.pad(rows, ((0, 8), (0, 0)))

        def from_slots(layer, back):
            return take_rows(back.reshape(slots, width), turned[layer]).astype(jnp.float32)

        def mix(act, layer):
            return (act.astype(jnp.float32) + dot32(act, w_dense[layer])).astype(jnp.bfloat16)

        def gated(grad, layer):
            return (gate_vals[layer] * grad.astype(jnp.float32)).astype(jnp.bfloat16)

        def go_out(blocks):
            return lax.all_to_all(blocks, ALL_AXES, 0, 0, axis_index_groups=groups)

        grads_two = extended(gated(grad_out, 1))
        grads_two = [take_rows(grads_two, owner[part].reshape(-1)).reshape(members, block, width) for part in range(2)]
        grads_first = go_out(grads_two[1])
        mixed_one = mix(act_in, 0)
        mixed_one, grads_late = lax.optimization_barrier((mixed_one, grads_two[0]))
        recv, back, shared_y, *foreign = forward_exchange(mesh, turned[0:1], mixed_one, experts, shared, got)
        back, grads_late, halves_two = lax.optimization_barrier((back, grads_late, halves_two))
        grads_second = go_out(grads_late)
        got_two = [lax.ppermute(half, ALL_AXES, to_partner) for half in halves_two]
        routed = from_slots(0, back)
        act_two = (mixed_one.astype(jnp.float32) + gate_vals[0] * routed + shared_y).astype(jnp.bfloat16)
        mixed_two = mix(act_two, 1)

        def finish(layer, act, grad_y, back, shared_dx):
            routed = from_slots(layer, back)
            grad_mixed = (grad_y.astype(jnp.float32) + routed + shared_dx).astype(jnp.bfloat16)
            g_dense = contract_rows(act, grad_mixed).astype(jnp.bfloat16)
            return (grad_mixed.astype(jnp.float32) + contract_cols(grad_mixed, w_dense[layer])).astype(jnp.bfloat16), g_dense

        def gather(half):
            return lax.all_gather(half, "dp", axis=0, tiled=True).reshape((dp // 2, 2 * half.shape[0], half.shape[1]))

        out = backward_exchange(mesh, 1, turned[1:2], [grads_second, grads_first], mixed_two, mixed_two, grad_out, experts, [foreign[3], *got_two], shared)
        shared_two, own_two = out[3:6], out[6:9]
        experts_two = [gather(half) for half in own_two]
        grad_one, dense_two = finish(1, act_two, grad_out, out[0], out[1])
        sums_two = [lax.psum(part, ALL_AXES) for part in (dense_two, *shared_two)]

        out = backward_exchange(mesh, 0, turned[0:1], [recv], gated(grad_one, 0), mixed_one, grad_one, experts, foreign[:3], shared)
        shared_one, own_one = out[3:6], out[6:9]
        grad_act, dense_one = finish(0, act_in, grad_one, out[0], out[1])
        experts_one, sums_one = final_exchange(mesh, own_one, [dense_one, *shared_one])

        expert_out = [jnp.stack(pair) for pair in zip(experts_one, experts_two)]
        sums_out = [jnp.stack(pair) for pair in zip(sums_one, sums_two)]
        return (grad_act, sums_out[0], *expert_out, *sums_out[1:])

    return jax.shard_map(body, mesh=mesh, in_specs=(tok_spec, tok_spec, route_spec, route_spec, repl_spec, exp_spec, exp_spec, exp_spec, repl_spec, repl_spec, repl_spec), out_specs=(tok_spec, repl_spec, exp_spec, exp_spec, exp_spec, repl_spec, repl_spec, repl_spec), check_vma=False)
```

```python
import functools

import jax
import jax.numpy as jnp
from jax import lax
from jax.experimental import pallas as pl
from jax.experimental.pallas import tpu as pltpu
from jax.sharding import PartitionSpec as P


ALL_AXES = ("ep", "dp")
MESH = pl.DeviceIdType.MESH
STEPS = 2
ORDER = (0, 1, 2, 4, 3, 6, 5, 7)
ORDER_CODE = sum(mask * 8**step for step, mask in enumerate(ORDER))


def contract_rows(left, right):
    return lax.dot_general(left, right, (((0,), (0,)), ((), ())), preferred_element_type=jnp.float32)


def contract_cols(left, right):
    return lax.dot_general(left, right, (((1,), (1,)), ((), ())), preferred_element_type=jnp.float32)


def dot32(left, right):
    return jnp.dot(left, right, preferred_element_type=jnp.float32)


class Geometry:
    def __init__(self, ep, dp):
        self.ep, self.dp = ep, dp
        self.chips = (ep // 2) * (dp // 2)
        z, j = lax.axis_index("ep"), lax.axis_index("dp")
        self.core = j % 2
        self.local = j // 2
        self.base = (z // (ep // 2)) * (ep // 2)
        self.chip = (z % (ep // 2)) * (dp // 2) + j // 2
        self.me = 2 * self.chip + self.core
        self.sibling = (z, (j // 2) * 2 + 1 - self.core)
        self.partner = ((z + ep // 2) % ep, j)

    def member(self, index):
        return (self.base + index // self.dp, index % self.dp)

    def across(self, mask):
        total = 0
        for bit in (1, 2, 4):
            total += (self.chip // bit + mask // bit) % 2 * bit
        return total

    def at_step(self, step):
        power = (1 + 7 * (step % 2)) * (1 + 63 * (step // 2 % 2)) * (1 + 4095 * (step // 4))
        return self.across(ORDER_CODE // power % 8)

    def entry_barrier(self):
        barrier = pltpu.get_barrier_semaphore()

        @pl.loop(1, self.chips)
        def _(mask):
            for core in range(2):
                pl.semaphore_signal(barrier, inc=1, device_id=self.member(2 * self.across(mask) + core), device_id_type=MESH)

        for device in (self.sibling, self.partner):
            pl.semaphore_signal(barrier, inc=1, device_id=device, device_id_type=MESH)
        pl.semaphore_wait(barrier, 2 * self.chips)


def one_hot(part, chip, slots, block):
    tokens = slots.shape[1]
    wanted = part * tokens + chip * 2 * block + lax.broadcasted_iota(jnp.int32, (2 * block, tokens), 0)
    return (wanted == slots[...]).astype(jnp.float32).astype(jnp.bfloat16)


class Outbound:
    def __init__(self, geo, part, send, recv, send_sem, recv_sem):
        self.geo, self.part = geo, part
        self.send, self.recv, self.send_sem, self.recv_sem = [ref.at[part] for ref in (send, recv, send_sem, recv_sem)]

    def copy(self, step, core):
        geo = self.geo
        index = 2 * geo.at_step(step) + core
        return pltpu.make_async_remote_copy(src_ref=self.send.at[index], dst_ref=self.recv.at[step, geo.core], send_sem=self.send_sem.at[step, core], recv_sem=self.recv_sem.at[step, geo.core], device_id=geo.member(index), device_id_type=MESH)

    def own(self):
        geo = self.geo
        return pltpu.make_async_copy(self.send.at[geo.me], self.recv.at[0, geo.core], self.recv_sem.at[0, geo.core])

    def pack(self, slots, rows):
        geo = self.geo
        block = self.send.shape[1]

        @pl.loop(0, geo.chips)
        def _(n):
            chip = geo.at_step((n + 1) % geo.chips)
            pick = one_hot(self.part, chip, slots, block)
            self.send[pl.ds(2 * chip, 2)] = dot32(pick, rows[...]).astype(jnp.bfloat16).reshape(2, block, rows.shape[1])
            pl.when(n > 0)(functools.partial(self.issue, n))

        self.own().start()
        self.copy(0, 1 - geo.core).start()

    def issue(self, step):
        for core in range(2):
            self.copy(step, core).start()

    def arrive(self, step):
        for core in range(2):
            pltpu.make_async_copy(self.send.at[0], self.recv.at[step, core], self.recv_sem.at[step, core]).wait()

    def wait_sends(self):
        self.copy(0, 1 - self.geo.core).wait_send()

        @pl.loop(1, self.geo.chips)
        def _(step):
            for core in range(2):
                self.copy(step, core).wait_send()


class Return:
    def __init__(self, geo, rows, back, send_sem, recv_sem):
        self.geo, self.rows, self.back, self.send_sem, self.recv_sem = geo, rows, back, send_sem, recv_sem

    def copy(self, step, core):
        geo = self.geo
        return pltpu.make_async_remote_copy(src_ref=self.rows.at[step, core], dst_ref=self.back.at[geo.me], send_sem=self.send_sem.at[step, core], recv_sem=self.recv_sem.at[geo.me], device_id=geo.member(2 * geo.at_step(step) + core), device_id_type=MESH)

    def start(self, step):
        geo = self.geo

        @pl.when(step == 0)
        def _():
            pltpu.make_async_copy(self.rows.at[0, geo.core], self.back.at[geo.me], self.recv_sem.at[geo.me]).start()
            self.copy(0, 1 - geo.core).start()

        @pl.when(step > 0)
        def _():
            for core in range(2):
                self.copy(step, core).start()

    def wait_sends(self):
        self.copy(0, 1 - self.geo.core).wait_send()

        @pl.loop(1, self.geo.chips)
        def _(step):
            for core in range(2):
                self.copy(step, core).wait_send()

    def wait_back(self, index):
        pltpu.make_async_copy(self.rows.at[0, 0], self.back.at[index], self.recv_sem.at[index]).wait()

    def wait_all(self):
        self.wait_sends()
        pl.loop(0, 2 * self.geo.chips)(self.wait_back)


def half_rows(rows, core):
    return pl.ds(pl.multiple_of(core * (rows // 2), 8), rows // 2)


class WeightSwap:
    def __init__(self, geo, layer, own, foreign, sems, which):
        self.geo, self.layer, self.own, self.foreign, self.sems, self.every = geo, layer, own, foreign, sems, which

    def over(self, which):
        geo = self.geo
        rows = half_rows(self.foreign[which].shape[0], geo.core)
        return pltpu.make_async_remote_copy(src_ref=self.own[which].at[self.layer, geo.local, rows], dst_ref=self.foreign[which].at[rows], send_sem=self.sems.at[0, which], recv_sem=self.sems.at[1, which], device_id=geo.partner, device_id_type=MESH)

    def across(self, which):
        geo = self.geo
        rows = self.foreign[which].at[half_rows(self.foreign[which].shape[0], geo.core)]
        return pltpu.make_async_remote_copy(src_ref=rows, dst_ref=rows, send_sem=self.sems.at[2, which], recv_sem=self.sems.at[3, which], device_id=geo.sibling, device_id_type=MESH)

    def start(self):
        for which in self.every:
            self.over(which).start()

    def pass_on(self):
        for which in self.every:
            self.over(which).wait()
            self.across(which).start()

    def finish(self):
        for which in self.every:
            self.across(which).wait()


def silu(value):
    return value * jax.nn.sigmoid(value)


def forward_kernel(ep, dp, slots, gates, mixed, *refs):
    refs = list(refs)

    def take(count):
        got = refs[:count]
        del refs[:count]
        return got

    experts, ws, got = take(3), take(3), take(2)
    recv_out, act = take(2)
    keep_out, next_out = take(3), take(1)
    send, recv, outs, back, shared, routed = take(6)
    shared_w, own_w, foreign_w = take(3), take(3), take(3)
    go_sem, get_sem, ret_sem, res_sem, swap_sem, down_sem, pass_sem, load_sem, save_sem = refs
    geo = Geometry(ep, dp)
    geo.entry_barrier()
    outbound = [Outbound(geo, part, send, recv, go_sem, get_sem) for part in range(2)]
    returns = [Return(geo, outs.at[part], back.at[part], ret_sem.at[part], res_sem.at[part]) for part in range(2)]
    swap = WeightSwap(geo, 1, experts, next_out, swap_sem, (0,))
    down = WeightSwap(geo, 0, experts, foreign_w, down_sem, (2,))
    loads = []
    passes = []
    for which in range(3):
        loads.append(pltpu.make_async_copy(ws[which].at[0], shared_w[which], load_sem.at[0, which]))
        loads.append(pltpu.make_async_copy(experts[which].at[0, geo.local], own_w[which], load_sem.at[1, which]))
    for which in range(2):
        mine = half_rows(foreign_w[which].shape[0], geo.core)
        loads.append(pltpu.make_async_copy(got[which], foreign_w[which].at[mine], load_sem.at[2, which]))
        passes.append(pltpu.make_async_remote_copy(src_ref=got[which], dst_ref=foreign_w[which].at[mine], send_sem=pass_sem.at[0, which], recv_sem=pass_sem.at[1, which], device_id=geo.sibling, device_id_type=MESH))
    down.start()
    for copy in loads + passes:
        copy.start()
    outbound[0].pack(slots, mixed)
    outbound[1].pack(slots, mixed)
    swap.start()

    tile = 2 * STEPS * recv.shape[3]

    def ffn(rows, w_one, w_three, w_two):
        a_one = dot32(rows, w_one[...])
        a_three = dot32(rows, w_three[...])
        hidden = (silu(a_one) * a_three).astype(jnp.bfloat16)
        return dot32(hidden, w_two[...])

    for copy in loads + passes:
        copy.wait()

    @pl.loop(0, mixed.shape[0] // tile)
    def _(t):
        at = pl.ds(pl.multiple_of(t * tile, tile), tile)
        shared[at, :] = ffn(mixed[at, :], *shared_w)

    width = mixed.shape[1]
    for part, weights in enumerate((own_w, foreign_w)):
        if part == 1:
            down.finish()
            keeps = [pltpu.make_async_copy(src, dst, load_sem.at[0, which]) for which, (src, dst) in enumerate(zip(foreign_w, keep_out))]
            for keep in keeps:
                keep.start()

        @pl.loop(0, geo.chips // STEPS)
        def _(t):
            steps = pl.ds(t * STEPS, STEPS)
            for step in range(STEPS):
                outbound[part].arrive(t * STEPS + step)
            pltpu.make_async_copy(recv.at[part, steps], recv_out.at[part, steps], save_sem.at[part, t]).start()
            rows = recv[part, steps].reshape(tile, width)
            outs[part, steps] = ffn(rows, *weights).astype(jnp.bfloat16).reshape(STEPS, 2, tile // (2 * STEPS), width)

            @pl.when(t > 0)
            def _():
                for step in range(STEPS):
                    returns[part].start((t - 1) * STEPS + step)

        for step in range(STEPS):
            returns[part].start(geo.chips - STEPS + step)
        if part == 0:
            down.pass_on()
    swap.pass_on()
    block = send.shape[2]
    routed[...] = jnp.zeros(routed.shape, jnp.float32)
    for part in range(2):

        @pl.loop(0, geo.chips)
        def _(step):
            chip = geo.at_step(step)
            for core in range(2):
                returns[part].wait_back(2 * chip + core)
            came = back[part, pl.ds(2 * chip, 2)].reshape(2 * block, width)
            routed[...] += contract_rows(one_hot(part, chip, slots, block), came)

    @pl.loop(0, mixed.shape[0] // tile)
    def _(t):
        at = pl.ds(pl.multiple_of(t * tile, tile), tile)
        act[at, :] = (mixed[at, :].astype(jnp.float32) + gates[at, :] * routed[at, :] + shared[at, :]).astype(jnp.bfloat16)

    for part in range(2):
        outbound[part].wait_sends()
        returns[part].wait_sends()

        @pl.loop(0, geo.chips // STEPS)
        def _(t):
            steps = pl.ds(t * STEPS, STEPS)
            pltpu.make_async_copy(recv.at[part, steps], recv_out.at[part, steps], save_sem.at[part, t]).wait()

    for keep in keeps:
        keep.wait()
    swap.finish()


def forward_exchange(mesh, slots, gates, mixed, experts, shared, got):
    ep, dp = mesh.shape["ep"], mesh.shape["dp"]
    tokens, width = mixed.shape
    members = ep * dp // 2
    block = tokens // members
    bf16, f32 = jnp.bfloat16, jnp.float32
    shapes = [w.shape[2:] for w in experts]
    hidden = shapes[0][1]
    chips = members // 2
    anywhere = pl.BlockSpec(memory_space=pl.ANY)
    inside = pl.BlockSpec(memory_space=pltpu.VMEM)
    flops = 2 * 3 * width * hidden * (2 * members * block + tokens)
    expert = [jax.ShapeDtypeStruct(s, bf16) for s in shapes]
    dma = pltpu.SemaphoreType.DMA
    return pl.pallas_call(
        functools.partial(forward_kernel, ep, dp),
        name="forward_exchange",
        out_shape=[jax.ShapeDtypeStruct((2, chips, 2, block, width), bf16), jax.ShapeDtypeStruct((tokens, width), bf16)] + expert + expert[:1],
        in_specs=[inside] * 3 + [anywhere] * 8,
        out_specs=[anywhere, inside] + [anywhere] * 4,
        scratch_shapes=[pltpu.VMEM((2, members, block, width), bf16)]
        + [pltpu.VMEM((2, chips, 2, block, width), bf16) for _ in range(2)]
        + [pltpu.VMEM((2, members, block, width), bf16), pltpu.VMEM((tokens, width), f32), pltpu.VMEM((tokens, width), f32)]
        + [pltpu.VMEM(s, bf16) for _ in range(3) for s in shapes]
        + [dma((2, chips, 2)), dma((2, chips, 2)), dma((2, chips, 2)), dma((2, members)), dma((4, 3)), dma((4, 3)), dma((2, 3)), dma((3, 3)), dma((2, chips // STEPS))],
        compiler_params=pltpu.CompilerParams(collective_id=0, has_side_effects=True, vmem_limit_bytes=60 * 2**20),
        cost_estimate=pl.CostEstimate(flops=flops, bytes_accessed=40 * 2**20, transcendentals=0),
    )(slots, gates, mixed, *experts, *shared, *got)


class PairSum:
    def __init__(self, geo, stages, theirs, sems, expert):
        self.geo, self.stages, self.theirs, self.sems, self.expert = geo, stages, theirs, sems, expert

    def mine(self, which):
        return self.stages[which].at[self.expert, half_rows(self.stages[which].shape[1], self.geo.core)]

    def copy(self, which):
        geo = self.geo
        return pltpu.make_async_remote_copy(src_ref=self.stages[which].at[self.expert, half_rows(self.stages[which].shape[1], 1 - geo.core)], dst_ref=self.theirs[which].at[self.expert], send_sem=self.sems.at[0, self.expert, which], recv_sem=self.sems.at[1, self.expert, which], device_id=geo.sibling, device_id_type=MESH)

    def start(self):
        for which in range(3):
            self.copy(which).start()

    def finish(self):
        for which in range(3):
            self.copy(which).wait()
            mine = self.mine(which)
            mine[...] = (mine[...].astype(jnp.float32) + self.theirs[which][self.expert].astype(jnp.float32)).astype(jnp.bfloat16)


def backward_kernel(ep, dp, layer, *refs):
    refs = list(refs)

    def take(count):
        got = refs[:count]
        del refs[:count]
        return got

    slots = take(1)[0]
    held = take(2 if layer else 1)
    rows_in, mixed, grad_y = take(3)
    own_w, foreign_w, shared_w = take(3), take(3), take(3)
    back, shared_dx, recv = take(3)
    shared_out, own_out = take(3), take(3)
    source, send, x_buf, g_buf, dx_rows, dx_buf = take(6)
    weights, acc, stages, theirs, partner_in = take(3), take(3), take(3), take(3), take(3)
    go_sem, get_sem, ret_sem, res_sem, partner_sem, load_sem, x_sem, g_sem, dx_sem, pair_sem, pass_sem = refs

    geo = Geometry(ep, dp)
    geo.entry_barrier()
    tile = 2 * send.shape[2]
    fill = pltpu.make_async_copy(rows_in, source, dx_sem.at[0])
    fill.start()
    width = mixed.shape[1]
    per_set = mixed.shape[0] // tile
    total = 3 * per_set
    outbound = [Outbound(geo, part, send, recv, go_sem, get_sem) for part in range(2)]
    returns = [Return(geo, dx_rows.at[part], back.at[part], ret_sem.at[part], res_sem.at[part]) for part in range(2)]
    pairs = [PairSum(geo, stages, theirs, pair_sem, expert) for expert in range(2)]
    begins = (2 * per_set, 0)
    loads = []
    for which in range(3):
        loads.append(pltpu.make_async_copy(shared_w[which].at[layer], weights[which].at[2], load_sem.at[2, which]))
        loads.append(pltpu.make_async_copy(own_w[which].at[layer, geo.local], weights[which].at[0], load_sem.at[0, which]))
        whole = foreign_w[which].shape == weights[which].shape[1:]
        rows = weights[which].at[1] if whole else weights[which].at[1, half_rows(weights[which].shape[1], geo.core)]
        loads.append(pltpu.make_async_copy(foreign_w[which], rows, load_sem.at[1, which]))
        if not whole:
            loads.append(pltpu.make_async_remote_copy(src_ref=foreign_w[which], dst_ref=rows, send_sem=pass_sem.at[0, which], recv_sem=pass_sem.at[1, which], device_id=geo.sibling, device_id_type=MESH))
    for load in loads:
        load.start()
    fill.wait()
    outbound[1].pack(slots, source)
    outbound[0].pack(slots, source)
    moved, moved_sem, kept, kept_sem = (x_buf, x_sem, g_buf, g_sem) if layer else (g_buf, g_sem, x_buf, x_sem)

    def held_block(part, step, core):
        if layer:
            return held[part].at[2 * geo.at_step(step) + core]
        return held[0].at[part, step, core]

    def fetch(i, slot):
        @pl.when(i // per_set == 1)
        def _():
            at = pl.ds(pl.multiple_of((i - per_set) * tile, tile), tile)
            pltpu.make_async_copy(mixed.at[at], x_buf.at[slot], x_sem.at[slot]).start()
            pltpu.make_async_copy(grad_y.at[at], g_buf.at[slot], g_sem.at[slot]).start()

        for part in range(2):
            begin = begins[part]

            @pl.when((i >= begin) & (i < begin + per_set))
            def _(part=part, begin=begin):
                step = i - begin
                outbound[part].arrive(step)
                for core in range(2):
                    at = pl.ds(core * (tile // 2), tile // 2)
                    pltpu.make_async_copy(recv.at[part, step, core], moved.at[slot, at], moved_sem.at[slot]).start()
                    pltpu.make_async_copy(held_block(part, step, core), kept.at[slot, at], kept_sem.at[slot]).start()

    def store_shared(i):
        return pltpu.make_async_copy(dx_buf.at[i % 2], shared_dx.at[pl.ds(pl.multiple_of((i - per_set) * tile, tile), tile)], dx_sem.at[i % 2])

    def partner_copies():
        return [pltpu.make_async_remote_copy(src_ref=pairs[1].mine(which), dst_ref=partner_in[which], send_sem=partner_sem.at[0, which], recv_sem=partner_sem.at[1, which], device_id=geo.partner, device_id_type=MESH) for which in range(3)]

    fetch(0, 0)
    for load in loads:
        load.wait()

    @pl.loop(0, total)
    def _(i):
        slot = i % 2
        which_set = (i // per_set + 1) % 3
        fetch(i + 1, (i + 1) % 2)
        pltpu.make_async_copy(mixed.at[pl.ds(0, tile)], x_buf.at[slot], x_sem.at[slot]).wait()
        pltpu.make_async_copy(mixed.at[pl.ds(0, tile)], g_buf.at[slot], g_sem.at[slot]).wait()

        @pl.when(i % per_set == 0)
        def _():
            for a in acc:
                a[...] = jnp.zeros(a.shape, jnp.float32)

        x = x_buf[slot]
        g = g_buf[slot]
        w_one, w_three, w_two = [w.at[which_set] for w in weights]
        a_one = dot32(x, w_one[...])
        a_three = dot32(x, w_three[...])
        grad_hidden = contract_cols(g, w_two[...])
        sigma = jax.nn.sigmoid(a_one)
        gated = a_one * sigma
        hidden = (gated * a_three).astype(jnp.bfloat16)
        grad_one = (grad_hidden * a_three * (sigma * (1.0 + a_one * (1.0 - sigma)))).astype(jnp.bfloat16)
        grad_three = (grad_hidden * gated).astype(jnp.bfloat16)
        acc[0][...] += contract_rows(x, grad_one)
        acc[1][...] += contract_rows(x, grad_three)
        acc[2][...] += contract_rows(hidden, g)
        dx = contract_cols(grad_one, w_one[...]) + contract_cols(grad_three, w_three[...])

        @pl.when(i // per_set == 1)
        def _():
            pl.when(i >= per_set + 2)(lambda: store_shared(i - 2).wait())
            dx_buf[slot] = dx
            store_shared(i).start()

        @pl.when(i == 2 * per_set - 1)
        def _():
            for a, out in zip(acc, shared_out):
                out[...] = a[...].astype(jnp.bfloat16)

        for part in range(2):
            begin = begins[part]

            @pl.when((i >= begin) & (i < begin + per_set))
            def _(part=part, begin=begin):
                dx_rows[part, i - begin] = dx.astype(jnp.bfloat16).reshape(2, tile // 2, width)

            @pl.when((i > begin) & (i <= begin + per_set))
            def _(part=part, begin=begin):
                returns[part].start(i - 1 - begin)

            @pl.when(i == begin + per_set - 1)
            def _(part=part):
                for a, stage in zip(acc, stages):
                    stage[part] = a[...].astype(jnp.bfloat16)

        pl.when(i == per_set)(pairs[1].start)
        pl.when(i == per_set + 1)(pairs[1].finish)

        @pl.when(i == per_set + 2)
        def _():
            for copy in partner_copies():
                copy.start()

    returns[0].start(per_set - 1)
    pairs[0].start()
    pairs[0].finish()
    for which, copy in enumerate(partner_copies()):
        copy.wait()
        own_out[which][...] = (pairs[0].mine(which)[...].astype(jnp.float32) + partner_in[which][...].astype(jnp.float32)).astype(jnp.bfloat16)
    store_shared(2 * per_set - 2).wait()
    store_shared(2 * per_set - 1).wait()
    for part in range(2):
        outbound[part].wait_sends()
        returns[part].wait_all()


def backward_exchange(mesh, layer, slots, held, rows, mixed, grad_y, own, foreign, shared):
    ep, dp = mesh.shape["ep"], mesh.shape["dp"]
    tokens, width = mixed.shape
    members = ep * dp // 2
    block = tokens // members
    chips = members // 2
    tile = 2 * block
    bf16, f32 = jnp.bfloat16, jnp.float32
    anywhere = pl.BlockSpec(memory_space=pl.ANY)
    inside = pl.BlockSpec(memory_space=pltpu.VMEM)
    shapes = [w.shape[2:] for w in own]
    halves = [(s[0] // 2, s[1]) for s in shapes]
    like = jax.ShapeDtypeStruct
    by_step = like((2, chips, 2, block, width), bf16)
    outs = [like((2, members, block, width), bf16), like((tokens, width), f32), by_step] + [like(s, bf16) for s in shapes + halves]
    vmem = pltpu.VMEM
    scratch = [vmem((tokens, width), bf16), vmem((2, members, block, width), bf16), vmem((2, tile, width), bf16), vmem((2, tile, width), bf16), vmem(by_step.shape, bf16), vmem((2, tile, width), f32)]
    scratch += [vmem((3,) + s, bf16) for s in shapes] + [vmem(s, f32) for s in shapes] + [vmem((2,) + s, bf16) for s in shapes]
    scratch += [vmem((2,) + s, bf16) for s in halves] + [vmem(s, bf16) for s in halves]
    dma = pltpu.SemaphoreType.DMA
    scratch += [dma((2, chips, 2)), dma((2, chips, 2)), dma((2, chips, 2)), dma((2, members)), dma((2, 3)), dma((3, 3)), dma((2,)), dma((2,)), dma((2,)), dma((2, 2, 3)), dma((2, 3))]
    operands = [slots, *held, rows, mixed, grad_y, *own, *foreign, *shared]
    flops = 2 * 8 * width * shapes[0][1] * (2 * members * block + tokens)
    return pl.pallas_call(
        functools.partial(backward_kernel, ep, dp, layer),
        name="backward_second" if layer else "backward_first",
        out_shape=outs,
        in_specs=[inside] + [anywhere] * (len(operands) - 1),
        out_specs=[anywhere] * 3 + [inside] * 6,
        scratch_shapes=scratch,
        compiler_params=pltpu.CompilerParams(collective_id=1 + layer, has_side_effects=True, vmem_limit_bytes=63 * 2**20),
        cost_estimate=pl.CostEstimate(flops=flops, bytes_accessed=60 * 2**20, transcendentals=0),
    )(*operands)


def final_kernel(ep, dp, *refs):
    refs = list(refs)

    def take(count):
        got = refs[:count]
        del refs[:count]
        return got

    halves, parts = take(3), take(4)
    full, sums = take(3), take(4)
    first, mine, wide, piece, other, last = [take(4) for _ in range(6)]
    load_sem, pair_sem, wide_send, wide_recv, partner_sem, spread_send, spread_recv, cross_sem, gather_sem, local_sem, fold_sem = refs
    geo = Geometry(ep, dp)
    geo.entry_barrier()
    z, core = lax.axis_index("ep"), geo.core
    four, three = range(4), range(3)
    f32, bf16 = jnp.float32, jnp.bfloat16

    to_sibling = [pltpu.make_async_remote_copy(src_ref=parts[n].at[1 - core], dst_ref=first[n], send_sem=pair_sem.at[0, n], recv_sem=pair_sem.at[1, n], device_id=geo.sibling, device_id_type=MESH) for n in four]
    keep = [pltpu.make_async_copy(parts[n].at[core], mine[n], load_sem.at[n]) for n in four]
    for copy in to_sibling + keep:
        copy.start()

    def place(mask):
        return geo.across(mask) % (dp // 2)

    def hop(n, index, src, dst, mask):
        return pltpu.make_async_remote_copy(src_ref=src, dst_ref=dst, send_sem=gather_sem.at[0, n, index], recv_sem=gather_sem.at[1, n, index], device_id=(z, 2 * place(mask) + core), device_id_type=MESH)

    def direct(n, mask):
        return hop(n, mask - 1, halves[n], full[n].at[geo.local, core], mask)

    def relay(n, mask):
        rows = halves[n].shape[0] // 2
        block = full[n].at[place(3 - mask), core, pl.ds((mask - 1) * rows, rows)]
        return hop(n, mask + 1, block, block, mask)

    def fold(n, mask):
        block = full[n].at[place(mask), core]
        return pltpu.make_async_remote_copy(src_ref=halves[n] if mask == 0 else block, dst_ref=block, send_sem=fold_sem.at[0, n, mask], recv_sem=fold_sem.at[1, n, mask], device_id=geo.sibling, device_id_type=MESH)

    local = [pltpu.make_async_copy(halves[n], full[n].at[geo.local, core], local_sem.at[n]) for n in three]

    def gather(n):
        for mask in (1, 2):
            direct(n, mask).start()
        fold(n, 0).start()
        local[n].start()

    def forward(n):
        for mask in (1, 2):
            direct(n, mask).wait()
        for mask in (1, 2):
            relay(n, mask).start()
            fold(n, mask).start()

    gather(2)
    for n in four:
        to_sibling[n].wait()
        keep[n].wait()
        mine[n][...] = (mine[n][...].astype(f32) + first[n][...].astype(f32)).astype(bf16)

    def widen(n, mask):
        to = geo.across(mask)
        return pltpu.make_async_remote_copy(src_ref=mine[n].at[to], dst_ref=wide[n].at[mask], send_sem=wide_send.at[n, mask], recv_sem=wide_recv.at[n, mask], device_id=geo.member(2 * to + core), device_id_type=MESH)

    for n in four:
        for mask in ORDER[1:]:
            widen(n, mask).start()
    gather(0)
    for n in four:
        for mask in ORDER[1:]:
            widen(n, mask).wait()
        total = mine[n][geo.chip].astype(f32)
        for mask in ORDER[1:]:
            total += wide[n][mask].astype(f32)
        piece[n][...] = total.astype(bf16)

    def swap(n):
        return pltpu.make_async_remote_copy(src_ref=piece[n], dst_ref=other[n], send_sem=partner_sem.at[0, n], recv_sem=partner_sem.at[1, n], device_id=geo.partner, device_id_type=MESH)

    for n in four:
        swap(n).start()
    forward(2)
    for n in four:
        swap(n).wait()
        last[n][...] = (piece[n][...].astype(f32) + other[n][...].astype(f32)).astype(bf16)

    def spread(n, mask):
        return pltpu.make_async_remote_copy(src_ref=last[n], dst_ref=sums[n].at[core, geo.chip], send_sem=spread_send.at[n, mask], recv_sem=spread_recv.at[n, mask], device_id=geo.member(2 * geo.across(mask) + core), device_id_type=MESH)

    own = [pltpu.make_async_copy(last[n], sums[n].at[core, geo.chip], load_sem.at[n]) for n in four]
    for n in four:
        own[n].start()
        for mask in ORDER[1:]:
            spread(n, mask).start()
    gather(1)
    forward(0)

    def cross(n):
        return pltpu.make_async_remote_copy(src_ref=sums[n].at[core], dst_ref=sums[n].at[core], send_sem=cross_sem.at[0, n], recv_sem=cross_sem.at[1, n], device_id=geo.sibling, device_id_type=MESH)

    for n in four:
        own[n].wait()
        for mask in ORDER[1:]:
            spread(n, mask).wait()
        cross(n).start()
    forward(1)
    for n in (2, 0, 1):
        for mask in (1, 2):
            relay(n, mask).wait()
        fold(n, 3).start()
    for n in three:
        local[n].wait()
        for mask in range(4):
            fold(n, mask).wait()
    for n in four:
        cross(n).wait()


def final_exchange(mesh, halves, parts):
    ep, dp = mesh.shape["ep"], mesh.shape["dp"]
    chips, plane = ep * dp // 4, dp // 2
    bf16 = jnp.bfloat16
    anywhere = pl.BlockSpec(memory_space=pl.ANY)
    like = jax.ShapeDtypeStruct
    cut = [part.reshape(2, chips, part.shape[0] // (2 * chips), part.shape[1]) for part in parts]
    piece = [c.shape[2:] for c in cut]
    vmem, dma = pltpu.VMEM, pltpu.SemaphoreType.DMA
    scratch = [vmem((chips,) + s, bf16) for _ in range(3) for s in piece] + [vmem(s, bf16) for _ in range(3) for s in piece]
    scratch += [dma((4,)), dma((2, 4)), dma((4, chips)), dma((4, chips)), dma((2, 4)), dma((4, chips)), dma((4, chips)), dma((2, 4)), dma((2, 3, 4)), dma((3,)), dma((2, 3, plane))]
    outs = pl.pallas_call(
        functools.partial(final_kernel, ep, dp),
        name="final_exchange",
        out_shape=[like((plane, 2) + h.shape, bf16) for h in halves] + [like(c.shape, bf16) for c in cut],
        in_specs=[anywhere] * 7,
        out_specs=[anywhere] * 7,
        scratch_shapes=scratch,
        compiler_params=pltpu.CompilerParams(collective_id=3, has_side_effects=True, vmem_limit_bytes=40 * 2**20),
        cost_estimate=pl.CostEstimate(flops=10**10, bytes_accessed=30 * 2**20, transcendentals=0),
    )(*halves, *cut)
    full = [out.reshape(plane, 2 * out.shape[2], out.shape[3]) for out in outs[:3]]
    return full, [out.reshape(part.shape) for out, part in zip(outs[3:], parts)]


def take_rows(source, index):
    return jnp.take(source, index, axis=0, mode="clip")


def slot_owners(slot_of_token, slots):
    tokens = slot_of_token.shape[1]
    fine = 64
    token = jnp.arange(tokens, dtype=jnp.int32)
    coarse = (slot_of_token[:, :, None] // fine == jnp.arange(slots // fine, dtype=jnp.int32)).astype(jnp.bfloat16)
    value = jnp.stack([token // 256, token % 256, jnp.ones_like(token)], axis=1).astype(jnp.bfloat16)
    within = (slot_of_token[:, :, None] % fine == jnp.arange(fine, dtype=jnp.int32)).astype(jnp.bfloat16)
    spread = (value[None, :, :, None] * within[:, :, None, :]).reshape(slot_of_token.shape[0], tokens, 3 * fine)
    found = jnp.einsum("lta,ltb->lab", coarse, spread, preferred_element_type=jnp.float32).astype(jnp.int32)
    high, low, used = found[:, :, :fine], found[:, :, fine:2 * fine], found[:, :, 2 * fine:]
    return (high * 256 + low + (1 - used) * tokens).reshape(slot_of_token.shape[0], slots)


def solution(mesh):
    tok_spec = P(ALL_AXES, None)
    route_spec = P(None, ALL_AXES, None)
    exp_spec = P(None, "ep", None, None)
    repl_spec = P(None, None, None)
    ep, dp = mesh.shape["ep"], mesh.shape["dp"]
    members = ep * dp // 2
    to_partner = [(d, (d + members) % (2 * members)) for d in range(2 * members)]
    groups = [[side * members + m for m in range(members)] for side in range(2)]

    def body(act_in, grad_out, slot_ids, gate_vals, w_dense, w_gate, w_up, w_down, ws_gate, ws_up, ws_down):
        tokens, width = act_in.shape
        slots = 2 * tokens
        block = tokens // members
        experts = (w_gate, w_up, w_down)
        shared = (ws_gate, ws_up, ws_down)
        core, local = lax.axis_index("dp") % 2, lax.axis_index("dp") // 2

        def my_half(layer, w):
            rows, columns = w.shape[2] // 2, w.shape[3]
            return lax.dynamic_slice(w, (layer, local, core * rows, 0), (1, 1, rows, columns)).reshape(rows, columns)

        got = [lax.ppermute(my_half(0, w), ALL_AXES, to_partner) for w in experts[:2]]
        halves_two = [my_half(1, w) for w in experts[1:]]

        side = lax.axis_index("ep") // (ep // 2)
        turned = (slot_ids.reshape(2, tokens) + side * tokens) % slots
        owner = slot_owners(turned[1:], slots).reshape(2, members, block)

        def extended(rows):
            return jnp.pad(rows, ((0, 8), (0, 0)))

        def from_slots(layer, back):
            return take_rows(back.reshape(slots, width), turned[layer]).astype(jnp.float32)

        def mix(act, layer):
            return (act.astype(jnp.float32) + dot32(act, w_dense[layer])).astype(jnp.bfloat16)

        def gated(grad, layer):
            return (gate_vals[layer] * grad.astype(jnp.float32)).astype(jnp.bfloat16)

        def go_out(blocks):
            return lax.all_to_all(blocks, ALL_AXES, 0, 0, axis_index_groups=groups)

        grads_two = extended(gated(grad_out, 1))
        grads_two = [take_rows(grads_two, owner[part].reshape(-1)).reshape(members, block, width) for part in range(2)]
        grads_first = go_out(grads_two[1])
        mixed_one = mix(act_in, 0)
        mixed_one, grads_late = lax.optimization_barrier((mixed_one, grads_two[0]))
        recv, act_two, *foreign = forward_exchange(mesh, turned[0:1], gate_vals[0], mixed_one, experts, shared, got)
        act_two, grads_late, halves_two = lax.optimization_barrier((act_two, grads_late, halves_two))
        grads_second = go_out(grads_late)
        got_two = [lax.ppermute(half, ALL_AXES, to_partner) for half in halves_two]
        mixed_two = mix(act_two, 1)

        def finish(layer, act, grad_y, back, shared_dx):
            routed = from_slots(layer, back)
            grad_mixed = (grad_y.astype(jnp.float32) + routed + shared_dx).astype(jnp.bfloat16)
            g_dense = contract_rows(act, grad_mixed).astype(jnp.bfloat16)
            return (grad_mixed.astype(jnp.float32) + contract_cols(grad_mixed, w_dense[layer])).astype(jnp.bfloat16), g_dense

        def gather(half):
            return lax.all_gather(half, "dp", axis=0, tiled=True).reshape((dp // 2, 2 * half.shape[0], half.shape[1]))

        out = backward_exchange(mesh, 1, turned[1:2], [grads_second, grads_first], mixed_two, mixed_two, grad_out, experts, [foreign[3], *got_two], shared)
        shared_two, own_two = out[3:6], out[6:9]
        experts_two = [gather(half) for half in own_two]
        grad_one, dense_two = finish(1, act_two, grad_out, out[0], out[1])
        sums_two = [lax.psum(part, ALL_AXES) for part in (dense_two, *shared_two)]

        out = backward_exchange(mesh, 0, turned[0:1], [recv], gated(grad_one, 0), mixed_one, grad_one, experts, foreign[:3], shared)
        shared_one, own_one = out[3:6], out[6:9]
        grad_act, dense_one = finish(0, act_in, grad_one, out[0], out[1])
        experts_one, sums_one = final_exchange(mesh, own_one, [dense_one, *shared_one])

        expert_out = [jnp.stack(pair) for pair in zip(experts_one, experts_two)]
        sums_out = [jnp.stack(pair) for pair in zip(sums_one, sums_two)]
        return (grad_act, sums_out[0], *expert_out, *sums_out[1:])

    return jax.shard_map(body, mesh=mesh, in_specs=(tok_spec, tok_spec, route_spec, route_spec, repl_spec, exp_spec, exp_spec, exp_spec, repl_spec, repl_spec, repl_spec), out_specs=(tok_spec, repl_spec, exp_spec, exp_spec, exp_spec, repl_spec, repl_spec, repl_spec), check_vma=False)
```

```python
import functools

import jax
import jax.numpy as jnp
from jax import lax
from jax.experimental import pallas as pl
from jax.experimental.pallas import tpu as pltpu
from jax.sharding import PartitionSpec as P


ALL_AXES = ("ep", "dp")
MESH = pl.DeviceIdType.MESH
STEPS = 2
ORDER = (0, 1, 2, 4, 3, 6, 5, 7)
ORDER_CODE = sum(mask * 8**step for step, mask in enumerate(ORDER))


def contract_rows(left, right):
    return lax.dot_general(left, right, (((0,), (0,)), ((), ())), preferred_element_type=jnp.float32)


def contract_cols(left, right):
    return lax.dot_general(left, right, (((1,), (1,)), ((), ())), preferred_element_type=jnp.float32)


def dot32(left, right):
    return jnp.dot(left, right, preferred_element_type=jnp.float32)


class Geometry:
    def __init__(self, ep, dp):
        self.ep, self.dp = ep, dp
        self.chips = (ep // 2) * (dp // 2)
        z, j = lax.axis_index("ep"), lax.axis_index("dp")
        self.core = j % 2
        self.local = j // 2
        self.base = (z // (ep // 2)) * (ep // 2)
        self.chip = (z % (ep // 2)) * (dp // 2) + j // 2
        self.me = 2 * self.chip + self.core
        self.sibling = (z, (j // 2) * 2 + 1 - self.core)
        self.partner = ((z + ep // 2) % ep, j)

    def member(self, index):
        return (self.base + index // self.dp, index % self.dp)

    def across(self, mask):
        total = 0
        for bit in (1, 2, 4):
            total += (self.chip // bit + mask // bit) % 2 * bit
        return total

    def at_step(self, step):
        power = (1 + 7 * (step % 2)) * (1 + 63 * (step // 2 % 2)) * (1 + 4095 * (step // 4))
        return self.across(ORDER_CODE // power % 8)

    def entry_barrier(self):
        barrier = pltpu.get_barrier_semaphore()

        @pl.loop(1, self.chips)
        def _(mask):
            for core in range(2):
                pl.semaphore_signal(barrier, inc=1, device_id=self.member(2 * self.across(mask) + core), device_id_type=MESH)

        for device in (self.sibling, self.partner):
            pl.semaphore_signal(barrier, inc=1, device_id=device, device_id_type=MESH)
        pl.semaphore_wait(barrier, 2 * self.chips)


def one_hot(part, chip, slots, block):
    tokens = slots.shape[1]
    wanted = part * tokens + chip * 2 * block + lax.broadcasted_iota(jnp.int32, (2 * block, tokens), 0)
    return (wanted == slots[...]).astype(jnp.float32).astype(jnp.bfloat16)


class Outbound:
    def __init__(self, geo, part, send, recv, send_sem, recv_sem):
        self.geo, self.part = geo, part
        self.send, self.recv, self.send_sem, self.recv_sem = [ref.at[part] for ref in (send, recv, send_sem, recv_sem)]

    def copy(self, step, core):
        geo = self.geo
        index = 2 * geo.at_step(step) + core
        return pltpu.make_async_remote_copy(src_ref=self.send.at[index], dst_ref=self.recv.at[step, geo.core], send_sem=self.send_sem.at[step, core], recv_sem=self.recv_sem.at[step, geo.core], device_id=geo.member(index), device_id_type=MESH)

    def own(self):
        geo = self.geo
        return pltpu.make_async_copy(self.send.at[geo.me], self.recv.at[0, geo.core], self.recv_sem.at[0, geo.core])

    def pack(self, slots, rows):
        geo = self.geo
        block = self.send.shape[1]

        @pl.loop(0, geo.chips)
        def _(n):
            chip = geo.at_step((n + 1) % geo.chips)
            pick = one_hot(self.part, chip, slots, block)
            self.send[pl.ds(2 * chip, 2)] = dot32(pick, rows[...]).astype(jnp.bfloat16).reshape(2, block, rows.shape[1])
            pl.when(n > 0)(functools.partial(self.issue, n))

        self.own().start()
        self.copy(0, 1 - geo.core).start()

    def issue(self, step):
        for core in range(2):
            self.copy(step, core).start()

    def arrive(self, step):
        for core in range(2):
            pltpu.make_async_copy(self.send.at[0], self.recv.at[step, core], self.recv_sem.at[step, core]).wait()

    def wait_sends(self):
        self.copy(0, 1 - self.geo.core).wait_send()

        @pl.loop(1, self.geo.chips)
        def _(step):
            for core in range(2):
                self.copy(step, core).wait_send()


class Return:
    def __init__(self, geo, rows, back, send_sem, recv_sem):
        self.geo, self.rows, self.back, self.send_sem, self.recv_sem = geo, rows, back, send_sem, recv_sem

    def copy(self, step, core):
        geo = self.geo
        return pltpu.make_async_remote_copy(src_ref=self.rows.at[step, core], dst_ref=self.back.at[geo.me], send_sem=self.send_sem.at[step, core], recv_sem=self.recv_sem.at[geo.me], device_id=geo.member(2 * geo.at_step(step) + core), device_id_type=MESH)

    def start(self, step):
        geo = self.geo

        @pl.when(step == 0)
        def _():
            pltpu.make_async_copy(self.rows.at[0, geo.core], self.back.at[geo.me], self.recv_sem.at[geo.me]).start()
            self.copy(0, 1 - geo.core).start()

        @pl.when(step > 0)
        def _():
            for core in range(2):
                self.copy(step, core).start()

    def wait_sends(self):
        self.copy(0, 1 - self.geo.core).wait_send()

        @pl.loop(1, self.geo.chips)
        def _(step):
            for core in range(2):
                self.copy(step, core).wait_send()

    def wait_back(self, index):
        pltpu.make_async_copy(self.rows.at[0, 0], self.back.at[index], self.recv_sem.at[index]).wait()

    def wait_all(self):
        self.wait_sends()
        pl.loop(0, 2 * self.geo.chips)(self.wait_back)


def half_rows(rows, core):
    return pl.ds(pl.multiple_of(core * (rows // 2), 8), rows // 2)


class WeightSwap:
    def __init__(self, geo, layer, own, foreign, sems, which):
        self.geo, self.layer, self.own, self.foreign, self.sems, self.every = geo, layer, own, foreign, sems, which

    def over(self, which):
        geo = self.geo
        rows = half_rows(self.foreign[which].shape[0], geo.core)
        return pltpu.make_async_remote_copy(src_ref=self.own[which].at[self.layer, geo.local, rows], dst_ref=self.foreign[which].at[rows], send_sem=self.sems.at[0, which], recv_sem=self.sems.at[1, which], device_id=geo.partner, device_id_type=MESH)

    def across(self, which):
        geo = self.geo
        rows = self.foreign[which].at[half_rows(self.foreign[which].shape[0], geo.core)]
        return pltpu.make_async_remote_copy(src_ref=rows, dst_ref=rows, send_sem=self.sems.at[2, which], recv_sem=self.sems.at[3, which], device_id=geo.sibling, device_id_type=MESH)

    def start(self):
        for which in self.every:
            self.over(which).start()

    def pass_on(self):
        for which in self.every:
            self.over(which).wait()
            self.across(which).start()

    def finish(self):
        for which in self.every:
            self.across(which).wait()


def silu(value):
    return value * jax.nn.sigmoid(value)


def forward_kernel(ep, dp, slots, gates, mixed, *refs):
    refs = list(refs)

    def take(count):
        got = refs[:count]
        del refs[:count]
        return got

    experts, ws, got = take(3), take(3), take(1)
    recv_out, act = take(2)
    keep_out, next_out = take(3), take(1)
    send, recv, outs, back, shared, routed = take(6)
    shared_w, own_w, foreign_w = take(3), take(3), take(3)
    go_sem, get_sem, ret_sem, res_sem, swap_sem, down_sem, pass_sem, load_sem, save_sem = refs
    geo = Geometry(ep, dp)
    geo.entry_barrier()
    outbound = [Outbound(geo, part, send, recv, go_sem, get_sem) for part in range(2)]
    returns = [Return(geo, outs.at[part], back.at[part], ret_sem.at[part], res_sem.at[part]) for part in range(2)]
    swap = WeightSwap(geo, 1, experts, next_out, swap_sem, (0,))
    down = WeightSwap(geo, 0, experts, foreign_w, down_sem, (1, 2))
    loads = []
    passes = []
    for which in range(3):
        loads.append(pltpu.make_async_copy(ws[which].at[0], shared_w[which], load_sem.at[0, which]))
        loads.append(pltpu.make_async_copy(experts[which].at[0, geo.local], own_w[which], load_sem.at[1, which]))
    for which in range(1):
        mine = half_rows(foreign_w[which].shape[0], geo.core)
        loads.append(pltpu.make_async_copy(got[which], foreign_w[which].at[mine], load_sem.at[2, which]))
        passes.append(pltpu.make_async_remote_copy(src_ref=got[which], dst_ref=foreign_w[which].at[mine], send_sem=pass_sem.at[0, which], recv_sem=pass_sem.at[1, which], device_id=geo.sibling, device_id_type=MESH))
    down.start()
    for copy in loads + passes:
        copy.start()
    outbound[0].pack(slots, mixed)
    outbound[1].pack(slots, mixed)
    swap.start()

    tile = 2 * STEPS * recv.shape[3]

    def ffn(rows, w_one, w_three, w_two):
        a_one = dot32(rows, w_one[...])
        a_three = dot32(rows, w_three[...])
        hidden = (silu(a_one) * a_three).astype(jnp.bfloat16)
        return dot32(hidden, w_two[...])

    for copy in loads + passes:
        copy.wait()

    @pl.loop(0, mixed.shape[0] // tile)
    def _(t):
        at = pl.ds(pl.multiple_of(t * tile, tile), tile)
        shared[at, :] = ffn(mixed[at, :], *shared_w)

    width = mixed.shape[1]
    for part, weights in enumerate((own_w, foreign_w)):
        if part == 1:
            down.finish()
            keeps = [pltpu.make_async_copy(src, dst, load_sem.at[0, which]) for which, (src, dst) in enumerate(zip(foreign_w, keep_out))]
            for keep in keeps:
                keep.start()

        @pl.loop(0, geo.chips // STEPS)
        def _(t):
            steps = pl.ds(t * STEPS, STEPS)
            for step in range(STEPS):
                outbound[part].arrive(t * STEPS + step)
            pltpu.make_async_copy(recv.at[part, steps], recv_out.at[part, steps], save_sem.at[part, t]).start()
            rows = recv[part, steps].reshape(tile, width)
            outs[part, steps] = ffn(rows, *weights).astype(jnp.bfloat16).reshape(STEPS, 2, tile // (2 * STEPS), width)

            @pl.when(t > 0)
            def _():
                for step in range(STEPS):
                    returns[part].start((t - 1) * STEPS + step)

        for step in range(STEPS):
            returns[part].start(geo.chips - STEPS + step)
        if part == 0:
            down.pass_on()
    swap.pass_on()
    block = send.shape[2]
    routed[...] = jnp.zeros(routed.shape, jnp.float32)
    for part in range(2):

        @pl.loop(0, geo.chips)
        def _(step):
            chip = geo.at_step(step)
            for core in range(2):
                returns[part].wait_back(2 * chip + core)
            came = back[part, pl.ds(2 * chip, 2)].reshape(2 * block, width)
            routed[...] += contract_rows(one_hot(part, chip, slots, block), came)

    @pl.loop(0, mixed.shape[0] // tile)
    def _(t):
        at = pl.ds(pl.multiple_of(t * tile, tile), tile)
        act[at, :] = (mixed[at, :].astype(jnp.float32) + gates[at, :] * routed[at, :] + shared[at, :]).astype(jnp.bfloat16)

    for part in range(2):
        outbound[part].wait_sends()
        returns[part].wait_sends()

        @pl.loop(0, geo.chips // STEPS)
        def _(t):
            steps = pl.ds(t * STEPS, STEPS)
            pltpu.make_async_copy(recv.at[part, steps], recv_out.at[part, steps], save_sem.at[part, t]).wait()

    for keep in keeps:
        keep.wait()
    swap.finish()


def forward_exchange(mesh, slots, gates, mixed, experts, shared, got):
    ep, dp = mesh.shape["ep"], mesh.shape["dp"]
    tokens, width = mixed.shape
    members = ep * dp // 2
    block = tokens // members
    bf16, f32 = jnp.bfloat16, jnp.float32
    shapes = [w.shape[2:] for w in experts]
    hidden = shapes[0][1]
    chips = members // 2
    anywhere = pl.BlockSpec(memory_space=pl.ANY)
    inside = pl.BlockSpec(memory_space=pltpu.VMEM)
    flops = 2 * 3 * width * hidden * (2 * members * block + tokens)
    expert = [jax.ShapeDtypeStruct(s, bf16) for s in shapes]
    dma = pltpu.SemaphoreType.DMA
    return pl.pallas_call(
        functools.partial(forward_kernel, ep, dp),
        name="forward_exchange",
        out_shape=[jax.ShapeDtypeStruct((2, chips, 2, block, width), bf16), jax.ShapeDtypeStruct((tokens, width), bf16)] + expert + expert[:1],
        in_specs=[inside] * 3 + [anywhere] * 7,
        out_specs=[anywhere, inside] + [anywhere] * 4,
        scratch_shapes=[pltpu.VMEM((2, members, block, width), bf16)]
        + [pltpu.VMEM((2, chips, 2, block, width), bf16) for _ in range(2)]
        + [pltpu.VMEM((2, members, block, width), bf16), pltpu.VMEM((tokens, width), f32), pltpu.VMEM((tokens, width), f32)]
        + [pltpu.VMEM(s, bf16) for _ in range(3) for s in shapes]
        + [dma((2, chips, 2)), dma((2, chips, 2)), dma((2, chips, 2)), dma((2, members)), dma((4, 3)), dma((4, 3)), dma((2, 3)), dma((3, 3)), dma((2, chips // STEPS))],
        compiler_params=pltpu.CompilerParams(collective_id=0, has_side_effects=True, vmem_limit_bytes=60 * 2**20),
        cost_estimate=pl.CostEstimate(flops=flops, bytes_accessed=40 * 2**20, transcendentals=0),
    )(slots, gates, mixed, *experts, *shared, *got)


class PairSum:
    def __init__(self, geo, stages, theirs, sems, expert):
        self.geo, self.stages, self.theirs, self.sems, self.expert = geo, stages, theirs, sems, expert

    def mine(self, which):
        return self.stages[which].at[self.expert, half_rows(self.stages[which].shape[1], self.geo.core)]

    def copy(self, which):
        geo = self.geo
        return pltpu.make_async_remote_copy(src_ref=self.stages[which].at[self.expert, half_rows(self.stages[which].shape[1], 1 - geo.core)], dst_ref=self.theirs[which].at[self.expert], send_sem=self.sems.at[0, self.expert, which], recv_sem=self.sems.at[1, self.expert, which], device_id=geo.sibling, device_id_type=MESH)

    def start(self):
        for which in range(3):
            self.copy(which).start()

    def finish(self):
        for which in range(3):
            self.copy(which).wait()
            mine = self.mine(which)
            mine[...] = (mine[...].astype(jnp.float32) + self.theirs[which][self.expert].astype(jnp.float32)).astype(jnp.bfloat16)


def backward_kernel(ep, dp, layer, *refs):
    refs = list(refs)

    def take(count):
        got = refs[:count]
        del refs[:count]
        return got

    slots = take(1)[0]
    held = take(2 if layer else 1)
    rows_in, mixed, grad_y = take(3)
    own_w, foreign_w, shared_w = take(3), take(3), take(3)
    back, grad_mixed, recv = take(3)
    shared_out, own_out = take(3), take(3)
    source, send, x_buf, g_buf, dx_rows, total, came = take(7)
    weights, acc, stages, theirs, partner_in = take(3), take(3), take(3), take(3), take(3)
    go_sem, get_sem, ret_sem, res_sem, partner_sem, load_sem, x_sem, g_sem, dx_sem, pair_sem, pass_sem, came_sem, keep_sem = refs

    geo = Geometry(ep, dp)
    geo.entry_barrier()
    tile = 2 * send.shape[2]
    fill = pltpu.make_async_copy(rows_in, source, dx_sem.at[0])
    fill.start()
    width = mixed.shape[1]
    per_set = mixed.shape[0] // tile
    tiles = 3 * per_set
    outbound = [Outbound(geo, part, send, recv, go_sem, get_sem) for part in range(2)]
    returns = [Return(geo, dx_rows.at[part], back.at[part], ret_sem.at[part], res_sem.at[part]) for part in range(2)]
    pairs = [PairSum(geo, stages, theirs, pair_sem, expert) for expert in range(2)]
    begins = (2 * per_set, 0)
    loads = []
    for which in range(3):
        loads.append(pltpu.make_async_copy(shared_w[which].at[layer], weights[which].at[2], load_sem.at[2, which]))
        loads.append(pltpu.make_async_copy(own_w[which].at[layer, geo.local], weights[which].at[0], load_sem.at[0, which]))
        whole = foreign_w[which].shape == weights[which].shape[1:]
        rows = weights[which].at[1] if whole else weights[which].at[1, half_rows(weights[which].shape[1], geo.core)]
        loads.append(pltpu.make_async_copy(foreign_w[which], rows, load_sem.at[1, which]))
        if not whole:
            loads.append(pltpu.make_async_remote_copy(src_ref=foreign_w[which], dst_ref=rows, send_sem=pass_sem.at[0, which], recv_sem=pass_sem.at[1, which], device_id=geo.sibling, device_id_type=MESH))
    for load in loads:
        load.start()
    fill.wait()
    outbound[1].pack(slots, source)
    outbound[0].pack(slots, source)
    moved, moved_sem, kept, kept_sem = (x_buf, x_sem, g_buf, g_sem) if layer else (g_buf, g_sem, x_buf, x_sem)

    def held_block(part, step, core):
        if layer:
            return held[part].at[2 * geo.at_step(step) + core]
        return held[0].at[part, step, core]

    def fetch(i, slot):
        @pl.when(i // per_set == 1)
        def _():
            at = pl.ds(pl.multiple_of((i - per_set) * tile, tile), tile)
            pltpu.make_async_copy(mixed.at[at], x_buf.at[slot], x_sem.at[slot]).start()
            pltpu.make_async_copy(grad_y.at[at], g_buf.at[slot], g_sem.at[slot]).start()

        for part in range(2):
            begin = begins[part]

            @pl.when((i >= begin) & (i < begin + per_set))
            def _(part=part, begin=begin):
                step = i - begin
                outbound[part].arrive(step)
                for core in range(2):
                    at = pl.ds(core * (tile // 2), tile // 2)
                    pltpu.make_async_copy(recv.at[part, step, core], moved.at[slot, at], moved_sem.at[slot]).start()
                    pltpu.make_async_copy(held_block(part, step, core), kept.at[slot, at], kept_sem.at[slot]).start()

    keeps = [pltpu.make_async_copy(stage.at[0], out, keep_sem.at[n]) for n, (stage, out) in enumerate(zip(stages, shared_out))]

    def partner_copies():
        return [pltpu.make_async_remote_copy(src_ref=pairs[1].mine(which), dst_ref=partner_in[which], send_sem=partner_sem.at[0, which], recv_sem=partner_sem.at[1, which], device_id=geo.partner, device_id_type=MESH) for which in range(3)]

    fetch(0, 0)
    for load in loads:
        load.wait()

    @pl.loop(0, tiles)
    def _(i):
        slot = i % 2
        which_set = (i // per_set + 1) % 3
        fetch(i + 1, (i + 1) % 2)
        pltpu.make_async_copy(mixed.at[pl.ds(0, tile)], x_buf.at[slot], x_sem.at[slot]).wait()
        pltpu.make_async_copy(mixed.at[pl.ds(0, tile)], g_buf.at[slot], g_sem.at[slot]).wait()

        @pl.when(i % per_set == 0)
        def _():
            for a in acc:
                a[...] = jnp.zeros(a.shape, jnp.float32)

        x = x_buf[slot]
        g = g_buf[slot]
        w_one, w_three, w_two = [w.at[which_set] for w in weights]
        a_one = dot32(x, w_one[...])
        a_three = dot32(x, w_three[...])
        grad_hidden = contract_cols(g, w_two[...])
        sigma = jax.nn.sigmoid(a_one)
        gated = a_one * sigma
        hidden = (gated * a_three).astype(jnp.bfloat16)
        grad_one = (grad_hidden * a_three * (sigma * (1.0 + a_one * (1.0 - sigma)))).astype(jnp.bfloat16)
        grad_three = (grad_hidden * gated).astype(jnp.bfloat16)
        acc[0][...] += contract_rows(x, grad_one)
        acc[1][...] += contract_rows(x, grad_three)
        acc[2][...] += contract_rows(hidden, g)
        dx = contract_cols(grad_one, w_one[...]) + contract_cols(grad_three, w_three[...])

        @pl.when(i // per_set == 1)
        def _():
            total[pl.ds(pl.multiple_of((i - per_set) * tile, tile), tile), :] = dx

        @pl.when(i == 2 * per_set - 1)
        def _():
            for a, stage in zip(acc, stages):
                stage[0] = a[...].astype(jnp.bfloat16)

        @pl.when(i == 2 * per_set)
        def _():
            for keep in keeps:
                keep.start()

        @pl.when(i == tiles - 1)
        def _():
            for keep in keeps:
                keep.wait()

        for part in range(2):
            begin = begins[part]

            @pl.when((i >= begin) & (i < begin + per_set))
            def _(part=part, begin=begin):
                dx_rows[part, i - begin] = dx.astype(jnp.bfloat16).reshape(2, tile // 2, width)

            @pl.when((i > begin) & (i <= begin + per_set))
            def _(part=part, begin=begin):
                returns[part].start(i - 1 - begin)

            @pl.when(i == begin + per_set - 1)
            def _(part=part):
                for a, stage in zip(acc, stages):
                    stage[part] = a[...].astype(jnp.bfloat16)

        pl.when(i == per_set)(pairs[1].start)
        pl.when(i == per_set + 1)(pairs[1].finish)

        @pl.when(i == per_set + 2)
        def _():
            for copy in partner_copies():
                copy.start()

    returns[0].start(per_set - 1)
    pairs[0].start()
    pairs[0].finish()

    block = tile // 2

    def bring(part, step):
        chip = geo.at_step(step)
        for core in range(2):
            returns[part].wait_back(2 * chip + core)
            pltpu.make_async_copy(back.at[part, 2 * chip + core], came.at[step % 2, pl.ds(core * block, block)], came_sem.at[step % 2]).start()

    for part in (1, 0):
        bring(part, 0)

        @pl.loop(0, geo.chips)
        def _(step):
            pl.when(step + 1 < geo.chips)(lambda: bring(part, step + 1))
            pltpu.make_async_copy(mixed.at[pl.ds(0, tile)], came.at[step % 2], came_sem.at[step % 2]).wait()
            total[...] += contract_rows(one_hot(part, geo.at_step(step), slots, block), came[step % 2])

    def grad_tile(t):
        return pltpu.make_async_copy(grad_y.at[pl.ds(pl.multiple_of(t * tile, tile), tile)], g_buf.at[t % 2], g_sem.at[t % 2])

    grad_tile(0).start()

    @pl.loop(0, per_set)
    def _(t):
        pl.when(t + 1 < per_set)(lambda: grad_tile(t + 1).start())
        grad_tile(t).wait()
        at = pl.ds(pl.multiple_of(t * tile, tile), tile)
        source[at, :] = (g_buf[t % 2].astype(jnp.float32) + total[at, :]).astype(jnp.bfloat16)

    for which, copy in enumerate(partner_copies()):
        copy.wait()
        own_out[which][...] = (pairs[0].mine(which)[...].astype(jnp.float32) + partner_in[which][...].astype(jnp.float32)).astype(jnp.bfloat16)
    store = pltpu.make_async_copy(source, grad_mixed, dx_sem.at[0])
    store.start()
    for part in range(2):
        outbound[part].wait_sends()
        returns[part].wait_sends()
    store.wait()


def backward_exchange(mesh, layer, slots, held, rows, mixed, grad_y, own, foreign, shared):
    ep, dp = mesh.shape["ep"], mesh.shape["dp"]
    tokens, width = mixed.shape
    members = ep * dp // 2
    block = tokens // members
    chips = members // 2
    tile = 2 * block
    bf16, f32 = jnp.bfloat16, jnp.float32
    anywhere = pl.BlockSpec(memory_space=pl.ANY)
    inside = pl.BlockSpec(memory_space=pltpu.VMEM)
    shapes = [w.shape[2:] for w in own]
    halves = [(s[0] // 2, s[1]) for s in shapes]
    like = jax.ShapeDtypeStruct
    by_step = like((2, chips, 2, block, width), bf16)
    outs = [like((2, members, block, width), bf16), like((tokens, width), bf16), by_step] + [like(s, bf16) for s in shapes + halves]
    vmem = pltpu.VMEM
    scratch = [vmem((tokens, width), bf16), vmem((2, members, block, width), bf16), vmem((2, tile, width), bf16), vmem((2, tile, width), bf16), vmem(by_step.shape, bf16), vmem((tokens, width), f32), vmem((2, tile, width), bf16)]
    scratch += [vmem((3,) + s, bf16) for s in shapes] + [vmem(s, f32) for s in shapes] + [vmem((2,) + s, bf16) for s in shapes]
    scratch += [vmem((2,) + s, bf16) for s in halves] + [vmem(s, bf16) for s in halves]
    dma = pltpu.SemaphoreType.DMA
    scratch += [dma((2, chips, 2)), dma((2, chips, 2)), dma((2, chips, 2)), dma((2, members)), dma((2, 3)), dma((3, 3)), dma((2,)), dma((2,)), dma((2,)), dma((2, 2, 3)), dma((2, 3)), dma((2,)), dma((3,))]
    operands = [slots, *held, rows, mixed, grad_y, *own, *foreign, *shared]
    flops = 2 * 8 * width * shapes[0][1] * (2 * members * block + tokens)
    return pl.pallas_call(
        functools.partial(backward_kernel, ep, dp, layer),
        name="backward_second" if layer else "backward_first",
        out_shape=outs,
        in_specs=[inside] + [anywhere] * (len(operands) - 1),
        out_specs=[anywhere] * 6 + [inside] * 3,
        scratch_shapes=scratch,
        compiler_params=pltpu.CompilerParams(collective_id=1 + layer, has_side_effects=True, vmem_limit_bytes=63 * 2**20),
        cost_estimate=pl.CostEstimate(flops=flops, bytes_accessed=60 * 2**20, transcendentals=0),
    )(*operands)


def final_kernel(ep, dp, *refs):
    refs = list(refs)

    def take(count):
        got = refs[:count]
        del refs[:count]
        return got

    halves, parts = take(3), take(4)
    full, sums = take(3), take(4)
    first, mine, wide, piece, other, last = [take(4) for _ in range(6)]
    load_sem, pair_sem, wide_send, wide_recv, partner_sem, spread_send, spread_recv, cross_sem, gather_sem, local_sem, fold_sem = refs
    geo = Geometry(ep, dp)
    geo.entry_barrier()
    z, core = lax.axis_index("ep"), geo.core
    four, three = range(4), range(3)
    f32, bf16 = jnp.float32, jnp.bfloat16

    to_sibling = [pltpu.make_async_remote_copy(src_ref=parts[n].at[1 - core], dst_ref=first[n], send_sem=pair_sem.at[0, n], recv_sem=pair_sem.at[1, n], device_id=geo.sibling, device_id_type=MESH) for n in four]
    keep = [pltpu.make_async_copy(parts[n].at[core], mine[n], load_sem.at[n]) for n in four]
    for copy in to_sibling + keep:
        copy.start()

    def place(mask):
        return geo.across(mask) % (dp // 2)

    def hop(n, index, src, dst, mask):
        return pltpu.make_async_remote_copy(src_ref=src, dst_ref=dst, send_sem=gather_sem.at[0, n, index], recv_sem=gather_sem.at[1, n, index], device_id=(z, 2 * place(mask) + core), device_id_type=MESH)

    def direct(n, mask):
        return hop(n, mask - 1, halves[n], full[n].at[geo.local, core], mask)

    def relay(n, mask):
        rows = halves[n].shape[0] // 2
        block = full[n].at[place(3 - mask), core, pl.ds((mask - 1) * rows, rows)]
        return hop(n, mask + 1, block, block, mask)

    def fold(n, mask):
        block = full[n].at[place(mask), core]
        return pltpu.make_async_remote_copy(src_ref=halves[n] if mask == 0 else block, dst_ref=block, send_sem=fold_sem.at[0, n, mask], recv_sem=fold_sem.at[1, n, mask], device_id=geo.sibling, device_id_type=MESH)

    local = [pltpu.make_async_copy(halves[n], full[n].at[geo.local, core], local_sem.at[n]) for n in three]

    def gather(n):
        for mask in (1, 2):
            direct(n, mask).start()
        fold(n, 0).start()
        local[n].start()

    def forward(n):
        for mask in (1, 2):
            direct(n, mask).wait()
        for mask in (1, 2):
            relay(n, mask).start()
            fold(n, mask).start()

    gather(2)
    for n in four:
        to_sibling[n].wait()
        keep[n].wait()
        mine[n][...] = (mine[n][...].astype(f32) + first[n][...].astype(f32)).astype(bf16)

    def widen(n, mask):
        to = geo.across(mask)
        return pltpu.make_async_remote_copy(src_ref=mine[n].at[to], dst_ref=wide[n].at[mask], send_sem=wide_send.at[n, mask], recv_sem=wide_recv.at[n, mask], device_id=geo.member(2 * to + core), device_id_type=MESH)

    for n in four:
        for mask in ORDER[1:]:
            widen(n, mask).start()
    gather(0)
    for n in four:
        for mask in ORDER[1:]:
            widen(n, mask).wait()
        total = mine[n][geo.chip].astype(f32)
        for mask in ORDER[1:]:
            total += wide[n][mask].astype(f32)
        piece[n][...] = total.astype(bf16)

    def swap(n):
        return pltpu.make_async_remote_copy(src_ref=piece[n], dst_ref=other[n], send_sem=partner_sem.at[0, n], recv_sem=partner_sem.at[1, n], device_id=geo.partner, device_id_type=MESH)

    for n in four:
        swap(n).start()
    forward(2)
    for n in four:
        swap(n).wait()
        last[n][...] = (piece[n][...].astype(f32) + other[n][...].astype(f32)).astype(bf16)

    def spread(n, mask):
        return pltpu.make_async_remote_copy(src_ref=last[n], dst_ref=sums[n].at[core, geo.chip], send_sem=spread_send.at[n, mask], recv_sem=spread_recv.at[n, mask], device_id=geo.member(2 * geo.across(mask) + core), device_id_type=MESH)

    own = [pltpu.make_async_copy(last[n], sums[n].at[core, geo.chip], load_sem.at[n]) for n in four]
    for n in four:
        own[n].start()
        for mask in ORDER[1:]:
            spread(n, mask).start()
    gather(1)
    forward(0)

    def cross(n):
        return pltpu.make_async_remote_copy(src_ref=sums[n].at[core], dst_ref=sums[n].at[core], send_sem=cross_sem.at[0, n], recv_sem=cross_sem.at[1, n], device_id=geo.sibling, device_id_type=MESH)

    for n in four:
        own[n].wait()
        for mask in ORDER[1:]:
            spread(n, mask).wait()
        cross(n).start()
    forward(1)
    for n in (2, 0, 1):
        for mask in (1, 2):
            relay(n, mask).wait()
        fold(n, 3).start()
    for n in three:
        local[n].wait()
        for mask in range(4):
            fold(n, mask).wait()
    for n in four:
        cross(n).wait()


def final_exchange(mesh, halves, parts):
    ep, dp = mesh.shape["ep"], mesh.shape["dp"]
    chips, plane = ep * dp // 4, dp // 2
    bf16 = jnp.bfloat16
    anywhere = pl.BlockSpec(memory_space=pl.ANY)
    like = jax.ShapeDtypeStruct
    cut = [part.reshape(2, chips, part.shape[0] // (2 * chips), part.shape[1]) for part in parts]
    piece = [c.shape[2:] for c in cut]
    vmem, dma = pltpu.VMEM, pltpu.SemaphoreType.DMA
    scratch = [vmem((chips,) + s, bf16) for _ in range(3) for s in piece] + [vmem(s, bf16) for _ in range(3) for s in piece]
    scratch += [dma((4,)), dma((2, 4)), dma((4, chips)), dma((4, chips)), dma((2, 4)), dma((4, chips)), dma((4, chips)), dma((2, 4)), dma((2, 3, 4)), dma((3,)), dma((2, 3, plane))]
    outs = pl.pallas_call(
        functools.partial(final_kernel, ep, dp),
        name="final_exchange",
        out_shape=[like((plane, 2) + h.shape, bf16) for h in halves] + [like(c.shape, bf16) for c in cut],
        in_specs=[anywhere] * 7,
        out_specs=[anywhere] * 7,
        scratch_shapes=scratch,
        compiler_params=pltpu.CompilerParams(collective_id=3, has_side_effects=True, vmem_limit_bytes=40 * 2**20),
        cost_estimate=pl.CostEstimate(flops=10**10, bytes_accessed=30 * 2**20, transcendentals=0),
    )(*halves, *cut)
    full = [out.reshape(plane, 2 * out.shape[2], out.shape[3]) for out in outs[:3]]
    return full, [out.reshape(part.shape) for out, part in zip(outs[3:], parts)]


def take_rows(source, index):
    return jnp.take(source, index, axis=0, mode="clip")


def slot_owners(slot_of_token, slots):
    tokens = slot_of_token.shape[1]
    fine = 64
    token = jnp.arange(tokens, dtype=jnp.int32)
    coarse = (slot_of_token[:, :, None] // fine == jnp.arange(slots // fine, dtype=jnp.int32)).astype(jnp.bfloat16)
    value = jnp.stack([token // 256, token % 256, jnp.ones_like(token)], axis=1).astype(jnp.bfloat16)
    within = (slot_of_token[:, :, None] % fine == jnp.arange(fine, dtype=jnp.int32)).astype(jnp.bfloat16)
    spread = (value[None, :, :, None] * within[:, :, None, :]).reshape(slot_of_token.shape[0], tokens, 3 * fine)
    found = jnp.einsum("lta,ltb->lab", coarse, spread, preferred_element_type=jnp.float32).astype(jnp.int32)
    high, low, used = found[:, :, :fine], found[:, :, fine:2 * fine], found[:, :, 2 * fine:]
    return (high * 256 + low + (1 - used) * tokens).reshape(slot_of_token.shape[0], slots)


def solution(mesh):
    tok_spec = P(ALL_AXES, None)
    route_spec = P(None, ALL_AXES, None)
    exp_spec = P(None, "ep", None, None)
    repl_spec = P(None, None, None)
    ep, dp = mesh.shape["ep"], mesh.shape["dp"]
    members = ep * dp // 2
    to_partner = [(d, (d + members) % (2 * members)) for d in range(2 * members)]
    groups = [[side * members + m for m in range(members)] for side in range(2)]

    def body(act_in, grad_out, slot_ids, gate_vals, w_dense, w_gate, w_up, w_down, ws_gate, ws_up, ws_down):
        tokens, width = act_in.shape
        slots = 2 * tokens
        block = tokens // members
        experts = (w_gate, w_up, w_down)
        shared = (ws_gate, ws_up, ws_down)
        core, local = lax.axis_index("dp") % 2, lax.axis_index("dp") // 2

        def my_half(layer, w):
            rows, columns = w.shape[2] // 2, w.shape[3]
            return lax.dynamic_slice(w, (layer, local, core * rows, 0), (1, 1, rows, columns)).reshape(rows, columns)

        got = [lax.ppermute(my_half(0, w), ALL_AXES, to_partner) for w in experts[:1]]
        halves_two = [my_half(1, w) for w in experts[1:]]

        side = lax.axis_index("ep") // (ep // 2)
        turned = (slot_ids.reshape(2, tokens) + side * tokens) % slots
        owner = slot_owners(turned[1:], slots).reshape(2, members, block)

        def extended(rows):
            return jnp.pad(rows, ((0, 8), (0, 0)))

        def mix(act, layer):
            return (act.astype(jnp.float32) + dot32(act, w_dense[layer])).astype(jnp.bfloat16)

        def gated(grad, layer):
            return (gate_vals[layer] * grad.astype(jnp.float32)).astype(jnp.bfloat16)

        def go_out(blocks):
            return lax.all_to_all(blocks, ALL_AXES, 0, 0, axis_index_groups=groups)

        grads_two = extended(gated(grad_out, 1))
        grads_first = go_out(take_rows(grads_two, owner[1].reshape(-1)).reshape(members, block, width))
        mixed_one = mix(act_in, 0)
        recv, act_two, *foreign = forward_exchange(mesh, turned[0:1], gate_vals[0], mixed_one, experts, shared, got)
        act_two, grads_two, halves_two = lax.optimization_barrier((act_two, grads_two, halves_two))
        grads_second = go_out(take_rows(grads_two, owner[0].reshape(-1)).reshape(members, block, width))
        got_two = [lax.ppermute(half, ALL_AXES, to_partner) for half in halves_two]
        mixed_two = mix(act_two, 1)

        def finish(layer, act, grad_mixed):
            g_dense = contract_rows(act, grad_mixed).astype(jnp.bfloat16)
            return (grad_mixed.astype(jnp.float32) + contract_cols(grad_mixed, w_dense[layer])).astype(jnp.bfloat16), g_dense

        def gather(half):
            return lax.all_gather(half, "dp", axis=0, tiled=True).reshape((dp // 2, 2 * half.shape[0], half.shape[1]))

        out = backward_exchange(mesh, 1, turned[1:2], [grads_second, grads_first], mixed_two, mixed_two, grad_out, experts, [foreign[3], *got_two], shared)
        shared_two, own_two = out[3:6], out[6:9]
        experts_two = [gather(half) for half in own_two]
        grad_one, dense_two = finish(1, act_two, out[1])
        sums_two = [lax.psum(part, ALL_AXES) for part in (dense_two, *shared_two)]

        out = backward_exchange(mesh, 0, turned[0:1], [recv], gated(grad_one, 0), mixed_one, grad_one, experts, foreign[:3], shared)
        shared_one, own_one = out[3:6], out[6:9]
        grad_act, dense_one = finish(0, act_in, out[1])
        experts_one, sums_one = final_exchange(mesh, own_one, [dense_one, *shared_one])

        expert_out = [jnp.stack(pair) for pair in zip(experts_one, experts_two)]
        sums_out = [jnp.stack(pair) for pair in zip(sums_one, sums_two)]
        return (grad_act, sums_out[0], *expert_out, *sums_out[1:])

    return jax.shard_map(body, mesh=mesh, in_specs=(tok_spec, tok_spec, route_spec, route_spec, repl_spec, exp_spec, exp_spec, exp_spec, repl_spec, repl_spec, repl_spec), out_specs=(tok_spec, repl_spec, exp_spec, exp_spec, exp_spec, repl_spec, repl_spec, repl_spec), check_vma=False)
```

```python
import functools

import jax
import jax.numpy as jnp
from jax import lax
from jax.experimental import pallas as pl
from jax.experimental.pallas import tpu as pltpu
from jax.sharding import PartitionSpec as P


ALL_AXES = ("ep", "dp")
MESH = pl.DeviceIdType.MESH
STEPS = 2
ORDER = (0, 1, 2, 4, 3, 6, 5, 7)
ORDER_CODE = sum(mask * 8**step for step, mask in enumerate(ORDER))


def contract_rows(left, right):
    return lax.dot_general(left, right, (((0,), (0,)), ((), ())), preferred_element_type=jnp.float32)


def contract_cols(left, right):
    return lax.dot_general(left, right, (((1,), (1,)), ((), ())), preferred_element_type=jnp.float32)


def dot32(left, right):
    return jnp.dot(left, right, preferred_element_type=jnp.float32)


class Geometry:
    def __init__(self, ep, dp):
        self.ep, self.dp = ep, dp
        self.chips = (ep // 2) * (dp // 2)
        z, j = lax.axis_index("ep"), lax.axis_index("dp")
        self.core = j % 2
        self.local = j // 2
        self.base = (z // (ep // 2)) * (ep // 2)
        self.chip = (z % (ep // 2)) * (dp // 2) + j // 2
        self.me = 2 * self.chip + self.core
        self.sibling = (z, (j // 2) * 2 + 1 - self.core)
        self.partner = ((z + ep // 2) % ep, j)

    def member(self, index):
        return (self.base + index // self.dp, index % self.dp)

    def across(self, mask):
        total = 0
        for bit in (1, 2, 4):
            total += (self.chip // bit + mask // bit) % 2 * bit
        return total

    def at_step(self, step):
        power = (1 + 7 * (step % 2)) * (1 + 63 * (step // 2 % 2)) * (1 + 4095 * (step // 4))
        return self.across(ORDER_CODE // power % 8)

    def entry_barrier(self):
        barrier = pltpu.get_barrier_semaphore()

        @pl.loop(1, self.chips)
        def _(mask):
            for core in range(2):
                pl.semaphore_signal(barrier, inc=1, device_id=self.member(2 * self.across(mask) + core), device_id_type=MESH)

        for device in (self.sibling, self.partner):
            pl.semaphore_signal(barrier, inc=1, device_id=device, device_id_type=MESH)
        pl.semaphore_wait(barrier, 2 * self.chips)


def one_hot(part, chip, slots, block):
    tokens = slots.shape[1]
    wanted = part * tokens + chip * 2 * block + lax.broadcasted_iota(jnp.int32, (2 * block, tokens), 0)
    return (wanted == slots[...]).astype(jnp.float32).astype(jnp.bfloat16)


class Outbound:
    def __init__(self, geo, part, send, recv, send_sem, recv_sem):
        self.geo, self.part = geo, part
        self.send, self.recv, self.send_sem, self.recv_sem = [ref.at[part] for ref in (send, recv, send_sem, recv_sem)]

    def copy(self, step, core):
        geo = self.geo
        index = 2 * geo.at_step(step) + core
        return pltpu.make_async_remote_copy(src_ref=self.send.at[index], dst_ref=self.recv.at[step, geo.core], send_sem=self.send_sem.at[step, core], recv_sem=self.recv_sem.at[step, geo.core], device_id=geo.member(index), device_id_type=MESH)

    def own(self):
        geo = self.geo
        return pltpu.make_async_copy(self.send.at[geo.me], self.recv.at[0, geo.core], self.recv_sem.at[0, geo.core])

    def pack(self, slots, rows):
        geo = self.geo
        block = self.send.shape[1]

        @pl.loop(0, geo.chips)
        def _(n):
            chip = geo.at_step((n + 1) % geo.chips)
            pick = one_hot(self.part, chip, slots, block)
            self.send[pl.ds(2 * chip, 2)] = dot32(pick, rows[...]).astype(jnp.bfloat16).reshape(2, block, rows.shape[1])
            pl.when(n > 0)(functools.partial(self.issue, n))

        self.own().start()
        self.copy(0, 1 - geo.core).start()

    def issue(self, step):
        for core in range(2):
            self.copy(step, core).start()

    def arrive(self, step):
        for core in range(2):
            pltpu.make_async_copy(self.send.at[0], self.recv.at[step, core], self.recv_sem.at[step, core]).wait()

    def wait_sends(self):
        self.copy(0, 1 - self.geo.core).wait_send()

        @pl.loop(1, self.geo.chips)
        def _(step):
            for core in range(2):
                self.copy(step, core).wait_send()


class Return:
    def __init__(self, geo, rows, back, send_sem, recv_sem):
        self.geo, self.rows, self.back, self.send_sem, self.recv_sem = geo, rows, back, send_sem, recv_sem

    def copy(self, step, core):
        geo = self.geo
        return pltpu.make_async_remote_copy(src_ref=self.rows.at[step, core], dst_ref=self.back.at[geo.me], send_sem=self.send_sem.at[step, core], recv_sem=self.recv_sem.at[geo.me], device_id=geo.member(2 * geo.at_step(step) + core), device_id_type=MESH)

    def start(self, step):
        geo = self.geo

        @pl.when(step == 0)
        def _():
            pltpu.make_async_copy(self.rows.at[0, geo.core], self.back.at[geo.me], self.recv_sem.at[geo.me]).start()
            self.copy(0, 1 - geo.core).start()

        @pl.when(step > 0)
        def _():
            for core in range(2):
                self.copy(step, core).start()

    def wait_sends(self):
        self.copy(0, 1 - self.geo.core).wait_send()

        @pl.loop(1, self.geo.chips)
        def _(step):
            for core in range(2):
                self.copy(step, core).wait_send()

    def wait_back(self, index):
        pltpu.make_async_copy(self.rows.at[0, 0], self.back.at[index], self.recv_sem.at[index]).wait()

    def wait_all(self):
        self.wait_sends()
        pl.loop(0, 2 * self.geo.chips)(self.wait_back)


def half_rows(rows, core):
    return pl.ds(pl.multiple_of(core * (rows // 2), 8), rows // 2)


class WeightSwap:
    def __init__(self, geo, layer, own, foreign, sems, which):
        self.geo, self.layer, self.own, self.foreign, self.sems, self.every = geo, layer, own, foreign, sems, which

    def over(self, which):
        geo = self.geo
        rows = half_rows(self.foreign[which].shape[0], geo.core)
        return pltpu.make_async_remote_copy(src_ref=self.own[which].at[self.layer, geo.local, rows], dst_ref=self.foreign[which].at[rows], send_sem=self.sems.at[0, which], recv_sem=self.sems.at[1, which], device_id=geo.partner, device_id_type=MESH)

    def across(self, which):
        geo = self.geo
        rows = self.foreign[which].at[half_rows(self.foreign[which].shape[0], geo.core)]
        return pltpu.make_async_remote_copy(src_ref=rows, dst_ref=rows, send_sem=self.sems.at[2, which], recv_sem=self.sems.at[3, which], device_id=geo.sibling, device_id_type=MESH)

    def start(self):
        for which in self.every:
            self.over(which).start()

    def pass_on(self):
        for which in self.every:
            self.over(which).wait()
            self.across(which).start()

    def finish(self):
        for which in self.every:
            self.across(which).wait()


def silu(value):
    return value * jax.nn.sigmoid(value)


def forward_kernel(ep, dp, slots, gates, mixed, *refs):
    refs = list(refs)

    def take(count):
        got = refs[:count]
        del refs[:count]
        return got

    experts, ws, got = take(3), take(3), take(1)
    recv_out, act = take(2)
    keep_out, next_out = take(3), take(1)
    send, recv, outs, back, shared, routed = take(6)
    shared_w, own_w, foreign_w = take(3), take(3), take(3)
    go_sem, get_sem, ret_sem, res_sem, swap_sem, down_sem, pass_sem, load_sem, save_sem = refs
    geo = Geometry(ep, dp)
    geo.entry_barrier()
    outbound = [Outbound(geo, part, send, recv, go_sem, get_sem) for part in range(2)]
    returns = [Return(geo, outs.at[part], back.at[part], ret_sem.at[part], res_sem.at[part]) for part in range(2)]
    swap = WeightSwap(geo, 1, experts, next_out, swap_sem, (0,))
    down = WeightSwap(geo, 0, experts, foreign_w, down_sem, (1, 2))
    loads = []
    passes = []
    for which in range(3):
        loads.append(pltpu.make_async_copy(ws[which].at[0], shared_w[which], load_sem.at[0, which]))
        loads.append(pltpu.make_async_copy(experts[which].at[0, geo.local], own_w[which], load_sem.at[1, which]))
    for which in range(1):
        mine = half_rows(foreign_w[which].shape[0], geo.core)
        loads.append(pltpu.make_async_copy(got[which], foreign_w[which].at[mine], load_sem.at[2, which]))
        passes.append(pltpu.make_async_remote_copy(src_ref=got[which], dst_ref=foreign_w[which].at[mine], send_sem=pass_sem.at[0, which], recv_sem=pass_sem.at[1, which], device_id=geo.sibling, device_id_type=MESH))
    down.start()
    for copy in loads + passes:
        copy.start()
    outbound[0].pack(slots, mixed)
    outbound[1].pack(slots, mixed)
    swap.start()

    tile = 2 * STEPS * recv.shape[3]

    def ffn(rows, w_one, w_three, w_two):
        a_one = dot32(rows, w_one[...])
        a_three = dot32(rows, w_three[...])
        hidden = (silu(a_one) * a_three).astype(jnp.bfloat16)
        return dot32(hidden, w_two[...])

    for copy in loads + passes:
        copy.wait()

    @pl.loop(0, mixed.shape[0] // tile)
    def _(t):
        at = pl.ds(pl.multiple_of(t * tile, tile), tile)
        shared[at, :] = ffn(mixed[at, :], *shared_w)

    width = mixed.shape[1]
    for part, weights in enumerate((own_w, foreign_w)):
        if part == 1:
            down.finish()
            keeps = [pltpu.make_async_copy(src, dst, load_sem.at[0, which]) for which, (src, dst) in enumerate(zip(foreign_w, keep_out))]
            for keep in keeps:
                keep.start()

        @pl.loop(0, geo.chips // STEPS)
        def _(t):
            steps = pl.ds(t * STEPS, STEPS)
            for step in range(STEPS):
                outbound[part].arrive(t * STEPS + step)
            pltpu.make_async_copy(recv.at[part, steps], recv_out.at[part, steps], save_sem.at[part, t]).start()
            rows = recv[part, steps].reshape(tile, width)
            outs[part, steps] = ffn(rows, *weights).astype(jnp.bfloat16).reshape(STEPS, 2, tile // (2 * STEPS), width)

            @pl.when(t > 0)
            def _():
                for step in range(STEPS):
                    returns[part].start((t - 1) * STEPS + step)

        for step in range(STEPS):
            returns[part].start(geo.chips - STEPS + step)
        if part == 0:
            down.pass_on()
    swap.pass_on()
    block = send.shape[2]
    routed[...] = jnp.zeros(routed.shape, jnp.float32)
    for part in range(2):

        @pl.loop(0, geo.chips)
        def _(step):
            chip = geo.at_step(step)
            for core in range(2):
                returns[part].wait_back(2 * chip + core)
            came = back[part, pl.ds(2 * chip, 2)].reshape(2 * block, width)
            routed[...] += contract_rows(one_hot(part, chip, slots, block), came)

    @pl.loop(0, mixed.shape[0] // tile)
    def _(t):
        at = pl.ds(pl.multiple_of(t * tile, tile), tile)
        act[at, :] = (mixed[at, :].astype(jnp.float32) + gates[at, :] * routed[at, :] + shared[at, :]).astype(jnp.bfloat16)

    for part in range(2):
        outbound[part].wait_sends()
        returns[part].wait_sends()

        @pl.loop(0, geo.chips // STEPS)
        def _(t):
            steps = pl.ds(t * STEPS, STEPS)
            pltpu.make_async_copy(recv.at[part, steps], recv_out.at[part, steps], save_sem.at[part, t]).wait()

    for keep in keeps:
        keep.wait()
    swap.finish()


def forward_exchange(mesh, slots, gates, mixed, experts, shared, got):
    ep, dp = mesh.shape["ep"], mesh.shape["dp"]
    tokens, width = mixed.shape
    members = ep * dp // 2
    block = tokens // members
    bf16, f32 = jnp.bfloat16, jnp.float32
    shapes = [w.shape[2:] for w in experts]
    hidden = shapes[0][1]
    chips = members // 2
    anywhere = pl.BlockSpec(memory_space=pl.ANY)
    inside = pl.BlockSpec(memory_space=pltpu.VMEM)
    flops = 2 * 3 * width * hidden * (2 * members * block + tokens)
    expert = [jax.ShapeDtypeStruct(s, bf16) for s in shapes]
    dma = pltpu.SemaphoreType.DMA
    return pl.pallas_call(
        functools.partial(forward_kernel, ep, dp),
        name="forward_exchange",
        out_shape=[jax.ShapeDtypeStruct((2, chips, 2, block, width), bf16), jax.ShapeDtypeStruct((tokens, width), bf16)] + expert + expert[:1],
        in_specs=[inside] * 3 + [anywhere] * 7,
        out_specs=[anywhere, inside] + [anywhere] * 4,
        scratch_shapes=[pltpu.VMEM((2, members, block, width), bf16)]
        + [pltpu.VMEM((2, chips, 2, block, width), bf16) for _ in range(2)]
        + [pltpu.VMEM((2, members, block, width), bf16), pltpu.VMEM((tokens, width), f32), pltpu.VMEM((tokens, width), f32)]
        + [pltpu.VMEM(s, bf16) for _ in range(3) for s in shapes]
        + [dma((2, chips, 2)), dma((2, chips, 2)), dma((2, chips, 2)), dma((2, members)), dma((4, 3)), dma((4, 3)), dma((2, 3)), dma((3, 3)), dma((2, chips // STEPS))],
        compiler_params=pltpu.CompilerParams(collective_id=0, has_side_effects=True, vmem_limit_bytes=60 * 2**20),
        cost_estimate=pl.CostEstimate(flops=flops, bytes_accessed=40 * 2**20, transcendentals=0),
    )(slots, gates, mixed, *experts, *shared, *got)


class PairSum:
    def __init__(self, geo, stages, theirs, sems, expert):
        self.geo, self.stages, self.theirs, self.sems, self.expert = geo, stages, theirs, sems, expert

    def mine(self, which):
        return self.stages[which].at[self.expert, half_rows(self.stages[which].shape[1], self.geo.core)]

    def copy(self, which):
        geo = self.geo
        return pltpu.make_async_remote_copy(src_ref=self.stages[which].at[self.expert, half_rows(self.stages[which].shape[1], 1 - geo.core)], dst_ref=self.theirs[which].at[self.expert], send_sem=self.sems.at[0, self.expert, which], recv_sem=self.sems.at[1, self.expert, which], device_id=geo.sibling, device_id_type=MESH)

    def start(self):
        for which in range(3):
            self.copy(which).start()

    def finish(self):
        for which in range(3):
            self.copy(which).wait()
            mine = self.mine(which)
            mine[...] = (mine[...].astype(jnp.float32) + self.theirs[which][self.expert].astype(jnp.float32)).astype(jnp.bfloat16)


def backward_kernel(ep, dp, layer, *refs):
    refs = list(refs)

    def take(count):
        got = refs[:count]
        del refs[:count]
        return got

    slots = take(1)[0]
    held = take(2 if layer else 1)
    rows_in, mixed, grad_y = take(3)
    own_w, foreign_w, shared_w = take(3), take(3), take(3)
    back, grad_mixed, recv = take(3)
    shared_out, own_out = take(3), take(3)
    source, send, x_buf, g_buf, dx_rows, total, came = take(7)
    weights, acc, stages, theirs, partner_in = take(3), take(3), take(3), take(3), take(3)
    go_sem, get_sem, ret_sem, res_sem, partner_sem, load_sem, x_sem, g_sem, dx_sem, pair_sem, pass_sem, came_sem, keep_sem = refs

    geo = Geometry(ep, dp)
    geo.entry_barrier()
    tile = 2 * send.shape[2]
    fill = pltpu.make_async_copy(rows_in, source, dx_sem.at[0])
    fill.start()
    width = mixed.shape[1]
    per_set = mixed.shape[0] // tile
    tiles = 3 * per_set
    outbound = [Outbound(geo, part, send, recv, go_sem, get_sem) for part in range(2)]
    returns = [Return(geo, dx_rows.at[part], back.at[part], ret_sem.at[part], res_sem.at[part]) for part in range(2)]
    pairs = [PairSum(geo, stages, theirs, pair_sem, expert) for expert in range(2)]
    begins = (2 * per_set, 0)
    loads = []
    for which in range(3):
        loads.append(pltpu.make_async_copy(shared_w[which].at[layer], weights[which].at[2], load_sem.at[2, which]))
        loads.append(pltpu.make_async_copy(own_w[which].at[layer, geo.local], weights[which].at[0], load_sem.at[0, which]))
        whole = foreign_w[which].shape == weights[which].shape[1:]
        rows = weights[which].at[1] if whole else weights[which].at[1, half_rows(weights[which].shape[1], geo.core)]
        loads.append(pltpu.make_async_copy(foreign_w[which], rows, load_sem.at[1, which]))
        if not whole:
            loads.append(pltpu.make_async_remote_copy(src_ref=foreign_w[which], dst_ref=rows, send_sem=pass_sem.at[0, which], recv_sem=pass_sem.at[1, which], device_id=geo.sibling, device_id_type=MESH))
    for load in loads:
        load.start()
    fill.wait()
    outbound[1].pack(slots, source)
    outbound[0].pack(slots, source)
    moved, moved_sem, kept, kept_sem = (x_buf, x_sem, g_buf, g_sem) if layer else (g_buf, g_sem, x_buf, x_sem)

    def held_block(part, step, core):
        if layer:
            return held[part].at[2 * geo.at_step(step) + core]
        return held[0].at[part, step, core]

    def fetch(i, slot):
        @pl.when(i // per_set == 1)
        def _():
            at = pl.ds(pl.multiple_of((i - per_set) * tile, tile), tile)
            pltpu.make_async_copy(mixed.at[at], x_buf.at[slot], x_sem.at[slot]).start()
            pltpu.make_async_copy(grad_y.at[at], g_buf.at[slot], g_sem.at[slot]).start()

        for part in range(2):
            begin = begins[part]

            @pl.when((i >= begin) & (i < begin + per_set))
            def _(part=part, begin=begin):
                step = i - begin
                outbound[part].arrive(step)
                for core in range(2):
                    at = pl.ds(core * (tile // 2), tile // 2)
                    pltpu.make_async_copy(recv.at[part, step, core], moved.at[slot, at], moved_sem.at[slot]).start()
                    pltpu.make_async_copy(held_block(part, step, core), kept.at[slot, at], kept_sem.at[slot]).start()

    keeps = [pltpu.make_async_copy(stage.at[0], out, keep_sem.at[n]) for n, (stage, out) in enumerate(zip(stages, shared_out))]

    def partner_copies():
        return [pltpu.make_async_remote_copy(src_ref=pairs[1].mine(which), dst_ref=partner_in[which], send_sem=partner_sem.at[0, which], recv_sem=partner_sem.at[1, which], device_id=geo.partner, device_id_type=MESH) for which in range(3)]

    fetch(0, 0)
    for load in loads:
        load.wait()

    @pl.loop(0, tiles)
    def _(i):
        slot = i % 2
        which_set = (i // per_set + 1) % 3
        fetch(i + 1, (i + 1) % 2)
        pltpu.make_async_copy(mixed.at[pl.ds(0, tile)], x_buf.at[slot], x_sem.at[slot]).wait()
        pltpu.make_async_copy(mixed.at[pl.ds(0, tile)], g_buf.at[slot], g_sem.at[slot]).wait()

        @pl.when(i % per_set == 0)
        def _():
            for a in acc:
                a[...] = jnp.zeros(a.shape, jnp.float32)

        x = x_buf[slot]
        g = g_buf[slot]
        w_one, w_three, w_two = [w.at[which_set] for w in weights]
        a_one = dot32(x, w_one[...])
        a_three = dot32(x, w_three[...])
        grad_hidden = contract_cols(g, w_two[...])
        sigma = jax.nn.sigmoid(a_one)
        gated = a_one * sigma
        hidden = (gated * a_three).astype(jnp.bfloat16)
        grad_one = (grad_hidden * a_three * (sigma * (1.0 + a_one * (1.0 - sigma)))).astype(jnp.bfloat16)
        grad_three = (grad_hidden * gated).astype(jnp.bfloat16)
        acc[0][...] += contract_rows(x, grad_one)
        acc[1][...] += contract_rows(x, grad_three)
        acc[2][...] += contract_rows(hidden, g)
        dx = contract_cols(grad_one, w_one[...]) + contract_cols(grad_three, w_three[...])

        @pl.when(i // per_set == 1)
        def _():
            total[pl.ds(pl.multiple_of((i - per_set) * tile, tile), tile), :] = dx

        @pl.when(i == 2 * per_set - 1)
        def _():
            for a, stage in zip(acc, stages):
                stage[0] = a[...].astype(jnp.bfloat16)

        @pl.when(i == 2 * per_set)
        def _():
            for keep in keeps:
                keep.start()

        @pl.when(i == tiles - 1)
        def _():
            for keep in keeps:
                keep.wait()

        for part in range(2):
            begin = begins[part]

            @pl.when((i >= begin) & (i < begin + per_set))
            def _(part=part, begin=begin):
                dx_rows[part, i - begin] = dx.astype(jnp.bfloat16).reshape(2, tile // 2, width)

            @pl.when((i > begin) & (i <= begin + per_set))
            def _(part=part, begin=begin):
                returns[part].start(i - 1 - begin)

            @pl.when(i == begin + per_set - 1)
            def _(part=part):
                for a, stage in zip(acc, stages):
                    stage[part] = a[...].astype(jnp.bfloat16)

        pl.when(i == per_set)(pairs[1].start)
        pl.when(i == per_set + 1)(pairs[1].finish)

        @pl.when(i == per_set + 2)
        def _():
            for copy in partner_copies():
                copy.start()

    returns[0].start(per_set - 1)
    pairs[0].start()
    pairs[0].finish()

    block = tile // 2

    def bring(part, step):
        chip = geo.at_step(step)
        for core in range(2):
            returns[part].wait_back(2 * chip + core)
            pltpu.make_async_copy(back.at[part, 2 * chip + core], came.at[step % 2, pl.ds(core * block, block)], came_sem.at[step % 2]).start()

    for part in (1, 0):
        bring(part, 0)

        @pl.loop(0, geo.chips)
        def _(step):
            pl.when(step + 1 < geo.chips)(lambda: bring(part, step + 1))
            pltpu.make_async_copy(mixed.at[pl.ds(0, tile)], came.at[step % 2], came_sem.at[step % 2]).wait()
            total[...] += contract_rows(one_hot(part, geo.at_step(step), slots, block), came[step % 2])

    def grad_tile(t):
        return pltpu.make_async_copy(grad_y.at[pl.ds(pl.multiple_of(t * tile, tile), tile)], g_buf.at[t % 2], g_sem.at[t % 2])

    grad_tile(0).start()

    @pl.loop(0, per_set)
    def _(t):
        pl.when(t + 1 < per_set)(lambda: grad_tile(t + 1).start())
        grad_tile(t).wait()
        at = pl.ds(pl.multiple_of(t * tile, tile), tile)
        source[at, :] = (g_buf[t % 2].astype(jnp.float32) + total[at, :]).astype(jnp.bfloat16)

    for which, copy in enumerate(partner_copies()):
        copy.wait()
        own_out[which][...] = (pairs[0].mine(which)[...].astype(jnp.float32) + partner_in[which][...].astype(jnp.float32)).astype(jnp.bfloat16)
    store = pltpu.make_async_copy(source, grad_mixed, dx_sem.at[0])
    store.start()
    for part in range(2):
        outbound[part].wait_sends()
        returns[part].wait_sends()
    store.wait()


def backward_exchange(mesh, layer, slots, held, rows, mixed, grad_y, own, foreign, shared):
    ep, dp = mesh.shape["ep"], mesh.shape["dp"]
    tokens, width = mixed.shape
    members = ep * dp // 2
    block = tokens // members
    chips = members // 2
    tile = 2 * block
    bf16, f32 = jnp.bfloat16, jnp.float32
    anywhere = pl.BlockSpec(memory_space=pl.ANY)
    inside = pl.BlockSpec(memory_space=pltpu.VMEM)
    shapes = [w.shape[2:] for w in own]
    halves = [(s[0] // 2, s[1]) for s in shapes]
    like = jax.ShapeDtypeStruct
    by_step = like((2, chips, 2, block, width), bf16)
    outs = [like((2, members, block, width), bf16), like((tokens, width), bf16), by_step] + [like(s, bf16) for s in shapes + halves]
    vmem = pltpu.VMEM
    scratch = [vmem((tokens, width), bf16), vmem((2, members, block, width), bf16), vmem((2, tile, width), bf16), vmem((2, tile, width), bf16), vmem(by_step.shape, bf16), vmem((tokens, width), f32), vmem((2, tile, width), bf16)]
    scratch += [vmem((3,) + s, bf16) for s in shapes] + [vmem(s, f32) for s in shapes] + [vmem((2,) + s, bf16) for s in shapes]
    scratch += [vmem((2,) + s, bf16) for s in halves] + [vmem(s, bf16) for s in halves]
    dma = pltpu.SemaphoreType.DMA
    scratch += [dma((2, chips, 2)), dma((2, chips, 2)), dma((2, chips, 2)), dma((2, members)), dma((2, 3)), dma((3, 3)), dma((2,)), dma((2,)), dma((2,)), dma((2, 2, 3)), dma((2, 3)), dma((2,)), dma((3,))]
    operands = [slots, *held, rows, mixed, grad_y, *own, *foreign, *shared]
    flops = 2 * 8 * width * shapes[0][1] * (2 * members * block + tokens)
    return pl.pallas_call(
        functools.partial(backward_kernel, ep, dp, layer),
        name="backward_second" if layer else "backward_first",
        out_shape=outs,
        in_specs=[inside] + [anywhere] * (len(operands) - 1),
        out_specs=[anywhere] * 6 + [inside] * 3,
        scratch_shapes=scratch,
        compiler_params=pltpu.CompilerParams(collective_id=1 + layer, has_side_effects=True, vmem_limit_bytes=63 * 2**20),
        cost_estimate=pl.CostEstimate(flops=flops, bytes_accessed=60 * 2**20, transcendentals=0),
    )(*operands)


def final_kernel(ep, dp, *refs):
    refs = list(refs)

    def take(count):
        got = refs[:count]
        del refs[:count]
        return got

    halves, parts = take(3), take(4)
    full, sums = take(3), take(4)
    first, mine, wide, piece, other, last = [take(4) for _ in range(6)]
    load_sem, pair_sem, wide_send, wide_recv, partner_sem, spread_send, spread_recv, cross_sem, gather_sem, local_sem, fold_sem = refs
    geo = Geometry(ep, dp)
    geo.entry_barrier()
    z, core = lax.axis_index("ep"), geo.core
    four, three = range(4), range(3)
    f32, bf16 = jnp.float32, jnp.bfloat16

    to_sibling = [pltpu.make_async_remote_copy(src_ref=parts[n].at[1 - core], dst_ref=first[n], send_sem=pair_sem.at[0, n], recv_sem=pair_sem.at[1, n], device_id=geo.sibling, device_id_type=MESH) for n in four]
    keep = [pltpu.make_async_copy(parts[n].at[core], mine[n], load_sem.at[n]) for n in four]
    for copy in to_sibling + keep:
        copy.start()

    def place(mask):
        return geo.across(mask) % (dp // 2)

    def hop(n, index, src, dst, mask):
        return pltpu.make_async_remote_copy(src_ref=src, dst_ref=dst, send_sem=gather_sem.at[0, n, index], recv_sem=gather_sem.at[1, n, index], device_id=(z, 2 * place(mask) + core), device_id_type=MESH)

    def direct(n, mask):
        return hop(n, mask - 1, halves[n], full[n].at[geo.local, core], mask)

    def relay(n, mask):
        rows = halves[n].shape[0] // 2
        block = full[n].at[place(3 - mask), core, pl.ds((mask - 1) * rows, rows)]
        return hop(n, mask + 1, block, block, mask)

    def fold(n, mask):
        block = full[n].at[place(mask), core]
        return pltpu.make_async_remote_copy(src_ref=halves[n] if mask == 0 else block, dst_ref=block, send_sem=fold_sem.at[0, n, mask], recv_sem=fold_sem.at[1, n, mask], device_id=geo.sibling, device_id_type=MESH)

    local = [pltpu.make_async_copy(halves[n], full[n].at[geo.local, core], local_sem.at[n]) for n in three]

    def gather(n):
        for mask in (1, 2):
            direct(n, mask).start()
        fold(n, 0).start()
        local[n].start()

    def forward(n):
        for mask in (1, 2):
            direct(n, mask).wait()
        for mask in (1, 2):
            relay(n, mask).start()
            fold(n, mask).start()

    gather(2)
    for n in four:
        to_sibling[n].wait()
        keep[n].wait()
        mine[n][...] = (mine[n][...].astype(f32) + first[n][...].astype(f32)).astype(bf16)

    def widen(n, mask):
        to = geo.across(mask)
        return pltpu.make_async_remote_copy(src_ref=mine[n].at[to], dst_ref=wide[n].at[mask], send_sem=wide_send.at[n, mask], recv_sem=wide_recv.at[n, mask], device_id=geo.member(2 * to + core), device_id_type=MESH)

    for n in four:
        for mask in ORDER[1:]:
            widen(n, mask).start()
    gather(0)
    for n in four:
        for mask in ORDER[1:]:
            widen(n, mask).wait()
        total = mine[n][geo.chip].astype(f32)
        for mask in ORDER[1:]:
            total += wide[n][mask].astype(f32)
        piece[n][...] = total.astype(bf16)

    def swap(n):
        return pltpu.make_async_remote_copy(src_ref=piece[n], dst_ref=other[n], send_sem=partner_sem.at[0, n], recv_sem=partner_sem.at[1, n], device_id=geo.partner, device_id_type=MESH)

    for n in four:
        swap(n).start()
    forward(2)
    for n in four:
        swap(n).wait()
        last[n][...] = (piece[n][...].astype(f32) + other[n][...].astype(f32)).astype(bf16)

    def spread(n, mask):
        return pltpu.make_async_remote_copy(src_ref=last[n], dst_ref=sums[n].at[core, geo.chip], send_sem=spread_send.at[n, mask], recv_sem=spread_recv.at[n, mask], device_id=geo.member(2 * geo.across(mask) + core), device_id_type=MESH)

    own = [pltpu.make_async_copy(last[n], sums[n].at[core, geo.chip], load_sem.at[n]) for n in four]
    for n in four:
        own[n].start()
        for mask in ORDER[1:]:
            spread(n, mask).start()
    gather(1)
    forward(0)

    def cross(n):
        return pltpu.make_async_remote_copy(src_ref=sums[n].at[core], dst_ref=sums[n].at[core], send_sem=cross_sem.at[0, n], recv_sem=cross_sem.at[1, n], device_id=geo.sibling, device_id_type=MESH)

    for n in four:
        own[n].wait()
        for mask in ORDER[1:]:
            spread(n, mask).wait()
        cross(n).start()
    forward(1)
    for n in (2, 0, 1):
        for mask in (1, 2):
            relay(n, mask).wait()
        fold(n, 3).start()
    for n in three:
        local[n].wait()
        for mask in range(4):
            fold(n, mask).wait()
    for n in four:
        cross(n).wait()


def final_exchange(mesh, halves, parts):
    ep, dp = mesh.shape["ep"], mesh.shape["dp"]
    chips, plane = ep * dp // 4, dp // 2
    bf16 = jnp.bfloat16
    anywhere = pl.BlockSpec(memory_space=pl.ANY)
    like = jax.ShapeDtypeStruct
    cut = [part.reshape(2, chips, part.shape[0] // (2 * chips), part.shape[1]) for part in parts]
    piece = [c.shape[2:] for c in cut]
    vmem, dma = pltpu.VMEM, pltpu.SemaphoreType.DMA
    scratch = [vmem((chips,) + s, bf16) for _ in range(3) for s in piece] + [vmem(s, bf16) for _ in range(3) for s in piece]
    scratch += [dma((4,)), dma((2, 4)), dma((4, chips)), dma((4, chips)), dma((2, 4)), dma((4, chips)), dma((4, chips)), dma((2, 4)), dma((2, 3, 4)), dma((3,)), dma((2, 3, plane))]
    outs = pl.pallas_call(
        functools.partial(final_kernel, ep, dp),
        name="final_exchange",
        out_shape=[like((plane, 2) + h.shape, bf16) for h in halves] + [like(c.shape, bf16) for c in cut],
        in_specs=[anywhere] * 7,
        out_specs=[anywhere] * 7,
        scratch_shapes=scratch,
        compiler_params=pltpu.CompilerParams(collective_id=3, has_side_effects=True, vmem_limit_bytes=40 * 2**20),
        cost_estimate=pl.CostEstimate(flops=10**10, bytes_accessed=30 * 2**20, transcendentals=0),
    )(*halves, *cut)
    full = [out.reshape(plane, 2 * out.shape[2], out.shape[3]) for out in outs[:3]]
    return full, [out.reshape(part.shape) for out, part in zip(outs[3:], parts)]


def take_rows(source, index):
    return jnp.take(source, index, axis=0, mode="clip")


def slot_owners(slot_of_token, slots):
    tokens = slot_of_token.shape[1]
    fine = 64
    token = jnp.arange(tokens, dtype=jnp.int32)
    coarse = (slot_of_token[:, :, None] // fine == jnp.arange(slots // fine, dtype=jnp.int32)).astype(jnp.bfloat16)
    value = jnp.stack([token // 256, token % 256, jnp.ones_like(token)], axis=1).astype(jnp.bfloat16)
    within = (slot_of_token[:, :, None] % fine == jnp.arange(fine, dtype=jnp.int32)).astype(jnp.bfloat16)
    spread = (value[None, :, :, None] * within[:, :, None, :]).reshape(slot_of_token.shape[0], tokens, 3 * fine)
    found = jnp.einsum("lta,ltb->lab", coarse, spread, preferred_element_type=jnp.float32).astype(jnp.int32)
    high, low, used = found[:, :, :fine], found[:, :, fine:2 * fine], found[:, :, 2 * fine:]
    return (high * 256 + low + (1 - used) * tokens).reshape(slot_of_token.shape[0], slots)


def solution(mesh):
    tok_spec = P(ALL_AXES, None)
    route_spec = P(None, ALL_AXES, None)
    exp_spec = P(None, "ep", None, None)
    repl_spec = P(None, None, None)
    ep, dp = mesh.shape["ep"], mesh.shape["dp"]
    members = ep * dp // 2
    to_partner = [(d, (d + members) % (2 * members)) for d in range(2 * members)]
    groups = [[side * members + m for m in range(members)] for side in range(2)]

    def body(act_in, grad_out, slot_ids, gate_vals, w_dense, w_gate, w_up, w_down, ws_gate, ws_up, ws_down):
        tokens, width = act_in.shape
        slots = 2 * tokens
        block = tokens // members
        experts = (w_gate, w_up, w_down)
        shared = (ws_gate, ws_up, ws_down)
        core, local = lax.axis_index("dp") % 2, lax.axis_index("dp") // 2

        def my_half(layer, w):
            rows, columns = w.shape[2] // 2, w.shape[3]
            return lax.dynamic_slice(w, (layer, local, core * rows, 0), (1, 1, rows, columns)).reshape(rows, columns)

        got = [lax.ppermute(my_half(0, w), ALL_AXES, to_partner) for w in experts[:1]]
        halves_two = [my_half(1, w) for w in experts[1:]]

        side = lax.axis_index("ep") // (ep // 2)
        turned = (slot_ids.reshape(2, tokens) + side * tokens) % slots
        owner = slot_owners(turned[1:], slots).reshape(2, members, block)

        def extended(rows):
            return jnp.pad(rows, ((0, 8), (0, 0)))

        def mix(act, layer):
            return (act.astype(jnp.float32) + dot32(act, w_dense[layer])).astype(jnp.bfloat16)

        def gated(grad, layer):
            return (gate_vals[layer] * grad.astype(jnp.float32)).astype(jnp.bfloat16)

        def go_out(blocks):
            return lax.all_to_all(blocks, ALL_AXES, 0, 0, axis_index_groups=groups)

        grads_two = extended(gated(grad_out, 1))
        grads_two = [take_rows(grads_two, owner[part].reshape(-1)).reshape(members, block, width) for part in range(2)]
        grads_first = go_out(grads_two[1])
        mixed_one, grads_late = lax.optimization_barrier((mix(act_in, 0), grads_two[0]))
        recv, act_two, *foreign = forward_exchange(mesh, turned[0:1], gate_vals[0], mixed_one, experts, shared, got)
        act_two, grads_late, halves_two = lax.optimization_barrier((act_two, grads_late, halves_two))
        grads_second = go_out(grads_late)
        got_two = [lax.ppermute(half, ALL_AXES, to_partner) for half in halves_two]
        mixed_two = mix(act_two, 1)

        def finish(layer, act, grad_mixed):
            g_dense = contract_rows(act, grad_mixed).astype(jnp.bfloat16)
            return (grad_mixed.astype(jnp.float32) + contract_cols(grad_mixed, w_dense[layer])).astype(jnp.bfloat16), g_dense

        def gather(half):
            return lax.all_gather(half, "dp", axis=0, tiled=True).reshape((dp // 2, 2 * half.shape[0], half.shape[1]))

        out = backward_exchange(mesh, 1, turned[1:2], [grads_second, grads_first], mixed_two, mixed_two, grad_out, experts, [foreign[3], *got_two], shared)
        shared_two, own_two = out[3:6], out[6:9]
        experts_two = [gather(half) for half in own_two]
        grad_one, dense_two = finish(1, act_two, out[1])
        sums_two = [lax.psum(part, ALL_AXES) for part in (dense_two, *shared_two)]

        out = backward_exchange(mesh, 0, turned[0:1], [recv], gated(grad_one, 0), mixed_one, grad_one, experts, foreign[:3], shared)
        shared_one, own_one = out[3:6], out[6:9]
        grad_act, dense_one = finish(0, act_in, out[1])
        experts_one, sums_one = final_exchange(mesh, own_one, [dense_one, *shared_one])

        expert_out = [jnp.stack(pair) for pair in zip(experts_one, experts_two)]
        sums_out = [jnp.stack(pair) for pair in zip(sums_one, sums_two)]
        return (grad_act, sums_out[0], *expert_out, *sums_out[1:])

    return jax.shard_map(body, mesh=mesh, in_specs=(tok_spec, tok_spec, route_spec, route_spec, repl_spec, exp_spec, exp_spec, exp_spec, repl_spec, repl_spec, repl_spec), out_specs=(tok_spec, repl_spec, exp_spec, exp_spec, exp_spec, repl_spec, repl_spec, repl_spec), check_vma=False)
```
